32 devices in a mesh: dom: 32 (over z, y, x, core).
Axes of the slice: x: 2, y: 2, z: 4, core: 2. Of those that a mesh axis runs over, the one named last changes fastest.
Arguments:
- positions: float32 [3, 131072], P(None, 'dom'), may hold values from -1.5 to 1.5
- velocity: float32 [3, 131072], P(None, 'dom'), may hold values from -6 to 6
- density_weight: float32 [131072], P('dom'), may hold values from 0.5 to 2
- embed_strength: float32 [131072], P('dom'), may hold values from 0.5 to 2
- occupied: int32 [131072], P('dom'), may hold values 0 or 1
- send_list: int32 [32, 8, 8], P('dom'), may hold values from 0 to 31, as said below
- send_count: int32 [32, 8], P('dom'), may hold values from 0 to 8, as said below
- pair_tiles: int32 [1024, 24], P('dom'), may hold values from 0 to 95, as said below
- pair_count: int32 [1024], P('dom'), may hold values from 1 to 24, as said below
- migrate_dest: int32 [1024], P('dom'), may hold values from 0 to 31, as said below
Outputs:
- force: float32 [3, 131072], P(None, 'dom')
- energy: float32 [131072], P('dom')
- moved: float32 [7, 262144], P(None, 'dom')
- moved_count: int32 [32], P('dom')
The draws below stay inside these ranges and needn't reach their ends.
Inputs may be any that keep to these rules, and one draw needn't show every extreme that they name: `send_list`: for one domain and one offset the entries are distinct local tile indices. send_count[s, k] counts the tiles domain s sends to domain s - o_k; it is 0 where that domain does not exist and 8 for some pairs. `pair_tiles`: entries index the frame of the tile's domain; a tile's entries are distinct and its first entry is its own local index. `pair_count`: the first tile of every domain uses all 24 slots. `migrate_dest`: A tile's new domain is within 4 of its domain; at most 4 tiles go from one domain to any other, at most 64 tiles to one domain, and both bounds are reached in every draw.
All inputs are finite; a program needn't handle non-finite values. No bound on the sum of `occupied` on one device may be relied on, other than what follows from the above.
Results may differ from the reference program's by a relative error of at most 0.0003.
Values sent between devices are 32-bit elements; how exact they have to be, the bound alone decides.
No kernel may reach another device: no remote copies, remote signals or barrier semaphores. Data moves between devices by JAX's collectives and lax.ppermute only.
A program may use at most 64 MiB of HBM per device.

```python
import math
import jax
import jax.numpy as jnp
from jax import lax

TILE = 128
TILES_DEV = 32
PAIRS = 24
GMAX = 8
RADIUS = 4
MMAX = 4
SPAN = 8
CAP = 64
DOMAINS = 32
TILES = 1024
ATOMS = 131072


def offset_list_drawn():
    return [position - RADIUS for position in range(RADIUS)] + [position + 1 for position in range(RADIUS)]


def draw_send_list(key, part):
    keys = jax.random.split(key, DOMAINS * SPAN)
    chosen = jax.vmap(lambda single: jax.random.permutation(single, TILES_DEV)[:GMAX])(keys)
    return chosen.reshape(DOMAINS, SPAN, GMAX).astype(jnp.int32)


def draw_send_count(key, part):
    offsets = jnp.array(offset_list_drawn(), dtype=jnp.int32)
    counts = jax.random.randint(jax.random.fold_in(key, 11), (DOMAINS, SPAN), 0, GMAX + 1).astype(jnp.int32)
    source = jnp.arange(DOMAINS, dtype=jnp.int32)[:, None]
    offset_ids = jnp.arange(SPAN, dtype=jnp.int32)[None, :]
    target = source - offsets[None, :]
    counts = jnp.where((source + offset_ids) % SPAN == 0, GMAX, counts)
    counts = jnp.where((target >= 0) & (target < DOMAINS), counts, 0)
    return counts.astype(jnp.int32)


def draw_pair_tiles(key, part):
    frame_size = TILES_DEV + SPAN * GMAX
    scores = jax.random.randint(jax.random.fold_in(key, 21), (TILES, frame_size), 0, 1 << 20).astype(jnp.int32)
    column = jnp.arange(frame_size, dtype=jnp.int32)[None, :]
    scores = scores * frame_size + column
    own_local = (jnp.arange(TILES, dtype=jnp.int32) % TILES_DEV)[:, None]
    scores = jnp.where(column == own_local, (1 << 20) * frame_size + frame_size, scores)
    chosen = jax.lax.top_k(scores, PAIRS)[1]
    return chosen.astype(jnp.int32)


def draw_pair_count(key, part):
    counts = jax.random.randint(jax.random.fold_in(key, 31), (TILES,), 1, PAIRS + 1).astype(jnp.int32)
    first = jnp.arange(TILES, dtype=jnp.int32) % TILES_DEV == 0
    return jnp.where(first, PAIRS, counts).astype(jnp.int32)


def draw_migrate_dest(key, part):
    offsets = jnp.array(offset_list_drawn(), dtype=jnp.int32)
    hottest = jax.random.randint(jax.random.fold_in(key, 41), (), RADIUS, DOMAINS - RADIUS).astype(jnp.int32)
    counts = jax.random.randint(jax.random.fold_in(key, 42), (DOMAINS, SPAN), 0, MMAX + 1).astype(jnp.int32)
    source = jnp.arange(DOMAINS, dtype=jnp.int32)[:, None]
    target = source + offsets[None, :]
    counts = jnp.where((target >= 0) & (target < DOMAINS), counts, 0)
    counts = jnp.where(target == hottest, MMAX, counts)
    counts = jnp.where(source == hottest, 0, counts)
    keys = jax.random.split(jax.random.fold_in(key, 43), DOMAINS)
    orders = jax.vmap(lambda single: jax.random.permutation(single, TILES_DEV))(keys).astype(jnp.int32)
    rank_of = jnp.argsort(orders, axis=1, stable=True).astype(jnp.int32)
    limits = jnp.cumsum(counts, axis=1).astype(jnp.int32)
    which = jnp.sum((rank_of[:, :, None] >= limits[:, None, :]).astype(jnp.int32), axis=2)
    strides = jnp.concatenate([offsets, jnp.zeros((1,), jnp.int32)])
    return (source + strides[which]).reshape(TILES).astype(jnp.int32)


def with_ends(values, stream_key, low, largest):
    index_at = [jax.random.randint(jax.random.fold_in(stream_key, axis), (), 0, length) for axis, length in enumerate(values.shape)]
    longest = values.shape.index(max(values.shape))
    beside = index_at[:longest] + [(index_at[longest] + 1) % values.shape[longest]] + index_at[longest + 1:]
    return values.at[tuple(index_at)].set(low).at[tuple(beside)].set(largest)


def shard_levels(key, shape, shards, smallest, high):
    def one(dim, blocks):
        steps = jax.random.uniform(jax.random.fold_in(jax.random.fold_in(key, 6), dim), (blocks,), jnp.float32, smallest / len(shards), high / len(shards))
        return jnp.repeat(jnp.exp(steps), shape[dim] // blocks).reshape((-1,) + (1,) * (len(shape) - dim - 1))

    factor_of = one(*shards[0])
    for cut in shards[1:]:
        factor_of = factor_of * one(*cut)
    return factor_of


def normal_values(rng, shape, spread, most, cuts=(), kind=jnp.bfloat16):
    loudness = shard_levels(rng, shape, cuts, -0.22, 0.18) if cuts else 1.0
    values = jax.random.normal(rng, shape, jnp.float32) * spread * loudness
    return jnp.minimum(jnp.maximum(values, -most), most).astype(kind)


def setup_inputs(seed: int = 0) -> dict:
    key_list = jax.random.split(jax.random.key(seed), 11)
    return {
        "positions": jnp.clip(jax.random.uniform(key_list[0], (3, ATOMS), jnp.float32, -1.5, 1.5) * shard_levels(key_list[0], (3, ATOMS), ((1, 32),), -0.4, 0.0), -1.5, 1.5),
        "velocity": normal_values(key_list[1], (3, ATOMS), 1.0, 6.0, ((1, 32),), jnp.float32),
        "density_weight": jnp.clip(jnp.exp(math.log(2.0) - 1.3862944 * jax.random.uniform(key_list[2], (ATOMS,), jnp.float32) ** shard_levels(key_list[2], (ATOMS,), ((0, 32),), -0.2, 0.2)), 0.5, 2.0),
        "embed_strength": jnp.clip(jnp.exp(math.log(2.0) - 1.3862944 * jax.random.uniform(key_list[3], (ATOMS,), jnp.float32) ** shard_levels(key_list[3], (ATOMS,), ((0, 32),), -0.2, 0.2)), 0.5, 2.0),
        "occupied": with_ends((jax.random.randint(key_list[4], (ATOMS,), 0, 4) < 3).astype(jnp.int32), jax.random.fold_in(key_list[4], 1), 0, 1),
        "send_list": draw_send_list(jax.random.fold_in(key_list[10], 71), 0),
        "send_count": draw_send_count(jax.random.fold_in(key_list[10], 71), 0),
        "pair_tiles": draw_pair_tiles(jax.random.fold_in(key_list[10], 71), 0),
        "pair_count": draw_pair_count(jax.random.fold_in(key_list[10], 71), 0),
        "migrate_dest": draw_migrate_dest(jax.random.fold_in(key_list[10], 71), 0),
    }


CUTOFF_SQUARE = 4.0
REPULSE = 0.05
TIME_STEP = 0.05
EXACT_PRODUCT = lax.Precision.HIGHEST

def offset_list():
    return [position - RADIUS for position in range(RADIUS)] + [position + 1 for position in range(RADIUS)]

def pair_weights(own_occ, near_occ, slot_list, used_count, tile_ids):
    tile_width = own_occ.shape[-1]
    used_mask = (jnp.arange(slot_list.shape[1], dtype=jnp.int32)[None, :] < used_count[:, None]).astype(jnp.float32)
    itself = (slot_list == tile_ids[:, None]).astype(jnp.float32)
    identity_mask = jnp.eye(tile_width, dtype=jnp.float32)
    weight = used_mask[:, :, None, None] * own_occ[:, None, :, None] * near_occ[:, :, None, :]
    return weight * (1.0 - itself[:, :, None, None] * identity_mask[None, None])

def closeness(own_pos, near_pos):
    distance = jnp.zeros(near_pos.shape[:2] + (own_pos.shape[2], near_pos.shape[3]), jnp.float32)
    for coordinate in range(3):
        difference = own_pos[:, None, coordinate, :, None] - near_pos[:, :, coordinate, None, :]
        distance = distance + difference * difference
    return jnp.maximum(1.0 - distance / CUTOFF_SQUARE, 0.0)

def density_terms(own_pos, own_occ, near_pos, near_chi, near_occ, slot_list, used_count, tile_ids):
    weight = pair_weights(own_occ, near_occ, slot_list, used_count, tile_ids)
    within = closeness(own_pos, near_pos)
    reach_cube = weight * within * within * within
    density = lax.optimization_barrier(jnp.sum(reach_cube * near_chi[:, :, None, :], axis=(1, 3)))
    pair_energy = lax.optimization_barrier(jnp.sum(reach_cube * within, axis=(1, 3)))
    return (density, pair_energy)

def force_terms(own_pos, own_occ, own_chi, own_slope, near_pos, near_chi, near_occ, near_slope, slot_list, used_count, tile_ids):
    weight = pair_weights(own_occ, near_occ, slot_list, used_count, tile_ids)
    within = closeness(own_pos, near_pos)
    square = within * within
    mixed_slope = own_slope[:, None, :, None] * near_chi[:, :, None, :] + near_slope[:, :, None, :] * own_chi[:, None, :, None]
    pair_coef = weight * (2.0 / CUTOFF_SQUARE) * (3.0 * square * mixed_slope + 4.0 * REPULSE * square * within)
    total_coef = lax.optimization_barrier(jnp.sum(pair_coef, axis=(1, 3)))
    pulled = jnp.einsum('bpij,bpcj->bci', pair_coef, near_pos, precision=EXACT_PRODUCT)
    return own_pos * total_coef[:, None, :] - pulled

def ghost_tiles(per_domain, send_list, send_count):
    domains = per_domain.shape[0]
    offsets = jnp.array(offset_list(), dtype=jnp.int32)
    source = jnp.arange(domains, dtype=jnp.int32)[:, None] + offsets[None, :]
    inside = (source >= 0) & (source < domains)
    clipped = jnp.clip(source, 0, domains - 1).astype(jnp.int32)
    offset_ids = jnp.arange(SPAN, dtype=jnp.int32)[None, :]
    tile_list = send_list[clipped, offset_ids]
    counts = send_count[clipped, offset_ids]
    live_mask = inside[:, :, None] & (jnp.arange(GMAX, dtype=jnp.int32)[None, None, :] < counts[:, :, None])
    picked = per_domain[clipped[:, :, None], tile_list]
    live_float = live_mask.astype(jnp.float32).reshape(live_mask.shape + (1,) * (picked.ndim - 3))
    return (picked * live_float).reshape((domains, SPAN * GMAX) + per_domain.shape[2:])

def reference(positions, velocity, density_weight, embed_strength, occupied, send_list, send_count, pair_tiles, pair_count, migrate_dest):
    domains = send_list.shape[0]
    tiles_here = pair_tiles.shape[0] // domains
    tile_width = TILE
    filled = occupied.astype(jnp.float32).reshape(domains, tiles_here, tile_width)
    pos_tiles = positions.reshape(3, domains, tiles_here, tile_width).transpose(1, 2, 0, 3)
    vel_tiles = velocity.reshape(3, domains, tiles_here, tile_width).transpose(1, 2, 0, 3)
    weight_tiles = density_weight.reshape(domains, tiles_here, tile_width)
    embed_tiles = embed_strength.reshape(domains, tiles_here, tile_width)
    packed = jnp.concatenate([pos_tiles, weight_tiles[:, :, None], filled[:, :, None]], axis=2)
    frame_tiles = jnp.concatenate([packed, ghost_tiles(packed, send_list, send_count)], axis=1)
    slot_tiles = pair_tiles.reshape(domains, tiles_here, PAIRS)
    used_tiles = pair_count.reshape(domains, tiles_here)
    tile_ids = jnp.arange(tiles_here, dtype=jnp.int32)

    def density_domain(batch_items):
        native, frames, slot_list, used_count = batch_items
        nearby = frames[slot_list]
        return density_terms(native[:, 0:3], native[:, 4], nearby[:, :, 0:3], nearby[:, :, 3], nearby[:, :, 4], slot_list, used_count, tile_ids)
    density, pair_energy = lax.map(density_domain, (packed, frame_tiles, slot_tiles, used_tiles))
    root_term = jnp.sqrt(1.0 + density)
    slope_tiles = -0.5 * embed_tiles * filled / root_term
    energy_tiles = filled * (-embed_tiles * root_term + 0.5 * REPULSE * pair_energy)
    slope_frame = jnp.concatenate([slope_tiles, ghost_tiles(slope_tiles, send_list, send_count)], axis=1)

    def force_domain(batch_items):
        native, frames, slot_list, used_count, own_slope, frame_slope = batch_items
        nearby = frames[slot_list]
        near_slope = frame_slope[slot_list]
        return force_terms(native[:, 0:3], native[:, 4], native[:, 3], own_slope, nearby[:, :, 0:3], nearby[:, :, 3], nearby[:, :, 4], near_slope, slot_list, used_count, tile_ids)
    force_tiles = lax.map(force_domain, (packed, frame_tiles, slot_tiles, used_tiles, slope_tiles, slope_frame))
    new_vel = vel_tiles + TIME_STEP * force_tiles
    new_pos = pos_tiles + TIME_STEP * new_vel
    payload = jnp.concatenate([new_pos, new_vel, filled[:, :, None]], axis=2).reshape(domains * tiles_here, 7, tile_width)
    onehot = (migrate_dest[:, None] == jnp.arange(domains, dtype=jnp.int32)[None, :]).astype(jnp.int32)
    before = (jnp.cumsum(onehot, axis=0) - onehot).astype(jnp.int32)
    slot_index = lax.optimization_barrier(jnp.sum(onehot * before, axis=1)).astype(jnp.int32)
    moved_tiles = jnp.zeros((domains * CAP, 7, tile_width), jnp.float32).at[migrate_dest * CAP + slot_index].set(payload)
    tile_atoms = lax.optimization_barrier(jnp.sum(occupied.reshape(domains * tiles_here, tile_width), axis=1)).astype(jnp.int32)
    moved_count = lax.optimization_barrier(jnp.sum(onehot * tile_atoms[:, None], axis=0)).astype(jnp.int32)
    force = force_tiles.transpose(2, 0, 1, 3).reshape(3, domains * tiles_here * tile_width)
    energy = energy_tiles.reshape(domains * tiles_here * tile_width)
    moved = moved_tiles.transpose(1, 0, 2).reshape(7, domains * CAP * tile_width)
    return (force, energy, moved, moved_count)
```

```python
import functools

import jax
import jax.numpy as jnp
from jax import lax
from jax.experimental import pallas as pl
from jax.experimental.pallas import tpu as pltpu
from jax.sharding import PartitionSpec as P

TILE = 128
RADIUS = 4
MMAX = 4
REPULSE = 0.05
TIME_STEP = 0.05
SPAN = 2 * RADIUS
GROUP = 2 * RADIUS
F32 = jnp.float32
BF16 = jnp.bfloat16
I32 = jnp.int32
CHUNK = 16
FEATURES = 32
SCALE = 0.1 ** (1.0 / 3.0)
OFFSETS = [k - RADIUS for k in range(RADIUS)] + [k + 1 for k in range(RADIUS)]
CONTRACT_FIRST = (((0,), (0,)), ((), ()))

VMEM = pl.BlockSpec(memory_space=pltpu.VMEM)
SMEM = pl.BlockSpec(memory_space=pltpu.SMEM)
PARAMS = pltpu.CompilerParams(vmem_limit_bytes=56 * 1024 * 1024)


def columns(tile):
    return pl.ds(pl.multiple_of(tile * TILE, TILE), TILE)


def split(value):
    high = value.astype(BF16).astype(F32)
    rest = value - high
    mid = rest.astype(BF16).astype(F32)
    return high, mid, rest - mid


def pack_kernel(
    domains,
    me_ref,
    send_list,
    send_count,
    dest_ref,
    pos_ref,
    vel_ref,
    chi_ref,
    occ_ref,
    own_ref,
    cross_ref,
    ghost_row,
    move_row,
    rank_ref,
):
    me = me_ref[0]
    tiles = chi_ref.shape[0]
    ghosts = send_list.shape[1]
    base = 4 * ghosts
    filled = occ_ref[...].astype(F32)
    weight = chi_ref[...] * filled
    for t in range(tiles):
        span = slice(t * TILE, (t + 1) * TILE)
        ghost_row[t, 0:3] = pos_ref[:, span]
        ghost_row[t, 3:4] = weight[t : t + 1]
        move_row[t, 0:3] = pos_ref[:, span]
        move_row[t, 3:4] = filled[t : t + 1]
        move_row[t, 4:7] = vel_ref[:, span]
    nothing = jnp.full((1, TILE), -1.0, F32)

    def place(target, rows):
        inside = (target // GROUP) == (me // GROUP)

        @pl.when(inside)
        def _():
            rows(own_ref, target % GROUP)

        @pl.when(jnp.logical_not(inside))
        def _():
            rows(cross_ref, (target + RADIUS) % GROUP)

    for k, offset in enumerate(OFFSETS):
        target = me - offset

        @pl.when((target >= 0) & (target < domains))
        def _(k=k, target=target):
            used = send_count[k]

            def rows(out_ref, at):
                for g in range(ghosts):
                    block = ghost_row[send_list[k, g]]
                    live = g < used
                    out_ref[at, 4 * g : 4 * g + 3] = block[0:3]
                    out_ref[at, 4 * g + 3 : 4 * g + 4] = jnp.where(live, block[3:4], nothing)
                for m in range(MMAX):
                    out_ref[at, base + 8 * m + 3 : base + 8 * m + 4] = nothing

            place(target, rows)

    for r in range(2 * RADIUS + 1):
        rank_ref[r] = 0

    def move(t, carry):
        target = dest_ref[t]
        relative = target - me + RADIUS

        @pl.when(target != me)
        def _():
            rank = rank_ref[relative]
            rank_ref[relative] = rank + 1

            def rows(out_ref, at):
                out_ref[at, pl.ds(pl.multiple_of(base + 8 * rank, 8), 8)] = move_row[t]

            place(target, rows)

        return carry

    lax.fori_loop(0, tiles, move, 0)


def arrived(me, source, own_ref, cross_ref, use):
    inside = (source // GROUP) == (me // GROUP)

    @pl.when(inside)
    def _():
        use(own_ref, source % GROUP)

    @pl.when(jnp.logical_not(inside))
    def _():
        use(cross_ref, (source + RADIUS) % GROUP)


def load_frame(me, domains, ghosts, pos_ref, chi_ref, occ_ref, own_ref, cross_ref, frame):
    tiles = chi_ref.shape[0]
    weight = chi_ref[...] * occ_ref[...].astype(F32)
    for t in range(tiles):
        frame[t, 0:3] = pos_ref[:, t * TILE : (t + 1) * TILE]
        frame[t, 3:4] = weight[t : t + 1]
    for k, offset in enumerate(OFFSETS):
        source = me + offset
        start = tiles + k * ghosts
        valid = (source >= 0) & (source < domains)

        @pl.when(valid)
        def _(start=start, source=source):
            def use(ref, at):
                for g in range(ghosts):
                    frame[start + g, 0:4] = ref[at, 4 * g : 4 * g + 4]

            arrived(me, source, own_ref, cross_ref, use)

        @pl.when(jnp.logical_not(valid))
        def _(start=start):
            for g in range(ghosts):
                frame[start + g, 0:4] = jnp.full((4, TILE), -1.0, F32)

    frame[tiles + SPAN * ghosts, 0:4] = jnp.full((4, TILE), -1.0, F32)


def live_counts(tiles, ghosts, frame, used_ref):
    for k in range(SPAN):
        start = tiles + k * ghosts
        first = frame[start : start + ghosts, 3, :]
        lane = lax.broadcasted_iota(I32, first.shape, 1)
        flag = jnp.where((first >= 0.0) & (lane == 0), 1.0, 0.0)
        used_ref[k] = jnp.sum(flag).astype(I32)


def build_list(pair_tiles, pair_count, used_ref, tiles, ghosts, null, list_ref):
    def tile_step(t, n):
        def pair_step(p, n):
            f = pair_tiles[t, p]
            slot = jnp.maximum(f - tiles, 0)
            live = (f < tiles) | (slot % ghosts < used_ref[slot // ghosts])
            list_ref[n] = t * TILE + f
            return n + live.astype(I32)

        return lax.fori_loop(1, pair_count[t], pair_step, n)

    n = lax.fori_loop(0, tiles, tile_step, 0)
    for e in range(CHUNK):
        list_ref[n + e] = null
    return n


def scaled(rows, scale):
    half = rows[0:3] * 0.5
    norm = 0.5 - (half[0:1] * half[0:1] + half[1:2] * half[1:2] + half[2:3] * half[2:3])
    norm = jnp.where(rows[3:4] > 0.0, norm, -64.0) * scale
    return half, norm


def stream_features(rows, scale, slope):
    half, norm = scaled(rows, scale)
    high, mid, low = split(half + half)
    one = jnp.ones((1, TILE), F32)
    nh, nm, nl = split(norm)
    weight = jnp.maximum(rows[3:4], 0.0)
    wh, wm, _ = split(weight)
    if slope is None:
        tail = [wh, wm, jnp.zeros((6, TILE), F32)]
    else:
        sh, sm, _ = split(slope)
        tail = [wh, wm, wh, sh, sm, sh, jnp.zeros((2, TILE), F32)]
    parts = [high, one, high, one, high, one, mid, nm, low, nl, mid, nh] + tail
    return jnp.concatenate(parts, axis=0).astype(BF16)


def held_features(rows, scale):
    half, norm = scaled(rows, scale)
    high, mid, low = split(half * scale)
    nh, nm, nl = split(norm)
    one = jnp.ones((1, TILE), F32)
    parts = [high, nh, mid, nm, low, nl, high, one, high, one, mid, one, jnp.zeros((8, TILE), F32)]
    return jnp.concatenate(parts, axis=0).astype(BF16)


def row_mask(columns_of, width):
    row = lax.broadcasted_iota(I32, (FEATURES, width), 0)
    lane = lax.broadcasted_iota(I32, (FEATURES, width), 1) // TILE
    mask = jnp.zeros((FEATURES, width), jnp.bool_)
    for block, rows in enumerate(columns_of):
        for r in rows:
            mask = mask | ((row == r) & (lane == block))
    return jnp.where(mask, 1.0, 0.0).astype(BF16)


def fold(value):
    return value.reshape(TILE // 8, 8, TILE).sum(axis=0)


def off_diagonal():
    row = lax.broadcasted_iota(I32, (TILE, TILE), 0)
    lane = lax.broadcasted_iota(I32, (TILE, TILE), 1)
    return row != lane


def density_kernel(
    domains,
    me_ref,
    send_list,
    pair_tiles,
    pair_count,
    pos_ref,
    chi_ref,
    embed_ref,
    occ_ref,
    own_ref,
    cross_ref,
    slope_ref,
    energy_ref,
    out_ref,
    frame,
    stream,
    held,
    acc_rho,
    acc_pair,
    list_ref,
    used_ref,
):
    me = me_ref[0]
    tiles = chi_ref.shape[0]
    ghosts = send_list.shape[1]
    frames = tiles + SPAN * ghosts
    load_frame(me, domains, ghosts, pos_ref, chi_ref, occ_ref, own_ref, cross_ref, frame)
    live_counts(tiles, ghosts, frame, used_ref)
    n = build_list(pair_tiles, pair_count, used_ref, tiles, ghosts, frames, list_ref)
    picks = row_mask([[24, 25]], TILE)
    for t in range(tiles):
        rows = frame[t, 0:4]
        held[t, :, 0:TILE] = held_features(rows, 1.0)
        held[t, :, TILE:] = picks
    for f in range(frames + 1):
        stream[f] = stream_features(frame[f, 0:4], 1.0, None)
    apart = off_diagonal()

    def terms(t, f):
        both = lax.dot_general(stream[f], held[t], CONTRACT_FIRST, preferred_element_type=F32)
        reach = jnp.maximum(both[:, :TILE], 0.0)
        return reach, both[:, TILE:]

    def own_step(c, carry):
        for e in range(8):
            t = c * 8 + e
            reach, weight = terms(t, t)
            reach = jnp.where(apart, reach, 0.0)
            square = reach * reach
            acc_rho[t] = fold(square * reach * weight)
            acc_pair[t] = fold(square * square)
        return carry

    lax.fori_loop(0, tiles // 8, own_step, 0)

    def step(c, carry):
        for e in range(CHUNK):
            code = list_ref[c * CHUNK + e]
            t = code // TILE
            f = code % TILE
            reach, weight = terms(t, f)
            square = reach * reach
            acc_rho[t] += fold(square * reach * weight)
            acc_pair[t] += fold(square * square)
        return carry

    lax.fori_loop(0, (n + CHUNK - 1) // CHUNK, step, 0)

    filled = occ_ref[...].astype(F32)
    embed = embed_ref[...]
    root = jnp.sqrt(1.0 + jnp.sum(acc_rho[...], axis=1))
    slope = -0.5 * embed * filled / root
    slope_ref[...] = slope
    energy_ref[...] = filled * (0.5 * REPULSE * jnp.sum(acc_pair[...], axis=1) - embed * root)
    for k, offset in enumerate(OFFSETS):
        target = me - offset

        @pl.when((target >= 0) & (target < domains))
        def _(k=k, target=target):
            for g in range(ghosts):
                out_ref[target, g : g + 1] = slope_ref[pl.ds(send_list[k, g], 1)]


def force_kernel(
    domains,
    me_ref,
    dest_ref,
    pair_tiles,
    pair_count,
    pos_ref,
    chi_ref,
    occ_ref,
    own_ref,
    cross_ref,
    slope_ref,
    ghost_slope_ref,
    force_ref,
    out_ref,
    frame,
    stream,
    held,
    wide,
    acc,
    total,
    list_ref,
    used_ref,
    rank_ref,
):
    me = me_ref[0]
    tiles = chi_ref.shape[0]
    ghosts = ghost_slope_ref.shape[1]
    frames = tiles + SPAN * ghosts
    load_frame(me, domains, ghosts, pos_ref, chi_ref, occ_ref, own_ref, cross_ref, frame)
    live_counts(tiles, ghosts, frame, used_ref)
    n = build_list(pair_tiles, pair_count, used_ref, tiles, ghosts, frames, list_ref)
    for t in range(tiles):
        frame[t, 4:5] = slope_ref[t : t + 1]
    for k, offset in enumerate(OFFSETS):
        source = jnp.clip(me + offset, 0, domains - 1)
        for g in range(ghosts):
            frame[tiles + k * ghosts + g, 4:5] = ghost_slope_ref[source, g : g + 1]
    frame[frames, 4:5] = jnp.zeros((1, TILE), F32)
    ratio = 1.5 / (SCALE * SCALE)
    for t in range(tiles):
        rows = frame[t, 0:4]
        held[t, :, 0:TILE] = held_features(rows, SCALE)
        sh, sm, _ = split(frame[t, 4:5] * ratio)
        wh, wm, _ = split(rows[3:4] * ratio)
        parts = [jnp.zeros((24, TILE), F32), sh, sh, sm, wh, wh, wm, jnp.zeros((2, TILE), F32)]
        held[t, :, TILE:] = jnp.concatenate(parts, axis=0).astype(BF16)
    for f in range(frames + 1):
        filled = frame[f, 3:4] > 0.0
        slope = jnp.where(filled, frame[f, 4:5], 0.0)
        stream[f] = stream_features(frame[f, 0:4], SCALE, slope)
    picks = row_mask([[c, 12 + c, 16 + c] for c in range(3)], 3 * TILE)

    def widen(f):
        three = lax.dot_general(stream[f], picks, CONTRACT_FIRST, preferred_element_type=F32)
        for c in range(3):
            wide[f, c] = three[:, c * TILE : (c + 1) * TILE]

    def widen_own(c, carry):
        for e in range(4):
            widen(c * 4 + e)
        return carry

    lax.fori_loop(0, tiles // 4, widen_own, 0)

    def widen_some(k, carry):
        def one(g, carry):
            widen(tiles + k * ghosts + g)
            return carry

        return lax.fori_loop(0, used_ref[k], one, carry)

    lax.fori_loop(0, SPAN, widen_some, 0)
    widen(frames)
    apart = off_diagonal()

    def coefficient(t, f):
        both = lax.dot_general(stream[f], held[t], CONTRACT_FIRST, preferred_element_type=F32)
        reach = jnp.maximum(both[:, :TILE], 0.0)
        return reach * reach * (reach + both[:, TILE:])

    def own_step(c, carry):
        for e in range(8):
            t = c * 8 + e
            coef = jnp.where(apart, coefficient(t, t), 0.0)
            acc[t, 3] = fold(coef)
            for q in range(3):
                acc[t, q] = fold(coef * wide[t, q])
        return carry

    lax.fori_loop(0, tiles // 8, own_step, 0)

    def step(c, carry):
        for e in range(CHUNK):
            code = list_ref[c * CHUNK + e]
            t = code // TILE
            f = code % TILE
            coef = coefficient(t, f)
            acc[t, 3] += fold(coef)
            for q in range(3):
                acc[t, q] += fold(coef * wide[f, q])
        return carry

    lax.fori_loop(0, (n + CHUNK - 1) // CHUNK, step, 0)

    whole = jnp.sum(acc[:, 3], axis=1)
    pulled = [jnp.sum(acc[:, q], axis=1) for q in range(3)]
    for q in range(3):
        total[q] = pulled[q]
    total[3] = whole
    for t in range(tiles):
        sums = jnp.concatenate([total[q, t : t + 1] for q in range(3)], axis=0)
        force_ref[:, t * TILE : (t + 1) * TILE] = frame[t, 0:3] * total[3, t : t + 1] - sums

    for r in range(2 * RADIUS + 1):
        rank_ref[r] = 0

    def move(t, carry):
        target = dest_ref[t]
        relative = target - me + RADIUS

        @pl.when(target != me)
        def _():
            rank = rank_ref[relative]
            rank_ref[relative] = rank + 1
            out_ref[target, pl.ds(4 * rank, 3)] = force_ref[:, columns(t)]

        return carry

    lax.fori_loop(0, tiles, move, 0)


def unpack_kernel(
    domains,
    ghosts,
    me_ref,
    dest_ref,
    pos_ref,
    vel_ref,
    occ_ref,
    own_ref,
    cross_ref,
    force_ref,
    in_ref,
    moved_ref,
    count_ref,
    next_ref,
    held_ref,
    atoms_ref,
):
    me = me_ref[0]
    tiles = occ_ref.shape[0]
    base = 4 * ghosts
    held_ref[...] = occ_ref[...].astype(F32)
    moved_ref[...] = jnp.zeros_like(moved_ref)
    next_ref[0] = 0
    atoms_ref[...] = jnp.zeros_like(atoms_ref)

    def put(rows, velocity, filled, force):
        at = next_ref[0]
        next_ref[0] = at + 1
        new_vel = velocity + TIME_STEP * force
        new_pos = rows + TIME_STEP * new_vel
        moved_ref[0:3, columns(at)] = new_pos
        moved_ref[3:6, columns(at)] = new_vel
        moved_ref[6:7, columns(at)] = filled
        atoms_ref[...] += filled

    def from_other(source):
        @pl.when((source >= 0) & (source < domains))
        def _():
            def use(ref, at):
                first = jnp.concatenate(
                    [ref[at, base + 8 * m + 3 : base + 8 * m + 4, :] for m in range(MMAX)], axis=0
                )
                lane = lax.broadcasted_iota(I32, first.shape, 1)
                flag = jnp.where((first >= 0.0) & (lane == 0), 1.0, 0.0)
                count = jnp.sum(flag).astype(I32)
                for m in range(MMAX):

                    @pl.when(m < count)
                    def _(m=m):
                        row = base + 8 * m
                        put(
                            ref[at, row : row + 3],
                            ref[at, row + 4 : row + 7],
                            ref[at, row + 3 : row + 4],
                            in_ref[source, 4 * m : 4 * m + 3],
                        )

            arrived(me, source, own_ref, cross_ref, use)

    for offset in OFFSETS[:RADIUS]:
        from_other(me + offset)

    def stay(t, carry):
        @pl.when(dest_ref[t] == me)
        def _():
            put(
                pos_ref[:, columns(t)],
                vel_ref[:, columns(t)],
                held_ref[pl.ds(t, 1)],
                force_ref[:, columns(t)],
            )

        return carry

    lax.fori_loop(0, tiles, stay, 0)
    for offset in OFFSETS[RADIUS:]:
        from_other(me + offset)
    count_ref[0] = jnp.sum(atoms_ref[...]).astype(I32)


def per_device(
    positions,
    velocity,
    density_weight,
    embed_strength,
    occupied,
    send_list,
    send_count,
    pair_tiles,
    pair_count,
    migrate_dest,
):
    domains = lax.axis_size("dom")
    tiles, pairs = pair_tiles.shape
    ghosts = send_list.shape[2]
    frames = tiles + SPAN * ghosts
    me = lax.axis_index("dom").astype(I32)[None]
    chi = density_weight.reshape(tiles, TILE)
    embed = embed_strength.reshape(tiles, TILE)
    occ = occupied.reshape(tiles, TILE)
    sends = send_list[0]
    sent = send_count[0]
    rows = 4 * ghosts + 8 * MMAX
    capacity = tiles + 2 * RADIUS * MMAX
    entries = tiles * pairs + 2 * CHUNK
    shape = jax.ShapeDtypeStruct

    own, cross = pl.pallas_call(
        functools.partial(pack_kernel, domains),
        out_shape=[shape((GROUP, rows, TILE), F32)] * 2,
        in_specs=[SMEM] * 4 + [VMEM] * 4,
        out_specs=[VMEM] * 2,
        scratch_shapes=[
            pltpu.VMEM((tiles, 8, TILE), F32),
            pltpu.VMEM((tiles, 8, TILE), F32),
            pltpu.SMEM((2 * RADIUS + 1,), I32),
        ],
        name="pack",
    )(me, sends, sent, migrate_dest, positions, velocity, chi, occ)
    blocks = [[b + i for i in range(GROUP)] for b in range(0, domains, GROUP)]
    crossing = [[(b + i - RADIUS) % domains for i in range(GROUP)] for b in range(0, domains, GROUP)]
    own = lax.all_to_all(own, "dom", 0, 0, axis_index_groups=blocks)
    cross = lax.all_to_all(cross, "dom", 0, 0, axis_index_groups=crossing)

    slope, energy, slope_out = pl.pallas_call(
        functools.partial(density_kernel, domains),
        out_shape=[
            shape((tiles, TILE), F32),
            shape((tiles, TILE), F32),
            shape((domains, ghosts, TILE), F32),
        ],
        in_specs=[SMEM] * 4 + [VMEM] * 6,
        out_specs=[VMEM] * 3,
        scratch_shapes=[
            pltpu.VMEM((frames + 1, 8, TILE), F32),
            pltpu.VMEM((frames + 1, FEATURES, TILE), BF16),
            pltpu.VMEM((tiles, FEATURES, 2 * TILE), BF16),
            pltpu.VMEM((tiles, 8, TILE), F32),
            pltpu.VMEM((tiles, 8, TILE), F32),
            pltpu.SMEM((entries,), I32),
            pltpu.SMEM((SPAN,), I32),
        ],
        compiler_params=PARAMS,
        name="density",
    )(me, sends, pair_tiles, pair_count, positions, chi, embed, occ, own, cross)
    slope_in = lax.all_to_all(slope_out, "dom", 0, 0)

    force, force_out = pl.pallas_call(
        functools.partial(force_kernel, domains),
        out_shape=[shape(positions.shape, F32), shape((domains, 4 * MMAX, TILE), F32)],
        in_specs=[SMEM] * 4 + [VMEM] * 7,
        out_specs=[VMEM] * 2,
        scratch_shapes=[
            pltpu.VMEM((frames + 1, 8, TILE), F32),
            pltpu.VMEM((frames + 1, FEATURES, TILE), BF16),
            pltpu.VMEM((tiles, FEATURES, 2 * TILE), BF16),
            pltpu.VMEM((frames + 1, 3, TILE, TILE), F32),
            pltpu.VMEM((tiles, 4, 8, TILE), F32),
            pltpu.VMEM((4, tiles, TILE), F32),
            pltpu.SMEM((entries,), I32),
            pltpu.SMEM((SPAN,), I32),
            pltpu.SMEM((2 * RADIUS + 1,), I32),
        ],
        compiler_params=PARAMS,
        name="force",
    )(me, migrate_dest, pair_tiles, pair_count, positions, chi, occ, own, cross, slope, slope_in)
    force_in = lax.all_to_all(force_out, "dom", 0, 0)

    moved, count = pl.pallas_call(
        functools.partial(unpack_kernel, domains, ghosts),
        out_shape=[shape((7, capacity * TILE), F32), shape((1,), I32)],
        in_specs=[SMEM] * 2 + [VMEM] * 7,
        out_specs=[VMEM, SMEM],
        scratch_shapes=[pltpu.SMEM((1,), I32), pltpu.VMEM((tiles, TILE), F32), pltpu.VMEM((1, TILE), F32)],
        name="unpack",
    )(me, migrate_dest, positions, velocity, occ, own, cross, force, force_in)
    return (force, energy.reshape(tiles * TILE), moved, count)


def solution(mesh):
    placed = (
        P(None, "dom"),
        P(None, "dom"),
        P("dom"),
        P("dom"),
        P("dom"),
        P("dom", None, None),
        P("dom", None),
        P("dom", None),
        P("dom"),
        P("dom"),
    )
    return jax.shard_map(
        per_device,
        mesh=mesh,
        in_specs=placed,
        out_specs=(P(None, "dom"), P("dom"), P(None, "dom"), P("dom")),
        check_vma=False,
    )
```

```python
import functools

import jax
import jax.numpy as jnp
from jax import lax
from jax.experimental import pallas as pl
from jax.experimental.pallas import tpu as pltpu
from jax.sharding import PartitionSpec as P

TILE = 128
RADIUS = 4
MMAX = 4
REPULSE = 0.05
TIME_STEP = 0.05
SPAN = 2 * RADIUS
GROUP = 2 * RADIUS
F32 = jnp.float32
BF16 = jnp.bfloat16
I32 = jnp.int32
CHUNK = 16
WIDE = 8
FEATURES = 32
SCALE = 0.1 ** (1.0 / 3.0)
OFFSETS = [k - RADIUS for k in range(RADIUS)] + [k + 1 for k in range(RADIUS)]
CONTRACT_FIRST = (((0,), (0,)), ((), ()))

VMEM = pl.BlockSpec(memory_space=pltpu.VMEM)
SMEM = pl.BlockSpec(memory_space=pltpu.SMEM)
PARAMS = pltpu.CompilerParams(vmem_limit_bytes=56 * 1024 * 1024)


def columns(tile):
    return pl.ds(pl.multiple_of(tile * TILE, TILE), TILE)


def split(value):
    high = value.astype(BF16).astype(F32)
    rest = value - high
    mid = rest.astype(BF16).astype(F32)
    return high, mid, rest - mid


def pack_kernel(
    domains,
    me_ref,
    send_list,
    send_count,
    dest_ref,
    pos_ref,
    vel_ref,
    chi_ref,
    occ_ref,
    own_ref,
    cross_ref,
    ghost_row,
    move_row,
    rank_ref,
):
    me = me_ref[0]
    tiles = chi_ref.shape[0]
    ghosts = send_list.shape[1]
    base = 4 * ghosts
    filled = occ_ref[...].astype(F32)
    weight = chi_ref[...] * filled
    for t in range(tiles):
        span = slice(t * TILE, (t + 1) * TILE)
        ghost_row[t, 0:3] = pos_ref[:, span]
        ghost_row[t, 3:4] = weight[t : t + 1]
        move_row[t, 0:3] = pos_ref[:, span]
        move_row[t, 3:4] = filled[t : t + 1]
        move_row[t, 4:7] = vel_ref[:, span]
    nothing = jnp.full((1, TILE), -1.0, F32)

    def place(target, rows):
        inside = (target // GROUP) == (me // GROUP)

        @pl.when(inside)
        def _():
            rows(own_ref, target % GROUP)

        @pl.when(jnp.logical_not(inside))
        def _():
            rows(cross_ref, (target + RADIUS) % GROUP)

    for k, offset in enumerate(OFFSETS):
        target = me - offset

        @pl.when((target >= 0) & (target < domains))
        def _(k=k, target=target):
            used = send_count[k]

            def rows(out_ref, at):
                for g in range(ghosts):
                    block = ghost_row[send_list[k, g]]
                    live = g < used
                    out_ref[at, 4 * g : 4 * g + 3] = block[0:3]
                    out_ref[at, 4 * g + 3 : 4 * g + 4] = jnp.where(live, block[3:4], nothing)
                for m in range(MMAX):
                    out_ref[at, base + 8 * m + 3 : base + 8 * m + 4] = nothing

            place(target, rows)

    for r in range(2 * RADIUS + 1):
        rank_ref[r] = 0

    def move(t, carry):
        target = dest_ref[t]
        relative = target - me + RADIUS

        @pl.when(target != me)
        def _():
            rank = rank_ref[relative]
            rank_ref[relative] = rank + 1

            def rows(out_ref, at):
                out_ref[at, pl.ds(pl.multiple_of(base + 8 * rank, 8), 8)] = move_row[t]

            place(target, rows)

        return carry

    lax.fori_loop(0, tiles, move, 0)


def arrived(me, source, own_ref, cross_ref, use):
    inside = (source // GROUP) == (me // GROUP)

    @pl.when(inside)
    def _():
        use(own_ref, source % GROUP)

    @pl.when(jnp.logical_not(inside))
    def _():
        use(cross_ref, (source + RADIUS) % GROUP)


def load_own(pos_ref, chi_ref, occ_ref, frame):
    tiles = chi_ref.shape[0]
    weight = chi_ref[...] * occ_ref[...].astype(F32)
    for t in range(tiles):
        frame[t, 0:3] = pos_ref[:, t * TILE : (t + 1) * TILE]
        frame[t, 3:4] = weight[t : t + 1]
    last = frame.shape[0] - 1
    frame[last, 0:4] = jnp.full((4, TILE), -1.0, F32)
    frame[last, 4:5] = jnp.zeros((1, TILE), F32)


def load_ghosts(me, domains, tiles, ghosts, own_ref, cross_ref, frame):
    for k, offset in enumerate(OFFSETS):
        source = me + offset
        start = tiles + k * ghosts
        valid = (source >= 0) & (source < domains)

        @pl.when(valid)
        def _(start=start, source=source):
            def use(ref, at):
                for g in range(ghosts):
                    frame[start + g, 0:4] = ref[at, 4 * g : 4 * g + 4]

            arrived(me, source, own_ref, cross_ref, use)

        @pl.when(jnp.logical_not(valid))
        def _(start=start):
            for g in range(ghosts):
                frame[start + g, 0:4] = jnp.full((4, TILE), -1.0, F32)


def live_counts(tiles, ghosts, frame, used_ref):
    for k in range(SPAN):
        start = tiles + k * ghosts
        first = frame[start : start + ghosts, 3, :]
        lane = lax.broadcasted_iota(I32, first.shape, 1)
        flag = jnp.where((first >= 0.0) & (lane == 0), 1.0, 0.0)
        used_ref[k] = jnp.sum(flag).astype(I32)


def scaled(rows, scale):
    half = rows[0:3] * 0.5
    norm = 0.5 - (half[0:1] * half[0:1] + half[1:2] * half[1:2] + half[2:3] * half[2:3])
    norm = jnp.where(rows[3:4] > 0.0, norm, -64.0) * scale
    return half, norm


def stream_features(rows, scale, slope):
    half, norm = scaled(rows, scale)
    high, mid, low = split(half + half)
    one = jnp.ones((1, TILE), F32)
    nh, nm, nl = split(norm)
    weight = jnp.maximum(rows[3:4], 0.0)
    wh, wm, _ = split(weight)
    if slope is None:
        tail = [wh, wm, jnp.zeros((6, TILE), F32)]
    else:
        sh, sm, _ = split(slope)
        tail = [wh, wm, wh, sh, sm, sh, jnp.zeros((2, TILE), F32)]
    parts = [high, one, high, one, high, one, mid, nm, low, nl, mid, nh] + tail
    return jnp.concatenate(parts, axis=0).astype(BF16)


def held_features(rows, scale):
    half, norm = scaled(rows, scale)
    high, mid, low = split(half * scale)
    nh, nm, nl = split(norm)
    one = jnp.ones((1, TILE), F32)
    parts = [high, nh, mid, nm, low, nl, high, one, high, one, mid, one, jnp.zeros((8, TILE), F32)]
    return jnp.concatenate(parts, axis=0).astype(BF16)


def row_mask(columns_of, width):
    row = lax.broadcasted_iota(I32, (FEATURES, width), 0)
    lane = lax.broadcasted_iota(I32, (FEATURES, width), 1) // TILE
    mask = jnp.zeros((FEATURES, width), jnp.bool_)
    for block, rows in enumerate(columns_of):
        for r in rows:
            mask = mask | ((row == r) & (lane == block))
    return jnp.where(mask, 1.0, 0.0).astype(BF16)


def fold(value):
    return value.reshape(TILE // 8, 8, TILE).sum(axis=0)


def each_pair(list_ref, chunks, use):
    def step(c, carry):
        for e in range(CHUNK):
            code = list_ref[c * CHUNK + e]
            use(lax.shift_right_logical(code, 7), code & (TILE - 1))
        return carry

    lax.fori_loop(0, chunks, step, 0)


def close_segment(list_ref, n, null):
    for e in range(CHUNK):
        list_ref[n + e] = null
    return (n + CHUNK - 1) // CHUNK


def list_kernel(frames, pair_tiles, pair_count, own_list, ghost_list, bounds):
    tiles, pairs = pair_tiles.shape

    def tile_step(t, found):
        n, m = found
        count = pair_count[t]
        codes = [pair_tiles[t, p] for p in range(pairs)]
        for p, f in enumerate(codes):
            code = t * TILE + f
            own_list[n] = code
            ghost_list[m] = code
            used = (p < count).astype(I32)
            near = jnp.where(f < tiles, used, 0)
            n = n + near
            m = m + used - near
        return n, m

    n, m = lax.fori_loop(0, tiles, tile_step, (0, 0))
    bounds[0] = close_segment(own_list, n, frames)
    bounds[1] = m


def density_terms(stream, held, acc_rho, acc_pair):
    def use(t, f):
        both = lax.dot_general(stream[f], held[t], CONTRACT_FIRST, preferred_element_type=F32)
        reach = jnp.maximum(both[:, :TILE], 0.0)
        square = reach * reach
        acc_rho[t] += fold(square * reach * both[:, TILE:])
        acc_pair[t] += fold(square * square)

    return use


def hold_for_density(tiles, frame, held):
    picks = row_mask([[24, 25]], TILE)
    for t in range(tiles):
        held[t, :, 0:TILE] = held_features(frame[t, 0:4], 1.0)
        held[t, :, TILE:] = picks


def own_density_kernel(
    own_list,
    bounds,
    pos_ref,
    chi_ref,
    occ_ref,
    rho_ref,
    pair_ref,
    frame,
    stream,
    held,
    acc_rho,
    acc_pair,
):
    tiles = chi_ref.shape[0]
    last = frame.shape[0] - 1
    load_own(pos_ref, chi_ref, occ_ref, frame)
    hold_for_density(tiles, frame, held)
    for f in range(tiles):
        stream[f] = stream_features(frame[f, 0:4], 1.0, None)
    stream[last] = stream_features(frame[last, 0:4], 1.0, None)
    acc_rho[...] = jnp.zeros_like(acc_rho)
    acc_pair[...] = jnp.zeros_like(acc_pair)
    each_pair(own_list, bounds[0], density_terms(stream, held, acc_rho, acc_pair))
    filled = occ_ref[...].astype(F32)
    rho_ref[...] = jnp.sum(acc_rho[...], axis=1) - filled * chi_ref[...]
    pair_ref[...] = jnp.sum(acc_pair[...], axis=1) - filled


def ghost_density_kernel(
    domains,
    me_ref,
    send_list,
    ghost_list,
    bounds,
    pos_ref,
    chi_ref,
    embed_ref,
    occ_ref,
    rho_ref,
    pair_ref,
    own_ref,
    cross_ref,
    slope_ref,
    energy_ref,
    out_ref,
    live_list,
    live_slots,
    live_bounds,
    frame,
    stream,
    held,
    acc_rho,
    acc_pair,
    used_ref,
    live_ref,
):
    me = me_ref[0]
    tiles = chi_ref.shape[0]
    ghosts = send_list.shape[1]
    frames = tiles + SPAN * ghosts
    load_own(pos_ref, chi_ref, occ_ref, frame)
    load_ghosts(me, domains, tiles, ghosts, own_ref, cross_ref, frame)
    live_counts(tiles, ghosts, frame, used_ref)
    hold_for_density(tiles, frame, held)
    for f in range(tiles, frames + 1):
        stream[f] = stream_features(frame[f, 0:4], 1.0, None)
    acc_rho[...] = jnp.zeros_like(acc_rho)
    acc_pair[...] = jnp.zeros_like(acc_pair)
    slots = 0
    for k in range(SPAN):
        used = used_ref[k]
        for g in range(ghosts):
            live = (g < used).astype(I32)
            live_ref[tiles + k * ghosts + g] = live
            live_slots[slots] = tiles + k * ghosts + g
            slots = slots + live
    for e in range(WIDE):
        live_slots[slots + e] = frames
    live_bounds[1] = (slots + WIDE - 1) // WIDE
    unroll = 8
    last = bounds[1]

    def filter_step(c, n):
        codes = [ghost_list[c * unroll + e] for e in range(unroll)]
        live = [live_ref[code & (TILE - 1)] for code in codes]
        for e in range(unroll):
            live_list[n] = codes[e]
            n = n + jnp.where(c * unroll + e < last, live[e], 0)
        return n

    n = lax.fori_loop(0, (last + unroll - 1) // unroll, filter_step, 0)
    chunks = close_segment(live_list, n, frames)
    live_bounds[0] = chunks
    each_pair(live_list, chunks, density_terms(stream, held, acc_rho, acc_pair))

    filled = occ_ref[...].astype(F32)
    embed = embed_ref[...]
    root = jnp.sqrt(1.0 + rho_ref[...] + jnp.sum(acc_rho[...], axis=1))
    slope = -0.5 * embed * filled / root
    slope_ref[...] = slope
    pair = pair_ref[...] + jnp.sum(acc_pair[...], axis=1)
    energy_ref[...] = filled * (0.5 * REPULSE * pair - embed * root)
    for k, offset in enumerate(OFFSETS):
        target = me - offset

        @pl.when((target >= 0) & (target < domains))
        def _(k=k, target=target):
            for g in range(ghosts):
                out_ref[target, g : g + 1] = slope_ref[pl.ds(send_list[k, g], 1)]


def hold_for_force(tiles, frame, slope_ref, held):
    ratio = 1.5 / (SCALE * SCALE)
    for t in range(tiles):
        frame[t, 4:5] = slope_ref[t : t + 1]
    for t in range(tiles):
        rows = frame[t, 0:4]
        held[t, :, 0:TILE] = held_features(rows, SCALE)
        sh, sm, _ = split(frame[t, 4:5] * ratio)
        wh, wm, _ = split(rows[3:4] * ratio)
        parts = [jnp.zeros((24, TILE), F32), sh, sh, sm, wh, wh, wm, jnp.zeros((2, TILE), F32)]
        held[t, :, TILE:] = jnp.concatenate(parts, axis=0).astype(BF16)


def stream_for_force(which, frame, stream):
    for f in which:
        rows = frame[f, 0:4]
        slope = jnp.where(rows[3:4] > 0.0, frame[f, 4:5], 0.0)
        stream[f] = stream_features(rows, SCALE, slope)


def widener(stream, wide):
    picks = row_mask([[c, 12 + c, 16 + c] for c in range(3)], 3 * TILE)

    def widen(f):
        three = lax.dot_general(stream[f], picks, CONTRACT_FIRST, preferred_element_type=F32)
        for c in range(3):
            wide[f, c] = three[:, c * TILE : (c + 1) * TILE]

    return widen


def widen_own(widen, tiles, last):
    def some(c, carry):
        for e in range(WIDE):
            widen(c * WIDE + e)
        return carry

    lax.fori_loop(0, tiles // WIDE, some, 0)
    widen(last)


def widen_ghosts(widen, slots_ref, chunks):
    def some(c, carry):
        for e in range(WIDE):
            widen(slots_ref[c * WIDE + e])
        return carry

    lax.fori_loop(0, chunks, some, 0)


def force_terms(stream, held, wide, acc):
    def use(t, f):
        both = lax.dot_general(stream[f], held[t], CONTRACT_FIRST, preferred_element_type=F32)
        reach = jnp.maximum(both[:, :TILE], 0.0)
        coef = reach * reach * (reach + both[:, TILE:])
        acc[t, 3] += fold(coef)
        for q in range(3):
            acc[t, q] += fold(coef * wide[f, q])

    return use


def load_slopes(me, domains, tiles, ghosts, ghost_slope_ref, frame):
    for k, offset in enumerate(OFFSETS):
        source = jnp.clip(me + offset, 0, domains - 1)
        for g in range(ghosts):
            frame[tiles + k * ghosts + g, 4:5] = ghost_slope_ref[source, g : g + 1]


def own_force_kernel(
    own_list, bounds, pos_ref, chi_ref, occ_ref, slope_ref, sums_ref, frame, stream, held, wide, acc
):
    tiles = chi_ref.shape[0]
    last = frame.shape[0] - 1
    load_own(pos_ref, chi_ref, occ_ref, frame)
    hold_for_force(tiles, frame, slope_ref, held)
    stream_for_force([*range(tiles), last], frame, stream)
    widen_own(widener(stream, wide), tiles, last)
    acc[...] = jnp.zeros_like(acc)
    each_pair(own_list, bounds[0], force_terms(stream, held, wide, acc))
    for q in range(4):
        sums_ref[q] = jnp.sum(acc[:, q], axis=1)


def ghost_force_kernel(
    domains,
    me_ref,
    dest_ref,
    live_list,
    live_slots,
    live_bounds,
    pos_ref,
    chi_ref,
    occ_ref,
    own_ref,
    cross_ref,
    slope_ref,
    ghost_slope_ref,
    sums_ref,
    force_ref,
    out_ref,
    frame,
    stream,
    held,
    wide,
    acc,
    total,
    rank_ref,
):
    me = me_ref[0]
    tiles = chi_ref.shape[0]
    ghosts = ghost_slope_ref.shape[1]
    frames = tiles + SPAN * ghosts
    load_own(pos_ref, chi_ref, occ_ref, frame)
    load_ghosts(me, domains, tiles, ghosts, own_ref, cross_ref, frame)
    load_slopes(me, domains, tiles, ghosts, ghost_slope_ref, frame)
    hold_for_force(tiles, frame, slope_ref, held)
    stream_for_force(range(tiles, frames + 1), frame, stream)
    widen = widener(stream, wide)
    widen_ghosts(widen, live_slots, live_bounds[1])
    widen(frames)
    acc[...] = jnp.zeros_like(acc)
    each_pair(live_list, live_bounds[0], force_terms(stream, held, wide, acc))
    for q in range(4):
        total[q] = sums_ref[q] + jnp.sum(acc[:, q], axis=1)
    for t in range(tiles):
        sums = jnp.concatenate([total[q, t : t + 1] for q in range(3)], axis=0)
        force_ref[:, t * TILE : (t + 1) * TILE] = frame[t, 0:3] * total[3, t : t + 1] - sums

    for r in range(2 * RADIUS + 1):
        rank_ref[r] = 0

    def move(t, carry):
        target = dest_ref[t]
        relative = target - me + RADIUS

        @pl.when(target != me)
        def _():
            rank = rank_ref[relative]
            rank_ref[relative] = rank + 1
            out_ref[target, pl.ds(4 * rank, 3)] = force_ref[:, columns(t)]

        return carry

    lax.fori_loop(0, tiles, move, 0)


def order_kernel(
    domains,
    ghosts,
    me_ref,
    dest_ref,
    pos_ref,
    vel_ref,
    occ_ref,
    own_ref,
    cross_ref,
    table_ref,
    origin_ref,
    count_ref,
    next_ref,
    held_ref,
    atoms_ref,
):
    me = me_ref[0]
    tiles = occ_ref.shape[0]
    base = 4 * ghosts
    held_ref[...] = occ_ref[...].astype(F32)
    next_ref[0] = 0
    atoms_ref[...] = jnp.zeros_like(atoms_ref)

    def from_other(source):
        @pl.when((source >= 0) & (source < domains))
        def _():
            def use(ref, at):
                first = jnp.concatenate(
                    [ref[at, base + 8 * m + 3 : base + 8 * m + 4, :] for m in range(MMAX)], axis=0
                )
                lane = lax.broadcasted_iota(I32, first.shape, 1)
                flag = jnp.where((first >= 0.0) & (lane == 0), 1.0, 0.0)
                count = jnp.sum(flag).astype(I32)
                slot = next_ref[0]
                next_ref[0] = slot + count
                for m in range(MMAX):

                    @pl.when(m < count)
                    def _(m=m):
                        rows = ref[at, base + 8 * m : base + 8 * m + 8]
                        table_ref[slot + m] = rows
                        origin_ref[slot + m] = source * MMAX + m
                        atoms_ref[...] += rows[3:4]

            arrived(me, source, own_ref, cross_ref, use)

    for offset in OFFSETS[:RADIUS]:
        from_other(me + offset)

    def stay(t, carry):
        @pl.when(dest_ref[t] == me)
        def _():
            slot = next_ref[0]
            next_ref[0] = slot + 1
            origin_ref[slot] = -1 - t
            filled = held_ref[pl.ds(t, 1)]
            table_ref[slot, 0:3] = pos_ref[:, columns(t)]
            table_ref[slot, 3:4] = filled
            table_ref[slot, 4:7] = vel_ref[:, columns(t)]
            atoms_ref[...] += filled

        return carry

    lax.fori_loop(0, tiles, stay, 0)
    for offset in OFFSETS[RADIUS:]:
        from_other(me + offset)
    origin_ref[origin_ref.shape[0] - 1] = next_ref[0]
    count_ref[0] = jnp.sum(atoms_ref[...]).astype(I32)


def finish_kernel(origin_ref, table_ref, force_ref, in_ref, moved_ref):
    capacity = table_ref.shape[0]
    used = origin_ref[origin_ref.shape[0] - 1]

    def step(e, carry):
        origin = origin_ref[e]
        rows = table_ref[e]

        def put(force):
            new_vel = rows[4:7] + TIME_STEP * force
            moved_ref[0:3, columns(e)] = rows[0:3] + TIME_STEP * new_vel
            moved_ref[3:6, columns(e)] = new_vel
            moved_ref[6:7, columns(e)] = rows[3:4]

        @pl.when(origin >= 0)
        def _():
            put(in_ref[origin // MMAX, pl.ds(4 * (origin % MMAX), 3)])

        @pl.when(origin < 0)
        def _():
            put(force_ref[:, columns(-1 - origin)])

        return carry

    lax.fori_loop(0, used, step, 0)

    def clear(e, carry):
        moved_ref[:, columns(e)] = jnp.zeros((7, TILE), F32)
        return carry

    lax.fori_loop(used, capacity, clear, 0)


def per_device(
    positions,
    velocity,
    density_weight,
    embed_strength,
    occupied,
    send_list,
    send_count,
    pair_tiles,
    pair_count,
    migrate_dest,
):
    domains = lax.axis_size("dom")
    tiles, pairs = pair_tiles.shape
    ghosts = send_list.shape[2]
    frames = tiles + SPAN * ghosts
    me = lax.axis_index("dom").astype(I32)[None]
    chi = density_weight.reshape(tiles, TILE)
    embed = embed_strength.reshape(tiles, TILE)
    occ = occupied.reshape(tiles, TILE)
    sends = send_list[0]
    sent = send_count[0]
    rows = 4 * ghosts + 8 * MMAX
    capacity = tiles + 2 * RADIUS * MMAX
    entries = tiles * pairs + 4 * CHUNK
    shape = jax.ShapeDtypeStruct
    scalars = shape((4,), I32)
    one_tile = shape((tiles, TILE), F32)

    def call(kernel, name, outs, in_specs, out_specs, scratch, args):
        return pl.pallas_call(
            kernel,
            out_shape=outs,
            in_specs=in_specs,
            out_specs=out_specs,
            scratch_shapes=scratch,
            compiler_params=PARAMS,
            name=name,
        )(*args)

    own, cross = call(
        functools.partial(pack_kernel, domains),
        "pack",
        [shape((GROUP, rows, TILE), F32)] * 2,
        [SMEM] * 4 + [VMEM] * 4,
        [VMEM] * 2,
        [
            pltpu.VMEM((tiles, 8, TILE), F32),
            pltpu.VMEM((tiles, 8, TILE), F32),
            pltpu.SMEM((2 * RADIUS + 1,), I32),
        ],
        (me, sends, sent, migrate_dest, positions, velocity, chi, occ),
    )
    blocks = [[b + i for i in range(GROUP)] for b in range(0, domains, GROUP)]
    crossing = [[(b + i - RADIUS) % domains for i in range(GROUP)] for b in range(0, domains, GROUP)]
    own = lax.all_to_all(own, "dom", 0, 0, axis_index_groups=blocks)
    own_list, ghost_list, bounds = call(
        functools.partial(list_kernel, frames),
        "lists",
        [shape((entries,), I32)] * 2 + [scalars],
        [SMEM] * 2,
        [SMEM] * 3,
        [],
        (pair_tiles, pair_count),
    )
    cross, own, bounds = lax.optimization_barrier((cross, own, bounds))
    cross = lax.all_to_all(cross, "dom", 0, 0, axis_index_groups=crossing)

    table = [
        pltpu.VMEM((frames + 1, 8, TILE), F32),
        pltpu.VMEM((frames + 1, FEATURES, TILE), BF16),
        pltpu.VMEM((tiles, FEATURES, 2 * TILE), BF16),
    ]
    density_sums = [pltpu.VMEM((tiles, 8, TILE), F32)] * 2
    rho, pair_sum = call(
        own_density_kernel,
        "own_density",
        [one_tile] * 2,
        [SMEM] * 2 + [VMEM] * 3,
        [VMEM] * 2,
        table + density_sums,
        (own_list, bounds, positions, chi, occ),
    )
    slope, energy, slope_out, live_list, live_slots, live_bounds = call(
        functools.partial(ghost_density_kernel, domains),
        "ghost_density",
        [one_tile, one_tile, shape((domains, ghosts, TILE), F32)]
        + [shape((entries,), I32), shape((SPAN * ghosts + 2 * WIDE,), I32), scalars],
        [SMEM] * 4 + [VMEM] * 8,
        [VMEM] * 3 + [SMEM] * 3,
        table + density_sums + [pltpu.SMEM((SPAN,), I32), pltpu.SMEM((TILE,), I32)],
        (me, sends, ghost_list, bounds, positions, chi, embed, occ, rho, pair_sum, own, cross),
    )
    slope_in = lax.all_to_all(slope_out, "dom", 0, 0)

    force_sums = [
        pltpu.VMEM((frames + 1, 3, TILE, TILE), F32),
        pltpu.VMEM((tiles, 4, 8, TILE), F32),
    ]
    total = [pltpu.VMEM((4, tiles, TILE), F32)]
    sums = call(
        own_force_kernel,
        "own_force",
        shape((4, tiles, TILE), F32),
        [SMEM] * 2 + [VMEM] * 4,
        VMEM,
        table + force_sums,
        (own_list, bounds, positions, chi, occ, slope),
    )
    force, force_out = call(
        functools.partial(ghost_force_kernel, domains),
        "ghost_force",
        [shape(positions.shape, F32), shape((domains, 4 * MMAX, TILE), F32)],
        [SMEM] * 5 + [VMEM] * 8,
        [VMEM] * 2,
        table + force_sums + total + [pltpu.SMEM((2 * RADIUS + 1,), I32)],
        (me, migrate_dest, live_list, live_slots, live_bounds)
        + (positions, chi, occ, own, cross, slope, slope_in, sums),
    )
    force_in = lax.all_to_all(force_out, "dom", 0, 0)

    ordered, origin, count = call(
        functools.partial(order_kernel, domains, ghosts),
        "order",
        [shape((capacity, 8, TILE), F32), shape((capacity + 1,), I32), shape((1,), I32)],
        [SMEM] * 2 + [VMEM] * 5,
        [VMEM, SMEM, SMEM],
        [pltpu.SMEM((1,), I32), pltpu.VMEM((tiles, TILE), F32), pltpu.VMEM((1, TILE), F32)],
        (me, migrate_dest, positions, velocity, occ, own, cross),
    )
    moved = call(
        finish_kernel,
        "finish",
        shape((7, capacity * TILE), F32),
        [SMEM] + [VMEM] * 3,
        VMEM,
        [],
        (origin, ordered, force, force_in),
    )
    return (force, energy.reshape(tiles * TILE), moved, count)


def solution(mesh):
    placed = (
        P(None, "dom"),
        P(None, "dom"),
        P("dom"),
        P("dom"),
        P("dom"),
        P("dom", None, None),
        P("dom", None),
        P("dom", None),
        P("dom"),
        P("dom"),
    )
    return jax.shard_map(
        per_device,
        mesh=mesh,
        in_specs=placed,
        out_specs=(P(None, "dom"), P("dom"), P(None, "dom"), P("dom")),
        check_vma=False,
    )
```

```python
import functools

import jax
import jax.numpy as jnp
from jax import lax
from jax.experimental import pallas as pl
from jax.experimental.pallas import tpu as pltpu
from jax.sharding import PartitionSpec as P

TILE = 128
RADIUS = 4
MMAX = 4
REPULSE = 0.05
TIME_STEP = 0.05
SPAN = 2 * RADIUS
GROUP = 2 * RADIUS
F32 = jnp.float32
BF16 = jnp.bfloat16
I32 = jnp.int32
LARGE = 48
CHUNK = 16
WIDE = 8
FEATURES = 32
SCALE = 0.1 ** (1.0 / 3.0)
OFFSETS = [k - RADIUS for k in range(RADIUS)] + [k + 1 for k in range(RADIUS)]
CONTRACT_FIRST = (((0,), (0,)), ((), ()))

VMEM = pl.BlockSpec(memory_space=pltpu.VMEM)
SMEM = pl.BlockSpec(memory_space=pltpu.SMEM)
PARAMS = pltpu.CompilerParams(vmem_limit_bytes=28 * 1024 * 1024)


def columns(tile):
    return pl.ds(pl.multiple_of(tile * TILE, TILE), TILE)


def split(value):
    high = value.astype(BF16).astype(F32)
    rest = value - high
    mid = rest.astype(BF16).astype(F32)
    return high, mid, rest - mid


def pack_kernel(
    domains,
    me_ref,
    send_list,
    send_count,
    dest_ref,
    pos_ref,
    vel_ref,
    chi_ref,
    occ_ref,
    own_ref,
    cross_ref,
    ghost_row,
    move_row,
    rank_ref,
):
    me = me_ref[0]
    tiles = chi_ref.shape[0]
    ghosts = send_list.shape[1]
    base = 4 * ghosts
    filled = occ_ref[...].astype(F32)
    weight = chi_ref[...] * filled
    for t in range(tiles):
        span = slice(t * TILE, (t + 1) * TILE)
        ghost_row[t, 0:3] = pos_ref[:, span]
        ghost_row[t, 3:4] = weight[t : t + 1]
        move_row[t, 0:3] = pos_ref[:, span]
        move_row[t, 3:4] = filled[t : t + 1]
        move_row[t, 4:7] = vel_ref[:, span]
    nothing = jnp.full((1, TILE), -1.0, F32)

    def place(target, rows):
        inside = (target // GROUP) == (me // GROUP)

        @pl.when(inside)
        def _():
            rows(own_ref, target % GROUP)

        @pl.when(jnp.logical_not(inside))
        def _():
            rows(cross_ref, (target + RADIUS) % GROUP)

    for k, offset in enumerate(OFFSETS):
        target = me - offset

        @pl.when((target >= 0) & (target < domains))
        def _(k=k, target=target):
            used = send_count[k]

            def rows(out_ref, at):
                for g in range(ghosts):
                    block = ghost_row[send_list[k, g]]
                    live = g < used
                    out_ref[at, 4 * g : 4 * g + 3] = block[0:3]
                    out_ref[at, 4 * g + 3 : 4 * g + 4] = jnp.where(live, block[3:4], nothing)
                for m in range(MMAX):
                    out_ref[at, base + 8 * m + 3 : base + 8 * m + 4] = nothing

            place(target, rows)

    for r in range(2 * RADIUS + 1):
        rank_ref[r] = 0

    def move(t, carry):
        target = dest_ref[t]
        relative = target - me + RADIUS

        @pl.when(target != me)
        def _():
            rank = rank_ref[relative]
            rank_ref[relative] = rank + 1

            def rows(out_ref, at):
                out_ref[at, pl.ds(pl.multiple_of(base + 8 * rank, 8), 8)] = move_row[t]

            place(target, rows)

        return carry

    lax.fori_loop(0, tiles, move, 0)


def arrived(me, source, own_ref, cross_ref, use):
    inside = (source // GROUP) == (me // GROUP)

    @pl.when(inside)
    def _():
        use(own_ref, source % GROUP)

    @pl.when(jnp.logical_not(inside))
    def _():
        use(cross_ref, (source + RADIUS) % GROUP)


def load_own(base_ref, frame):
    tiles = base_ref.shape[0]
    last = frame.shape[0] - 1
    frame[0:tiles] = base_ref[...]
    frame[last, 0:4] = jnp.full((4, TILE), -1.0, F32)


def load_ghosts(me, domains, tiles, ghosts, own_ref, cross_ref, frame):
    for k, offset in enumerate(OFFSETS):
        source = me + offset
        start = tiles + k * ghosts
        valid = (source >= 0) & (source < domains)

        @pl.when(valid)
        def _(start=start, source=source):
            def use(ref, at):
                for g in range(ghosts):
                    frame[start + g, 0:4] = ref[at, 4 * g : 4 * g + 4]

            arrived(me, source, own_ref, cross_ref, use)

        @pl.when(jnp.logical_not(valid))
        def _(start=start):
            for g in range(ghosts):
                frame[start + g, 0:4] = jnp.full((4, TILE), -1.0, F32)


def live_counts(tiles, ghosts, frame, used_ref):
    for k in range(SPAN):
        start = tiles + k * ghosts
        first = frame[start : start + ghosts, 3, :]
        lane = lax.broadcasted_iota(I32, first.shape, 1)
        flag = jnp.where((first >= 0.0) & (lane == 0), 1.0, 0.0)
        used_ref[k] = jnp.sum(flag).astype(I32)


def scaled(rows, scale):
    half = rows[0:3] * 0.5
    norm = 0.5 - (half[0:1] * half[0:1] + half[1:2] * half[1:2] + half[2:3] * half[2:3])
    norm = jnp.where(rows[3:4] > 0.0, norm, -64.0) * scale
    return half, norm


def stream_features(rows, scale, slope):
    half, norm = scaled(rows, scale)
    high, mid, low = split(half + half)
    one = jnp.ones((1, TILE), F32)
    nh, nm, nl = split(norm)
    weight = jnp.maximum(rows[3:4], 0.0)
    wh, wm, _ = split(weight)
    if slope is None:
        tail = [wh, wm, jnp.zeros((6, TILE), F32)]
    else:
        sh, sm, _ = split(slope)
        tail = [wh, wm, wh, sh, sm, sh, jnp.zeros((2, TILE), F32)]
    parts = [high, one, high, one, high, one, mid, nm, low, nl, mid, nh] + tail
    return jnp.concatenate(parts, axis=0).astype(BF16)


def held_features(rows, scale):
    half, norm = scaled(rows, scale)
    high, mid, low = split(half * scale)
    nh, nm, nl = split(norm)
    one = jnp.ones((1, TILE), F32)
    parts = [high, nh, mid, nm, low, nl, high, one, high, one, mid, one, jnp.zeros((8, TILE), F32)]
    return jnp.concatenate(parts, axis=0).astype(BF16)


def row_mask(columns_of, width):
    row = lax.broadcasted_iota(I32, (FEATURES, width), 0)
    lane = lax.broadcasted_iota(I32, (FEATURES, width), 1) // TILE
    mask = jnp.zeros((FEATURES, width), jnp.bool_)
    for block, rows in enumerate(columns_of):
        for r in rows:
            mask = mask | ((row == r) & (lane == block))
    return jnp.where(mask, 1.0, 0.0).astype(BF16)


def fold(value):
    return value.reshape(TILE // 8, 8, TILE).sum(axis=0)


def each_pair(list_ref, chunks, use):
    def group(start, size):
        for e in range(size):
            code = list_ref[start + e]
            use(lax.shift_right_logical(code, 7), code & (TILE - 1))

    def large(c, carry):
        group(c * LARGE, LARGE)
        return carry

    def small(c, carry):
        group(c * CHUNK, CHUNK)
        return carry

    many = chunks * CHUNK // LARGE
    lax.fori_loop(0, many, large, 0)
    lax.fori_loop(many * (LARGE // CHUNK), chunks, small, 0)


def close_segment(list_ref, n, null):
    for e in range(CHUNK):
        list_ref[n + e] = null
    return (n + CHUNK - 1) // CHUNK


def list_kernel(frames, pair_tiles, pair_count, own_list, ghost_list, bounds):
    pairs, tiles = pair_tiles.shape

    def tile_step(t, found):
        n, m = found
        count = pair_count[t]
        codes = [pair_tiles[p, t] for p in range(pairs)]
        for p, f in enumerate(codes):
            code = t * TILE + f
            own_list[n] = code
            ghost_list[m] = code
            used = (p < count).astype(I32)
            near = jnp.where(f < tiles, used, 0)
            n = n + near
            m = m + used - near
        return n, m

    n, m = lax.fori_loop(0, tiles, tile_step, (0, 0))
    bounds[0] = close_segment(own_list, n, frames)
    bounds[1] = m


def density_terms(stream, held, acc_rho, acc_pair):
    def use(t, f):
        both = lax.dot_general(stream[f], held[t], CONTRACT_FIRST, preferred_element_type=F32)
        reach = jnp.maximum(both[:, :TILE], 0.0)
        square = reach * reach
        acc_rho[t] += fold(square * reach * both[:, TILE:])
        acc_pair[t] += fold(square * square)

    return use


def hold_for_density(tiles, frame, held):
    picks = row_mask([[24, 25]], TILE)
    for t in range(tiles):
        held[t, :, 0:TILE] = held_features(frame[t, 0:4], 1.0)
        held[t, :, TILE:] = picks


def own_density_kernel(
    own_list, bounds, base_ref, occ_ref, rho_ref, pair_ref, held, frame, stream, acc_rho, acc_pair
):
    tiles = occ_ref.shape[0]
    last = frame.shape[0] - 1
    load_own(base_ref, frame)
    hold_for_density(tiles, frame, held)
    for f in range(tiles):
        stream[f] = stream_features(frame[f, 0:4], 1.0, None)
    stream[last] = stream_features(frame[last, 0:4], 1.0, None)
    acc_rho[...] = jnp.zeros_like(acc_rho)
    acc_pair[...] = jnp.zeros_like(acc_pair)
    each_pair(own_list, bounds[0], density_terms(stream, held, acc_rho, acc_pair))
    for t in range(tiles):
        rho_ref[t : t + 1] = frame[t, 3:4]
    rho_ref[...] = jnp.sum(acc_rho[...], axis=1) - rho_ref[...]
    pair_ref[...] = jnp.sum(acc_pair[...], axis=1) - occ_ref[...].astype(F32)


def ghost_density_kernel(
    domains,
    me_ref,
    send_list,
    ghost_list,
    bounds,
    base_ref,
    embed_ref,
    occ_ref,
    rho_ref,
    pair_ref,
    held,
    own_ref,
    cross_ref,
    slope_ref,
    energy_ref,
    out_ref,
    frame,
    live_list,
    live_slots,
    live_bounds,
    stream,
    acc_rho,
    acc_pair,
    used_ref,
    live_ref,
):
    me = me_ref[0]
    tiles = occ_ref.shape[0]
    ghosts = send_list.shape[1]
    frames = tiles + SPAN * ghosts
    load_own(base_ref, frame)
    load_ghosts(me, domains, tiles, ghosts, own_ref, cross_ref, frame)
    live_counts(tiles, ghosts, frame, used_ref)
    stream[frames] = stream_features(frame[frames, 0:4], 1.0, None)
    acc_rho[...] = jnp.zeros_like(acc_rho)
    acc_pair[...] = jnp.zeros_like(acc_pair)
    slots = 0
    for k in range(SPAN):
        used = used_ref[k]
        for g in range(ghosts):
            live = (g < used).astype(I32)
            live_ref[tiles + k * ghosts + g] = live
            live_slots[slots] = tiles + k * ghosts + g
            slots = slots + live
    for e in range(WIDE):
        live_slots[slots + e] = frames
    live_bounds[1] = (slots + WIDE - 1) // WIDE
    unroll = 8
    last = bounds[1]

    count = frames - tiles

    def filter_step(c, n):
        codes = [ghost_list[c * unroll + e] for e in range(unroll)]
        live = [live_ref[code & (TILE - 1)] for code in codes]
        for e in range(unroll):
            live_list[n] = codes[e]
            n = n + jnp.where(c * unroll + e < last, live[e], 0)
        for e in range(2):
            f = tiles + jnp.minimum(2 * c + e, count - 1)
            stream[f] = stream_features(frame[f, 0:4], 1.0, None)
        return n

    steps = jnp.maximum((last + unroll - 1) // unroll, (count + 1) // 2)
    n = lax.fori_loop(0, steps, filter_step, 0)
    chunks = close_segment(live_list, n, frames)
    live_bounds[0] = chunks
    each_pair(live_list, chunks, density_terms(stream, held, acc_rho, acc_pair))

    filled = occ_ref[...].astype(F32)
    embed = embed_ref[...]
    root = jnp.sqrt(1.0 + rho_ref[...] + jnp.sum(acc_rho[...], axis=1))
    slope = -0.5 * embed * filled / root
    slope_ref[...] = slope
    pair = pair_ref[...] + jnp.sum(acc_pair[...], axis=1)
    energy_ref[...] = filled * (0.5 * REPULSE * pair - embed * root)
    for k, offset in enumerate(OFFSETS):
        target = me - offset

        @pl.when((target >= 0) & (target < domains))
        def _(k=k, target=target):
            for g in range(ghosts):
                out_ref[target, g : g + 1] = slope_ref[pl.ds(send_list[k, g], 1)]


def hold_for_force(tiles, frame, slope_ref, slopes, held):
    ratio = 1.5 / (SCALE * SCALE)
    for t in range(tiles):
        slopes[t] = slope_ref[t : t + 1]
    for t in range(tiles):
        rows = frame[t, 0:4]
        held[t, :, 0:TILE] = held_features(rows, SCALE)
        sh, sm, _ = split(slopes[t] * ratio)
        wh, wm, _ = split(rows[3:4] * ratio)
        parts = [jnp.zeros((24, TILE), F32), sh, sh, sm, wh, wh, wm, jnp.zeros((2, TILE), F32)]
        held[t, :, TILE:] = jnp.concatenate(parts, axis=0).astype(BF16)


def stream_for_force(which, frame, slopes, stream):
    for f in which:
        rows = frame[f, 0:4]
        slope = jnp.where(rows[3:4] > 0.0, slopes[f], 0.0)
        stream[f] = stream_features(rows, SCALE, slope)


def widener(stream, wide):
    picks = row_mask([[c, 12 + c, 16 + c] for c in range(3)], 3 * TILE)

    def widen(f):
        three = lax.dot_general(stream[f], picks, CONTRACT_FIRST, preferred_element_type=F32)
        for c in range(3):
            wide[f, c] = three[:, c * TILE : (c + 1) * TILE]

    return widen


def widen_own(widen, tiles, last):
    def some(c, carry):
        for e in range(WIDE):
            widen(c * WIDE + e)
        return carry

    lax.fori_loop(0, tiles // WIDE, some, 0)
    widen(last)


def widen_ghosts(widen, slots_ref, chunks):
    def some(c, carry):
        for e in range(WIDE):
            widen(slots_ref[c * WIDE + e])
        return carry

    lax.fori_loop(0, chunks, some, 0)


def force_terms(stream, held, wide, acc):
    def use(t, f):
        both = lax.dot_general(stream[f], held[t], CONTRACT_FIRST, preferred_element_type=F32)
        reach = jnp.maximum(both[:, :TILE], 0.0)
        coef = reach * reach * (reach + both[:, TILE:])
        acc[t, 3] += fold(coef)
        for q in range(3):
            acc[t, q] += fold(coef * wide[f, q])

    return use


def load_slopes(me, domains, tiles, ghosts, ghost_slope_ref, slopes):
    for k, offset in enumerate(OFFSETS):
        source = jnp.clip(me + offset, 0, domains - 1)
        for g in range(ghosts):
            slopes[tiles + k * ghosts + g] = ghost_slope_ref[source, g : g + 1]


def own_force_kernel(own_list, bounds, base_ref, slope_ref, sums_ref, held, frame, slopes, stream, wide, acc):
    tiles = base_ref.shape[0]
    last = frame.shape[0] - 1
    load_own(base_ref, frame)
    slopes[last] = jnp.zeros((1, TILE), F32)
    hold_for_force(tiles, frame, slope_ref, slopes, held)
    stream_for_force([*range(tiles), last], frame, slopes, stream)
    widen_own(widener(stream, wide), tiles, last)
    acc[...] = jnp.zeros_like(acc)
    each_pair(own_list, bounds[0], force_terms(stream, held, wide, acc))
    for q in range(4):
        sums_ref[q] = jnp.sum(acc[:, q], axis=1)


def ghost_force_kernel(
    domains,
    me_ref,
    dest_ref,
    live_list,
    live_slots,
    live_bounds,
    frame,
    held,
    ghost_slope_ref,
    sums_ref,
    force_ref,
    out_ref,
    slopes,
    stream,
    wide,
    acc,
    total,
    rank_ref,
):
    me = me_ref[0]
    tiles = held.shape[0]
    ghosts = ghost_slope_ref.shape[1]
    frames = tiles + SPAN * ghosts
    load_slopes(me, domains, tiles, ghosts, ghost_slope_ref, slopes)
    slopes[frames] = jnp.zeros((1, TILE), F32)
    stream_for_force(range(tiles, frames + 1), frame, slopes, stream)
    widen = widener(stream, wide)
    widen_ghosts(widen, live_slots, live_bounds[1])
    widen(frames)
    acc[...] = jnp.zeros_like(acc)
    each_pair(live_list, live_bounds[0], force_terms(stream, held, wide, acc))
    for q in range(4):
        total[q] = sums_ref[q] + jnp.sum(acc[:, q], axis=1)
    for t in range(tiles):
        sums = jnp.concatenate([total[q, t : t + 1] for q in range(3)], axis=0)
        force_ref[:, t * TILE : (t + 1) * TILE] = frame[t, 0:3] * total[3, t : t + 1] - sums

    for r in range(2 * RADIUS + 1):
        rank_ref[r] = 0

    def move(t, carry):
        target = dest_ref[t]
        relative = target - me + RADIUS

        @pl.when(target != me)
        def _():
            rank = rank_ref[relative]
            rank_ref[relative] = rank + 1
            out_ref[target, pl.ds(4 * rank, 3)] = force_ref[:, columns(t)]

        return carry

    lax.fori_loop(0, tiles, move, 0)


def order_kernel(
    domains,
    ghosts,
    me_ref,
    dest_ref,
    move_row,
    own_ref,
    cross_ref,
    table_ref,
    origin_ref,
    count_ref,
    next_ref,
    atoms_ref,
):
    me = me_ref[0]
    tiles = move_row.shape[0]
    base = 4 * ghosts
    next_ref[0] = 0
    atoms_ref[...] = jnp.zeros_like(atoms_ref)

    def from_other(source):
        @pl.when((source >= 0) & (source < domains))
        def _():
            def use(ref, at):
                first = jnp.concatenate(
                    [ref[at, base + 8 * m + 3 : base + 8 * m + 4, :] for m in range(MMAX)], axis=0
                )
                lane = lax.broadcasted_iota(I32, first.shape, 1)
                flag = jnp.where((first >= 0.0) & (lane == 0), 1.0, 0.0)
                count = jnp.sum(flag).astype(I32)
                slot = next_ref[0]
                next_ref[0] = slot + count
                for m in range(MMAX):

                    @pl.when(m < count)
                    def _(m=m):
                        rows = ref[at, base + 8 * m : base + 8 * m + 8]
                        table_ref[slot + m] = rows
                        origin_ref[slot + m] = source * MMAX + m
                        atoms_ref[...] += rows[3:4]

            arrived(me, source, own_ref, cross_ref, use)

    for offset in OFFSETS[:RADIUS]:
        from_other(me + offset)

    def stay(t, carry):
        @pl.when(dest_ref[t] == me)
        def _():
            slot = next_ref[0]
            next_ref[0] = slot + 1
            origin_ref[slot] = -1 - t
            rows = move_row[t]
            table_ref[slot] = rows
            atoms_ref[...] += rows[3:4]

        return carry

    lax.fori_loop(0, tiles, stay, 0)
    for offset in OFFSETS[RADIUS:]:
        from_other(me + offset)
    origin_ref[origin_ref.shape[0] - 1] = next_ref[0]
    count_ref[0] = jnp.sum(atoms_ref[...]).astype(I32)


def finish_kernel(origin_ref, table_ref, force_ref, in_ref, moved_ref):
    capacity = table_ref.shape[0]
    used = origin_ref[origin_ref.shape[0] - 1]

    def step(e, carry):
        origin = origin_ref[e]
        rows = table_ref[e]

        def put(force):
            new_vel = rows[4:7] + TIME_STEP * force
            moved_ref[0:3, columns(e)] = rows[0:3] + TIME_STEP * new_vel
            moved_ref[3:6, columns(e)] = new_vel
            moved_ref[6:7, columns(e)] = rows[3:4]

        @pl.when(origin >= 0)
        def _():
            put(in_ref[origin // MMAX, pl.ds(4 * (origin % MMAX), 3)])

        @pl.when(origin < 0)
        def _():
            put(force_ref[:, columns(-1 - origin)])

        return carry

    lax.fori_loop(0, used, step, 0)

    def clear(e, carry):
        moved_ref[:, columns(e)] = jnp.zeros((7, TILE), F32)
        return carry

    lax.fori_loop(used, capacity, clear, 0)


def per_device(
    positions,
    velocity,
    density_weight,
    embed_strength,
    occupied,
    send_list,
    send_count,
    pair_tiles,
    pair_count,
    migrate_dest,
):
    domains = lax.axis_size("dom")
    tiles, pairs = pair_tiles.shape
    ghosts = send_list.shape[2]
    frames = tiles + SPAN * ghosts
    me = lax.axis_index("dom").astype(I32)[None]
    chi = density_weight.reshape(tiles, TILE)
    embed = embed_strength.reshape(tiles, TILE)
    occ = occupied.reshape(tiles, TILE)
    sends = send_list[0]
    sent = send_count[0]
    pair_rows = pair_tiles.T
    inputs = (me, positions, velocity, chi, embed, occ, sends, sent, pair_rows, pair_count, migrate_dest)
    rows = 4 * ghosts + 8 * MMAX
    capacity = tiles + 2 * RADIUS * MMAX
    entries = tiles * pairs + 4 * CHUNK
    shape = jax.ShapeDtypeStruct
    scalars = shape((4,), I32)
    one_tile = shape((tiles, TILE), F32)

    def call(kernel, name, outs, in_specs, out_specs, scratch, args, final=(), keep=True):
        single = not isinstance(outs, list)
        outs = [outs] if single else outs
        out_specs = [out_specs] if single else out_specs
        outs = [
            (pltpu.VMEM if spec is VMEM else pltpu.SMEM)(out.shape, out.dtype) if i not in final else out
            for i, (out, spec) in enumerate(zip(outs, out_specs))
        ]
        args = [
            pltpu.with_memory_space_constraint(arg, pltpu.VMEM)
            if spec is VMEM and keep
            else pltpu.with_memory_space_constraint(arg, pltpu.HBM)
            if any(arg is given for given in inputs)
            else pltpu.with_memory_space_constraint(arg, pltpu.SMEM)
            for arg, spec in zip(args, in_specs)
        ]
        results = pl.pallas_call(
            kernel,
            out_shape=outs,
            in_specs=in_specs,
            out_specs=out_specs,
            scratch_shapes=scratch,
            compiler_params=PARAMS,
            name=name,
        )(*args)
        return results[0] if single else results

    own, cross, base, move_row = call(
        functools.partial(pack_kernel, domains),
        "pack",
        [shape((GROUP, rows, TILE), F32)] * 2 + [shape((tiles, 8, TILE), F32)] * 2,
        [SMEM] * 4 + [VMEM] * 4,
        [VMEM] * 4,
        [pltpu.SMEM((2 * RADIUS + 1,), I32)],
        (me, sends, sent, migrate_dest, positions, velocity, chi, occ),
        keep=False,
    )
    blocks = [[b + i for i in range(GROUP)] for b in range(0, domains, GROUP)]
    crossing = [[(b + i - RADIUS) % domains for i in range(GROUP)] for b in range(0, domains, GROUP)]
    own = lax.all_to_all(own, "dom", 0, 0, axis_index_groups=blocks)
    own_list, ghost_list, bounds = call(
        functools.partial(list_kernel, frames),
        "lists",
        [shape((entries,), I32)] * 2 + [scalars],
        [SMEM] * 2,
        [SMEM] * 3,
        [],
        (pair_rows, pair_count),
    )
    cross, own, bounds = lax.optimization_barrier((cross, own, bounds))
    cross = lax.all_to_all(cross, "dom", 0, 0, axis_index_groups=crossing)

    frame = pltpu.VMEM((frames + 1, 8, TILE), F32)
    stream = pltpu.VMEM((frames + 1, FEATURES, TILE), BF16)
    slopes = pltpu.VMEM((frames + 1, 1, TILE), F32)
    density_sums = [pltpu.VMEM((tiles, 8, TILE), F32)] * 2
    held_shape = shape((tiles, FEATURES, 2 * TILE), BF16)
    rho, pair_sum, held = call(
        own_density_kernel,
        "own_density",
        [one_tile] * 2 + [held_shape],
        [SMEM] * 2 + [VMEM] * 2,
        [VMEM] * 3,
        [frame, stream] + density_sums,
        (own_list, bounds, base, occ),
    )
    slope, energy, slope_out, frame_rows, live_list, live_slots, live_bounds = call(
        functools.partial(ghost_density_kernel, domains),
        "ghost_density",
        [one_tile, one_tile, shape((domains, ghosts, TILE), F32), shape((frames + 1, 8, TILE), F32)]
        + [shape((entries,), I32), shape((SPAN * ghosts + 2 * WIDE,), I32), scalars],
        [SMEM] * 4 + [VMEM] * 8,
        [VMEM] * 4 + [SMEM] * 3,
        [stream] + density_sums + [pltpu.SMEM((SPAN,), I32), pltpu.SMEM((TILE,), I32)],
        (me, sends, ghost_list, bounds, base, embed, occ, rho, pair_sum, held, own, cross),
        final=(1,),
    )
    slope_in = lax.all_to_all(slope_out, "dom", 0, 0)

    force_sums = [
        stream,
        pltpu.VMEM((frames + 1, 3, TILE, TILE), F32),
        pltpu.VMEM((tiles, 4, 8, TILE), F32),
    ]
    sums, held = call(
        own_force_kernel,
        "own_force",
        [shape((4, tiles, TILE), F32), held_shape],
        [SMEM] * 2 + [VMEM] * 2,
        [VMEM] * 2,
        [frame, slopes] + force_sums,
        (own_list, bounds, base, slope),
    )
    force, force_out = call(
        functools.partial(ghost_force_kernel, domains),
        "ghost_force",
        [shape(positions.shape, F32), shape((domains, 4 * MMAX, TILE), F32)],
        [SMEM] * 5 + [VMEM] * 4,
        [VMEM] * 2,
        [slopes] + force_sums + [pltpu.VMEM((4, tiles, TILE), F32), pltpu.SMEM((2 * RADIUS + 1,), I32)],
        (me, migrate_dest, live_list, live_slots, live_bounds, frame_rows, held, slope_in, sums),
        final=(0,),
    )
    force_in = lax.all_to_all(force_out, "dom", 0, 0)

    ordered, origin, count = call(
        functools.partial(order_kernel, domains, ghosts),
        "order",
        [shape((capacity, 8, TILE), F32), shape((capacity + 1,), I32), shape((1,), I32)],
        [SMEM] * 2 + [VMEM] * 3,
        [VMEM, SMEM, SMEM],
        [pltpu.SMEM((1,), I32), pltpu.VMEM((1, TILE), F32)],
        (me, migrate_dest, move_row, own, cross),
        final=(2,),
    )
    moved = call(
        finish_kernel,
        "finish",
        shape((7, capacity * TILE), F32),
        [SMEM] + [VMEM] * 3,
        VMEM,
        [],
        (origin, ordered, force, force_in),
        final=(0,),
    )
    return (force, energy.reshape(tiles * TILE), moved, count)


def solution(mesh):
    placed = (
        P(None, "dom"),
        P(None, "dom"),
        P("dom"),
        P("dom"),
        P("dom"),
        P("dom", None, None),
        P("dom", None),
        P("dom", None),
        P("dom"),
        P("dom"),
    )
    return jax.shard_map(
        per_device,
        mesh=mesh,
        in_specs=placed,
        out_specs=(P(None, "dom"), P("dom"), P(None, "dom"), P("dom")),
        check_vma=False,
    )
```

```python
import functools
import math

import jax
import jax.numpy as jnp
from jax import lax
from jax.experimental import pallas as pl
from jax.experimental.pallas import tpu as pltpu
from jax.sharding import PartitionSpec as P

TILE = 128
RADIUS = 4
MMAX = 4
REPULSE = 0.05
TIME_STEP = 0.05
SPAN = 2 * RADIUS
GROUP = 2 * RADIUS
F32 = jnp.float32
BF16 = jnp.bfloat16
I32 = jnp.int32
LARGE = 48
CHUNK = 16
WIDE = 8
FEATURES = 32
SCALE = 0.1 ** (1.0 / 3.0)
OFFSETS = [k - RADIUS for k in range(RADIUS)] + [k + 1 for k in range(RADIUS)]
CONTRACT_FIRST = (((0,), (0,)), ((), ()))

VMEM = pl.BlockSpec(memory_space=pltpu.VMEM)
SMEM = pl.BlockSpec(memory_space=pltpu.SMEM)
MIB = 1024 * 1024


def columns(tile):
    return pl.ds(pl.multiple_of(tile * TILE, TILE), TILE)


def split(value):
    high = value.astype(BF16).astype(F32)
    rest = value - high
    mid = rest.astype(BF16).astype(F32)
    return high, mid, rest - mid


def pack_kernel(
    domains,
    me_ref,
    send_list,
    send_count,
    dest_ref,
    pos_ref,
    vel_ref,
    chi_ref,
    occ_ref,
    own_ref,
    cross_ref,
    ghost_row,
    move_row,
    place_ref,
    rank_ref,
):
    me = me_ref[0]
    tiles = chi_ref.shape[0]
    ghosts = send_list.shape[1]
    base = 4 * ghosts
    filled = occ_ref[...].astype(F32)
    weight = chi_ref[...] * filled
    for t in range(tiles):
        span = slice(t * TILE, (t + 1) * TILE)
        ghost_row[t, 0:3] = pos_ref[:, span]
        ghost_row[t, 3:4] = weight[t : t + 1]
        move_row[t, 0:3] = pos_ref[:, span]
        move_row[t, 3:4] = filled[t : t + 1]
        move_row[t, 4:7] = vel_ref[:, span]
    nothing = jnp.full((1, TILE), -1.0, F32)

    def place(target, rows):
        inside = (target // GROUP) == (me // GROUP)

        @pl.when(inside)
        def _():
            rows(own_ref, target % GROUP)

        @pl.when(jnp.logical_not(inside))
        def _():
            rows(cross_ref, (target + RADIUS) % GROUP)

    for k, offset in enumerate(OFFSETS):
        target = me - offset

        @pl.when((target >= 0) & (target < domains))
        def _(k=k, target=target):
            used = send_count[k]

            def rows(out_ref, at):
                for g in range(ghosts):
                    block = ghost_row[send_list[k, g]]
                    live = g < used
                    out_ref[at, 4 * g : 4 * g + 3] = block[0:3]
                    out_ref[at, 4 * g + 3 : 4 * g + 4] = jnp.where(live, block[3:4], nothing)
                for m in range(MMAX):
                    out_ref[at, base + 8 * m + 3 : base + 8 * m + 4] = nothing

            place(target, rows)

    for r in range(2 * RADIUS + 1):
        rank_ref[r] = 0

    for t in range(tiles):
        target = dest_ref[t]
        relative = target - me + RADIUS
        rank = rank_ref[relative]
        rank_ref[relative] = rank + 1
        rank = jnp.minimum(rank, MMAX - 1)
        place_ref[t] = rank
        inside = lax.div(target, GROUP) == lax.div(me, GROUP)
        row = pl.ds(pl.multiple_of(base + 8 * rank, 8), 8)
        own_ref[lax.rem(jnp.where(inside, target, me), GROUP), row] = move_row[t]
        cross_ref[lax.rem(jnp.where(inside, me, target) + RADIUS, GROUP), row] = move_row[t]


def arrived(me, source, own_ref, cross_ref, use):
    inside = (source // GROUP) == (me // GROUP)

    @pl.when(inside)
    def _():
        use(own_ref, source % GROUP)

    @pl.when(jnp.logical_not(inside))
    def _():
        use(cross_ref, (source + RADIUS) % GROUP)


def load_own(base_ref, frame):
    tiles = base_ref.shape[0]
    last = frame.shape[0] - 1
    frame[0:tiles] = base_ref[...]
    frame[last, 0:4] = jnp.full((4, TILE), -1.0, F32)


def load_ghosts(me, domains, tiles, ghosts, own_ref, cross_ref, frame):
    for k, offset in enumerate(OFFSETS):
        source = me + offset
        start = tiles + k * ghosts
        valid = (source >= 0) & (source < domains)

        @pl.when(valid)
        def _(start=start, source=source):
            def use(ref, at):
                for g in range(ghosts):
                    frame[start + g, 0:4] = ref[at, 4 * g : 4 * g + 4]

            arrived(me, source, own_ref, cross_ref, use)

        @pl.when(jnp.logical_not(valid))
        def _(start=start):
            for g in range(ghosts):
                frame[start + g, 0:4] = jnp.full((4, TILE), -1.0, F32)


def live_counts(tiles, ghosts, frame, used_ref):
    for k in range(SPAN):
        start = tiles + k * ghosts
        first = frame[start : start + ghosts, 3, :]
        lane = lax.broadcasted_iota(I32, first.shape, 1)
        flag = jnp.where((first >= 0.0) & (lane == 0), 1.0, 0.0)
        used_ref[k] = jnp.sum(flag).astype(I32)


def scaled(rows, scale):
    half = rows[0:3] * 0.5
    norm = 0.5 - (half[0:1] * half[0:1] + half[1:2] * half[1:2] + half[2:3] * half[2:3])
    norm = jnp.where(rows[3:4] > 0.0, norm, -64.0) * scale
    return half, norm


def stream_features(rows, scale, slope):
    half, norm = scaled(rows, scale)
    high, mid, low = split(half + half)
    one = jnp.ones((1, TILE), F32)
    nh, nm, nl = split(norm)
    weight = jnp.maximum(rows[3:4], 0.0)
    wh, wm, _ = split(weight)
    if slope is None:
        tail = [wh, wm, jnp.zeros((6, TILE), F32)]
    else:
        sh, sm, _ = split(slope)
        tail = [wh, wm, wh, sh, sm, sh, jnp.zeros((2, TILE), F32)]
    parts = [high, one, high, one, high, one, mid, nm, low, nl, mid, nh] + tail
    return jnp.concatenate(parts, axis=0).astype(BF16)


def held_features(rows, scale):
    half, norm = scaled(rows, scale)
    high, mid, low = split(half * scale)
    nh, nm, nl = split(norm)
    one = jnp.ones((1, TILE), F32)
    return [high, nh, mid, nm, low, nl, high, one, high, one, mid, one]


def row_mask(columns_of, width):
    row = lax.broadcasted_iota(I32, (FEATURES, width), 0)
    lane = lax.broadcasted_iota(I32, (FEATURES, width), 1) // TILE
    mask = jnp.zeros((FEATURES, width), jnp.bool_)
    for block, rows in enumerate(columns_of):
        for r in rows:
            mask = mask | ((row == r) & (lane == block))
    return jnp.where(mask, 1.0, 0.0).astype(BF16)


def fold(value):
    return value.reshape(TILE // 8, 8, TILE).sum(axis=0)


def each_pair(list_ref, chunks, use, base=0):
    def group(start, size):
        for e in range(size):
            code = list_ref[start + e]
            use(lax.shift_right_logical(code, 7), code & (TILE - 1))

    def large(c, carry):
        group(base + c * LARGE, LARGE)
        return carry

    def small(c, carry):
        group(base + c * CHUNK, CHUNK)
        return carry

    many = chunks * CHUNK // LARGE
    lax.fori_loop(0, many, large, 0)
    lax.fori_loop(many * (LARGE // CHUNK), chunks, small, 0)


def close_segment(list_ref, n, null, base=0):
    for e in range(CHUNK):
        list_ref[base + n + e] = null
    return (n + CHUNK - 1) // CHUNK


def list_kernel(
    frames,
    me_ref,
    sends_ref,
    dest_ref,
    pair_tiles,
    pair_count,
    own_list,
    ghost_list,
    bounds,
    me_out,
    sends_out,
    dest_out,
):
    pairs, tiles = pair_tiles.shape
    half = own_list.shape[0] // 2
    me = me_ref[0]

    def tile_step(t, found):
        leaving, staying, m = found
        stays = dest_ref[t] == me
        n = jnp.where(stays, staying, leaving)
        count = pair_count[t]
        codes = [pair_tiles[p, t] for p in range(pairs)]
        for p, f in enumerate(codes):
            code = t * TILE + f
            own_list[n] = code
            ghost_list[m] = code
            used = (p < count).astype(I32)
            near = jnp.where(f < tiles, used, 0)
            n = n + near
            m = m + used - near
        return jnp.where(stays, leaving, n), jnp.where(stays, n, staying), m

    leaving, staying, m = lax.fori_loop(0, tiles, tile_step, (0, half, 0))
    bounds[0] = close_segment(own_list, leaving, frames)
    bounds[1] = m
    bounds[2] = close_segment(own_list, staying - half, frames, half)
    me_out[0] = me_ref[0]
    for k in range(sends_ref.shape[0]):
        for g in range(sends_ref.shape[1]):
            sends_out[k, g] = sends_ref[k, g]
    for t in range(tiles):
        dest_out[t] = dest_ref[t]


def density_terms(stream, held, acc_rho, acc_pair):
    def use(t, f):
        both = lax.dot_general(stream[f], held[t], CONTRACT_FIRST, preferred_element_type=F32)
        reach = jnp.maximum(both[:, :TILE], 0.0)
        square = reach * reach
        acc_rho[t] += fold(square * reach * both[:, TILE:])
        acc_pair[t] += fold(square * square)

    return use


def hold_for_density(tiles, frame, held):
    picks = row_mask([[24, 25]], TILE)
    for t in range(tiles):
        parts = held_features(frame[t, 0:4], 1.0) + [jnp.zeros((8, TILE), F32)]
        held[t, :, 0:TILE] = jnp.concatenate(parts, axis=0).astype(BF16)
        held[t, :, TILE:] = picks


def own_density_kernel(
    own_list, bounds, base_ref, occ_ref, rho_ref, pair_ref, held, frame, stream, acc_rho, acc_pair
):
    tiles = occ_ref.shape[0]
    last = frame.shape[0] - 1
    load_own(base_ref, frame)
    hold_for_density(tiles, frame, held)
    for f in range(tiles):
        stream[f] = stream_features(frame[f, 0:4], 1.0, None)
    stream[last] = stream_features(frame[last, 0:4], 1.0, None)
    acc_rho[...] = jnp.zeros_like(acc_rho)
    acc_pair[...] = jnp.zeros_like(acc_pair)
    use = density_terms(stream, held, acc_rho, acc_pair)
    each_pair(own_list, bounds[0], use)
    each_pair(own_list, bounds[2], use, own_list.shape[0] // 2)
    for t in range(tiles):
        rho_ref[t : t + 1] = frame[t, 3:4]
    rho_ref[...] = jnp.sum(acc_rho[...], axis=1) - rho_ref[...]
    pair_ref[...] = jnp.sum(acc_pair[...], axis=1) - occ_ref[...].astype(F32)


def ghost_density_kernel(
    domains,
    me_ref,
    send_list,
    ghost_list,
    bounds,
    base_ref,
    embed_ref,
    occ_ref,
    rho_ref,
    pair_ref,
    held,
    own_ref,
    cross_ref,
    slope_ref,
    energy_ref,
    out_ref,
    frame,
    live_list,
    live_slots,
    live_bounds,
    stream,
    acc_rho,
    acc_pair,
    used_ref,
    live_ref,
):
    me = me_ref[0]
    tiles = occ_ref.shape[0]
    ghosts = send_list.shape[1]
    frames = tiles + SPAN * ghosts
    load_own(base_ref, frame)
    load_ghosts(me, domains, tiles, ghosts, own_ref, cross_ref, frame)
    live_counts(tiles, ghosts, frame, used_ref)
    stream[frames] = stream_features(frame[frames, 0:4], 1.0, None)
    acc_rho[...] = jnp.zeros_like(acc_rho)
    acc_pair[...] = jnp.zeros_like(acc_pair)
    slots = 0
    for k in range(SPAN):
        used = used_ref[k]
        for g in range(ghosts):
            live = (g < used).astype(I32)
            live_ref[tiles + k * ghosts + g] = live
            live_slots[slots] = tiles + k * ghosts + g
            slots = slots + live
    for e in range(WIDE):
        live_slots[slots + e] = frames
    live_bounds[1] = (slots + WIDE - 1) // WIDE
    unroll = 16
    last = bounds[1]

    count = frames - tiles

    def filter_step(c, n):
        codes = [ghost_list[c * unroll + e] for e in range(unroll)]
        live = [live_ref[code & (TILE - 1)] for code in codes]
        for e in range(unroll):
            live_list[n] = codes[e]
            n = n + jnp.where(c * unroll + e < last, live[e], 0)
        for e in range(4):
            f = tiles + jnp.minimum(4 * c + e, count - 1)
            stream[f] = stream_features(frame[f, 0:4], 1.0, None)
        return n

    steps = jnp.maximum((last + unroll - 1) // unroll, (count + 3) // 4)
    n = lax.fori_loop(0, steps, filter_step, 0)
    chunks = close_segment(live_list, n, frames)
    live_bounds[0] = chunks
    each_pair(live_list, chunks, density_terms(stream, held, acc_rho, acc_pair))

    filled = occ_ref[...].astype(F32)
    embed = embed_ref[...]
    root = jnp.sqrt(1.0 + rho_ref[...] + jnp.sum(acc_rho[...], axis=1))
    slope = -0.5 * embed * filled / root
    slope_ref[...] = slope
    pair = pair_ref[...] + jnp.sum(acc_pair[...], axis=1)
    energy_ref[...] = filled * (0.5 * REPULSE * pair - embed * root)
    for k, offset in enumerate(OFFSETS):
        target = me - offset

        @pl.when((target >= 0) & (target < domains))
        def _(k=k, target=target):
            for g in range(ghosts):
                out_ref[target, g : g + 1] = slope_ref[pl.ds(send_list[k, g], 1)]


def hold_for_force(tiles, frame, slope_ref, slopes, held):
    ratio = 1.5 / (SCALE * SCALE)
    for t in range(tiles):
        slopes[t] = slope_ref[t : t + 1]
    for t in range(tiles):
        rows = frame[t, 0:4]
        distance = held_features(rows, SCALE)
        sh, sm, _ = split(slopes[t] * ratio)
        wh, wm, _ = split(rows[3:4] * ratio)
        parts = [sh, sh, sm, wh, wh, wm, jnp.zeros((2, TILE), F32)]
        held[t, :, 0:TILE] = jnp.concatenate(distance + [jnp.zeros((8, TILE), F32)], axis=0).astype(BF16)
        held[t, :, TILE:] = jnp.concatenate(distance + parts, axis=0).astype(BF16)


def stream_for_force(which, frame, slopes, stream):
    for f in which:
        rows = frame[f, 0:4]
        slope = jnp.where(rows[3:4] > 0.0, slopes[f], 0.0)
        stream[f] = stream_features(rows, SCALE, slope)


def widener(stream, wide):
    picks = row_mask([[c, 12 + c, 16 + c] for c in range(3)], 3 * TILE)

    def widen(f, at=None):
        three = lax.dot_general(stream[f], picks, CONTRACT_FIRST, preferred_element_type=F32)
        for c in range(3):
            wide[f if at is None else at, c] = three[:, c * TILE : (c + 1) * TILE]

    return widen


def widen_own(widen, tiles, last):
    step = math.gcd(tiles, 2 * WIDE)

    def some(c, carry):
        for e in range(step):
            widen(c * step + e)
        return carry

    lax.fori_loop(0, tiles // step, some, 0)
    widen(last, tiles)


def widen_ghosts(widen, slots_ref, chunks):
    def some(c, carry):
        for e in range(WIDE):
            widen(slots_ref[c * WIDE + e])
        return carry

    lax.fori_loop(0, chunks, some, 0)


def force_terms(stream, held, wide, acc):
    null = wide.shape[0] - 1

    def use(t, f):
        both = lax.dot_general(stream[f], held[t], CONTRACT_FIRST, preferred_element_type=F32)
        reach = jnp.maximum(both[:, :TILE], 0.0)
        coef = reach * reach * both[:, TILE:]
        acc[t, 3] += fold(coef)
        for q in range(3):
            acc[t, q] += fold(coef * wide[jnp.minimum(f, null), q])

    return use


def load_slopes(me, domains, tiles, ghosts, ghost_slope_ref, slopes):
    for k, offset in enumerate(OFFSETS):
        source = jnp.clip(me + offset, 0, domains - 1)
        for g in range(ghosts):
            slopes[tiles + k * ghosts + g] = ghost_slope_ref[source, g : g + 1]


def own_force_kernel(own_list, bounds, base_ref, slope_ref, sums_ref, held, stream, frame, slopes, wide, acc):
    tiles = base_ref.shape[0]
    last = frame.shape[0] - 1
    load_own(base_ref, frame)
    slopes[last] = jnp.zeros((1, TILE), F32)
    hold_for_force(tiles, frame, slope_ref, slopes, held)
    stream_for_force([*range(tiles), last], frame, slopes, stream)
    widen_own(widener(stream, wide), tiles, last)
    acc[...] = jnp.zeros_like(acc)
    each_pair(own_list, bounds[0], force_terms(stream, held, wide, acc))
    for q in range(4):
        sums_ref[q] = jnp.sum(acc[:, q], axis=1)


def staying_force_kernel(own_list, bounds, base_ref, totals_ref, held, stream, force_ref, here_ref, wide, acc, total):
    tiles = base_ref.shape[0]
    widen_own(widener(stream, wide), tiles, stream.shape[0] - 1)
    acc[...] = jnp.zeros_like(acc)
    each_pair(own_list, bounds[2], force_terms(stream, held, wide, acc), own_list.shape[0] // 2)
    for q in range(4):
        total[q] = totals_ref[q] + jnp.sum(acc[:, q], axis=1)
    for t in range(tiles):
        force = force_of(base_ref, total, t)
        force_ref[:, t * TILE : (t + 1) * TILE] = force
        here_ref[:, t * TILE : (t + 1) * TILE] = force


def ghost_force_kernel(
    domains,
    me_ref,
    dest_ref,
    place_ref,
    live_list,
    live_slots,
    live_bounds,
    frame,
    held,
    ghost_slope_ref,
    sums_ref,
    total,
    out_ref,
    slopes,
    stream,
    wide,
    acc,
):
    me = me_ref[0]
    tiles = held.shape[0]
    ghosts = ghost_slope_ref.shape[1]
    frames = tiles + SPAN * ghosts
    load_slopes(me, domains, tiles, ghosts, ghost_slope_ref, slopes)
    slopes[frames] = jnp.zeros((1, TILE), F32)
    stream_for_force(range(tiles, frames + 1), frame, slopes, stream)
    widen = widener(stream, wide)
    widen_ghosts(widen, live_slots, live_bounds[1])
    widen(frames)
    acc[...] = jnp.zeros_like(acc)
    each_pair(live_list, live_bounds[0], force_terms(stream, held, wide, acc))
    for q in range(4):
        total[q] = sums_ref[q] + jnp.sum(acc[:, q], axis=1)
    for t in range(tiles):
        force = force_of(frame, total, t)
        target = dest_ref[t]
        for q in range(3):
            out_ref[target, :, columns(3 * place_ref[t] + q)] = force[q : q + 1]


def force_of(rows_ref, total, t):
    sums = jnp.concatenate([total[q, t : t + 1] for q in range(3)], axis=0)
    return rows_ref[t, 0:3] * total[3, t : t + 1] - sums


def order_kernel(
    domains,
    ghosts,
    me_ref,
    dest_ref,
    move_row,
    own_ref,
    cross_ref,
    table_ref,
    origin_ref,
    count_ref,
    next_ref,
    atoms_ref,
):
    me = me_ref[0]
    tiles = move_row.shape[0]
    base = 4 * ghosts
    next_ref[0] = 0
    atoms_ref[...] = jnp.zeros_like(atoms_ref)

    def from_other(source):
        @pl.when((source >= 0) & (source < domains))
        def _():
            def use(ref, at):
                first = jnp.concatenate(
                    [ref[at, base + 8 * m + 3 : base + 8 * m + 4, :] for m in range(MMAX)], axis=0
                )
                lane = lax.broadcasted_iota(I32, first.shape, 1)
                flag = jnp.where((first >= 0.0) & (lane == 0), 1.0, 0.0)
                count = jnp.sum(flag).astype(I32)
                slot = next_ref[0]
                next_ref[0] = slot + count
                for m in range(MMAX):

                    @pl.when(m < count)
                    def _(m=m):
                        rows = ref[at, base + 8 * m : base + 8 * m + 8]
                        table_ref[slot + m] = rows
                        origin_ref[slot + m] = source * MMAX + m
                        atoms_ref[...] += rows[3:4]

            arrived(me, source, own_ref, cross_ref, use)

    for offset in OFFSETS[:RADIUS]:
        from_other(me + offset)

    def stay(t, carry):
        @pl.when(dest_ref[t] == me)
        def _():
            slot = next_ref[0]
            next_ref[0] = slot + 1
            origin_ref[slot] = -1 - t
            rows = move_row[t]
            table_ref[slot] = rows
            atoms_ref[...] += rows[3:4]

        return carry

    lax.fori_loop(0, tiles, stay, 0)
    for offset in OFFSETS[RADIUS:]:
        from_other(me + offset)
    origin_ref[origin_ref.shape[0] - 1] = next_ref[0]
    count_ref[0] = jnp.sum(atoms_ref[...]).astype(I32)


def finish_kernel(origin_ref, table_ref, force_ref, in_ref, moved_ref):
    capacity = table_ref.shape[0]
    used = origin_ref[capacity]
    unroll = math.gcd(capacity, 8)

    def step(c, carry):
        for e in range(unroll):
            slot = c * unroll + e
            filled = slot < used
            origin = jnp.where(filled, origin_ref[slot], 0)
            other = jnp.maximum(origin, 0)
            stays = origin < 0
            rows = jnp.where(filled, table_ref[slot], 0.0)
            own = force_ref[:, columns(jnp.maximum(-1 - origin, 0))]
            source = lax.div(other, MMAX)
            place = lax.rem(other, MMAX)
            for q in range(3):
                sent = in_ref[source, :, columns(3 * place + q)]
                force = jnp.where(filled, jnp.where(stays, own[q : q + 1], sent), 0.0)
                new_vel = rows[4 + q : 5 + q] + TIME_STEP * force
                moved_ref[q : q + 1, columns(slot)] = rows[q : q + 1] + TIME_STEP * new_vel
                moved_ref[3 + q : 4 + q, columns(slot)] = new_vel
            moved_ref[6:7, columns(slot)] = rows[3:4]
        return carry

    lax.fori_loop(0, capacity // unroll, step, 0)


def per_device(
    positions,
    velocity,
    density_weight,
    embed_strength,
    occupied,
    send_list,
    send_count,
    pair_tiles,
    pair_count,
    migrate_dest,
):
    domains = lax.axis_size("dom")
    tiles, pairs = pair_tiles.shape
    ghosts = send_list.shape[2]
    frames = tiles + SPAN * ghosts
    me = lax.axis_index("dom").astype(I32)[None]
    chi = density_weight.reshape(tiles, TILE)
    embed = embed_strength.reshape(tiles, TILE)
    occ = occupied.reshape(tiles, TILE)
    sends = send_list[0]
    sent = send_count[0]
    pair_rows = pair_tiles.T
    inputs = (me, positions, velocity, chi, embed, occ, sends, sent, pair_rows, pair_count, migrate_dest)
    rows = 4 * ghosts + 8 * MMAX
    capacity = tiles + 2 * RADIUS * MMAX
    entries = tiles * pairs + 4 * CHUNK
    shape = jax.ShapeDtypeStruct
    scalars = shape((4,), I32)
    one_tile = shape((tiles, TILE), F32)

    def call(kernel, name, outs, in_specs, out_specs, scratch, args, final=(), keep=True, limit=8):
        single = not isinstance(outs, list)
        outs = [outs] if single else outs
        out_specs = [out_specs] if single else out_specs
        outs = [
            (pltpu.VMEM if spec is VMEM else pltpu.SMEM)(out.shape, out.dtype) if i not in final else out
            for i, (out, spec) in enumerate(zip(outs, out_specs))
        ]
        args = [
            pltpu.with_memory_space_constraint(arg, pltpu.VMEM)
            if spec is VMEM and keep
            else pltpu.with_memory_space_constraint(arg, pltpu.HBM)
            if any(arg is given for given in inputs)
            else pltpu.with_memory_space_constraint(arg, pltpu.SMEM)
            for arg, spec in zip(args, in_specs)
        ]
        results = pl.pallas_call(
            kernel,
            out_shape=outs,
            in_specs=in_specs,
            out_specs=out_specs,
            scratch_shapes=scratch,
            compiler_params=pltpu.CompilerParams(vmem_limit_bytes=limit * MIB),
            name=name,
        )(*args)
        return results[0] if single else results

    own, cross, base, move_row, places = call(
        functools.partial(pack_kernel, domains),
        "pack",
        [shape((GROUP, rows, TILE), F32)] * 2 + [shape((tiles, 8, TILE), F32)] * 2 + [shape((tiles,), I32)],
        [SMEM] * 4 + [VMEM] * 4,
        [VMEM] * 4 + [SMEM],
        [pltpu.SMEM((2 * RADIUS + 1,), I32)],
        (me, sends, sent, migrate_dest, positions, velocity, chi, occ),
        keep=False,
    )
    blocks = [[b + i for i in range(GROUP)] for b in range(0, domains, GROUP)]
    crossing = [[(b + i - RADIUS) % domains for i in range(GROUP)] for b in range(0, domains, GROUP)]
    own = lax.all_to_all(own, "dom", 0, 0, axis_index_groups=blocks)
    own_list, ghost_list, bounds, me_here, sends_here, dest_here = call(
        functools.partial(list_kernel, frames),
        "lists",
        [shape((2 * entries,), I32), shape((entries,), I32)]
        + [scalars, shape((1,), I32), shape(sends.shape, I32), shape((tiles,), I32)],
        [SMEM] * 5,
        [SMEM] * 6,
        [],
        (me, sends, migrate_dest, pair_rows, pair_count),
    )
    cross, own, bounds = lax.optimization_barrier((cross, own, bounds))
    cross = lax.all_to_all(cross, "dom", 0, 0, axis_index_groups=crossing)

    frame = pltpu.VMEM((frames + 1, 8, TILE), F32)
    stream = pltpu.VMEM((frames + 1, FEATURES, TILE), BF16)
    slopes = pltpu.VMEM((frames + 1, 1, TILE), F32)
    density_sums = [pltpu.VMEM((tiles, 8, TILE), F32)] * 2
    held_shape = shape((tiles, FEATURES, 2 * TILE), BF16)
    rho, pair_sum, held = call(
        own_density_kernel,
        "own_density",
        [one_tile] * 2 + [held_shape],
        [SMEM] * 2 + [VMEM] * 2,
        [VMEM] * 3,
        [frame, stream] + density_sums,
        (own_list, bounds, base, occ),
    )
    slope, energy, slope_out, frame_rows, live_list, live_slots, live_bounds = call(
        functools.partial(ghost_density_kernel, domains),
        "ghost_density",
        [one_tile, one_tile, shape((domains, ghosts, TILE), F32), shape((frames + 1, 8, TILE), F32)]
        + [shape((entries,), I32), shape((SPAN * ghosts + 2 * WIDE,), I32), scalars],
        [SMEM] * 4 + [VMEM] * 8,
        [VMEM] * 4 + [SMEM] * 3,
        [stream] + density_sums + [pltpu.SMEM((SPAN,), I32), pltpu.SMEM((TILE,), I32)],
        (me_here, sends_here, ghost_list, bounds, base, embed, occ, rho, pair_sum, held, own, cross),
        final=(1,),
    )
    slope_in = lax.all_to_all(slope_out, "dom", 0, 0)

    acc = pltpu.VMEM((tiles, 4, 8, TILE), F32)
    wide_own = pltpu.VMEM((tiles + 1, 3, TILE, TILE), F32)
    sums, held, stream_own = call(
        own_force_kernel,
        "own_force",
        [shape((4, tiles, TILE), F32), held_shape, shape((frames + 1, FEATURES, TILE), BF16)],
        [SMEM] * 2 + [VMEM] * 2,
        [VMEM] * 3,
        [frame, slopes, wide_own, acc],
        (own_list, bounds, base, slope),
        limit=16,
    )
    totals, force_out = call(
        functools.partial(ghost_force_kernel, domains),
        "ghost_force",
        [shape((4, tiles, TILE), F32), shape((domains, 1, 3 * MMAX * TILE), F32)],
        [SMEM] * 6 + [VMEM] * 4,
        [VMEM] * 2,
        [slopes, stream, pltpu.VMEM((frames + 1, 3, TILE, TILE), F32), acc],
        (me_here, dest_here, places, live_list, live_slots, live_bounds, frame_rows, held, slope_in, sums),
        limit=26,
    )
    force_in = lax.all_to_all(force_out, "dom", 0, 0)

    force, force_here = call(
        staying_force_kernel,
        "staying_force",
        [shape(positions.shape, F32)] * 2,
        [SMEM] * 2 + [VMEM] * 4,
        [VMEM] * 2,
        [wide_own, acc, pltpu.VMEM((4, tiles, TILE), F32)],
        (own_list, bounds, base, totals, held, stream_own),
        final=(0,),
        limit=16,
    )
    ordered, origin, count = call(
        functools.partial(order_kernel, domains, ghosts),
        "order",
        [shape((capacity, 8, TILE), F32), shape((capacity + 1,), I32), shape((1,), I32)],
        [SMEM] * 2 + [VMEM] * 3,
        [VMEM, SMEM, SMEM],
        [pltpu.SMEM((1,), I32), pltpu.VMEM((1, TILE), F32)],
        (me_here, dest_here, move_row, own, cross),
        final=(2,),
    )
    moved = call(
        finish_kernel,
        "finish",
        shape((7, capacity * TILE), F32),
        [SMEM] + [VMEM] * 3,
        VMEM,
        [],
        (origin, ordered, force_here, force_in),
        final=(0,),
    )
    return (force, energy.reshape(tiles * TILE), moved, count)


def solution(mesh):
    placed = (
        P(None, "dom"),
        P(None, "dom"),
        P("dom"),
        P("dom"),
        P("dom"),
        P("dom", None, None),
        P("dom", None),
        P("dom", None),
        P("dom"),
        P("dom"),
    )
    return jax.shard_map(
        per_device,
        mesh=mesh,
        in_specs=placed,
        out_specs=(P(None, "dom"), P("dom"), P(None, "dom"), P("dom")),
        check_vma=False,
    )
```

```python
import functools
import math

import jax
import jax.numpy as jnp
from jax import lax
from jax.experimental import pallas as pl
from jax.experimental.pallas import tpu as pltpu
from jax.sharding import PartitionSpec as P

TILE = 128
RADIUS = 4
MMAX = 4
REPULSE = 0.05
TIME_STEP = 0.05
SPAN = 2 * RADIUS
GROUP = 2 * RADIUS
F32 = jnp.float32
BF16 = jnp.bfloat16
I32 = jnp.int32
LARGE = 64
CHUNK = 16
BATCH = 8
WIDE = 8
FEATURES = 32
SCALE = 0.1 ** (1.0 / 3.0)
OFFSETS = [k - RADIUS for k in range(RADIUS)] + [k + 1 for k in range(RADIUS)]
CONTRACT_FIRST = (((0,), (0,)), ((), ()))

VMEM = pl.BlockSpec(memory_space=pltpu.VMEM)
SMEM = pl.BlockSpec(memory_space=pltpu.SMEM)
MIB = 1024 * 1024


def columns(tile):
    return pl.ds(pl.multiple_of(tile * TILE, TILE), TILE)


def split(value):
    high = value.astype(BF16).astype(F32)
    rest = value - high
    mid = rest.astype(BF16).astype(F32)
    return high, mid, rest - mid


def pack_kernel(
    domains,
    me_ref,
    send_list,
    send_count,
    dest_ref,
    pos_ref,
    vel_ref,
    chi_ref,
    occ_ref,
    own_ref,
    cross_ref,
    ghost_row,
    move_row,
    place_ref,
    rank_ref,
):
    me = me_ref[0]
    tiles = chi_ref.shape[0]
    ghosts = send_list.shape[1]
    base = 4 * ghosts
    filled = occ_ref[...].astype(F32)
    weight = chi_ref[...] * filled
    for t in range(tiles):
        span = slice(t * TILE, (t + 1) * TILE)
        ghost_row[t, 0:3] = pos_ref[:, span]
        ghost_row[t, 3:4] = weight[t : t + 1]
        move_row[t, 0:3] = pos_ref[:, span]
        move_row[t, 3:4] = filled[t : t + 1]
        move_row[t, 4:7] = vel_ref[:, span]
    nothing = jnp.full((1, TILE), -1.0, F32)

    def place(target, rows):
        inside = (target // GROUP) == (me // GROUP)

        @pl.when(inside)
        def _():
            rows(own_ref, target % GROUP)

        @pl.when(jnp.logical_not(inside))
        def _():
            rows(cross_ref, (target + RADIUS) % GROUP)

    for k, offset in enumerate(OFFSETS):
        target = me - offset

        @pl.when((target >= 0) & (target < domains))
        def _(k=k, target=target):
            used = send_count[k]

            def rows(out_ref, at):
                for g in range(ghosts):
                    block = ghost_row[send_list[k, g]]
                    live = g < used
                    out_ref[at, 4 * g : 4 * g + 3] = block[0:3]
                    out_ref[at, 4 * g + 3 : 4 * g + 4] = jnp.where(live, block[3:4], nothing)
                for m in range(MMAX):
                    out_ref[at, base + 8 * m + 3 : base + 8 * m + 4] = nothing

            place(target, rows)

    for r in range(2 * RADIUS + 1):
        rank_ref[r] = 0

    for t in range(tiles):
        target = dest_ref[t]
        relative = target - me + RADIUS
        rank = rank_ref[relative]
        rank_ref[relative] = rank + 1
        rank = jnp.minimum(rank, MMAX - 1)
        place_ref[t] = rank
        inside = lax.div(target, GROUP) == lax.div(me, GROUP)
        row = pl.ds(pl.multiple_of(base + 8 * rank, 8), 8)
        own_ref[lax.rem(jnp.where(inside, target, me), GROUP), row] = move_row[t]
        cross_ref[lax.rem(jnp.where(inside, me, target) + RADIUS, GROUP), row] = move_row[t]


def arrived(me, source, own_ref, cross_ref, use):
    inside = (source // GROUP) == (me // GROUP)

    @pl.when(inside)
    def _():
        use(own_ref, source % GROUP)

    @pl.when(jnp.logical_not(inside))
    def _():
        use(cross_ref, (source + RADIUS) % GROUP)


def load_own(base_ref, frame):
    tiles = base_ref.shape[0]
    last = frame.shape[0] - 1
    frame[0:tiles] = base_ref[...]
    frame[last, 0:4] = jnp.full((4, TILE), -1.0, F32)


def load_ghosts(me, domains, tiles, ghosts, own_ref, cross_ref, frame):
    for k, offset in enumerate(OFFSETS):
        source = me + offset
        start = tiles + k * ghosts
        valid = (source >= 0) & (source < domains)

        @pl.when(valid)
        def _(start=start, source=source):
            def use(ref, at):
                for g in range(ghosts):
                    frame[start + g, 0:4] = ref[at, 4 * g : 4 * g + 4]

            arrived(me, source, own_ref, cross_ref, use)

        @pl.when(jnp.logical_not(valid))
        def _(start=start):
            for g in range(ghosts):
                frame[start + g, 0:4] = jnp.full((4, TILE), -1.0, F32)


def live_counts(tiles, ghosts, frame, used_ref):
    for k in range(SPAN):
        start = tiles + k * ghosts
        first = frame[start : start + ghosts, 3, :]
        lane = lax.broadcasted_iota(I32, first.shape, 1)
        flag = jnp.where((first >= 0.0) & (lane == 0), 1.0, 0.0)
        used_ref[k] = jnp.sum(flag).astype(I32)


def scaled(rows, scale):
    half = rows[0:3] * 0.5
    norm = 0.5 - (half[0:1] * half[0:1] + half[1:2] * half[1:2] + half[2:3] * half[2:3])
    norm = jnp.where(rows[3:4] > 0.0, norm, -64.0) * scale
    return half, norm


def stream_features(rows, scale, slope):
    half, norm = scaled(rows, scale)
    high, mid, low = split(half + half)
    one = jnp.ones((1, TILE), F32)
    nh, nm, nl = split(norm)
    weight = jnp.maximum(rows[3:4], 0.0)
    wh, wm, _ = split(weight)
    if slope is None:
        tail = [wh, wm, jnp.zeros((6, TILE), F32)]
    else:
        sh, sm, _ = split(slope)
        tail = [wh, wm, wh, sh, sm, sh, jnp.zeros((2, TILE), F32)]
    parts = [high, one, high, one, high, one, mid, nm, low, nl, mid, nh] + tail
    return jnp.concatenate(parts, axis=0).astype(BF16)


def held_features(rows, scale):
    half, norm = scaled(rows, scale)
    high, mid, low = split(half * scale)
    nh, nm, nl = split(norm)
    one = jnp.ones((1, TILE), F32)
    return [high, nh, mid, nm, low, nl, high, one, high, one, mid, one]


def row_mask(columns_of, width):
    row = lax.broadcasted_iota(I32, (FEATURES, width), 0)
    lane = lax.broadcasted_iota(I32, (FEATURES, width), 1) // TILE
    mask = jnp.zeros((FEATURES, width), jnp.bool_)
    for block, rows in enumerate(columns_of):
        for r in rows:
            mask = mask | ((row == r) & (lane == block))
    return jnp.where(mask, 1.0, 0.0).astype(BF16)


def fold(value):
    return value.reshape(TILE // 8, 8, TILE).sum(axis=0)


def each_pair(list_ref, chunks, use, base=0):
    def group(start, size):
        for e in range(size):
            code = list_ref[start + e]
            use(lax.shift_right_logical(code, 7), code & (TILE - 1))

    def large(c, carry):
        group(base + c * LARGE, LARGE)
        return carry

    def small(c, carry):
        group(base + c * CHUNK, CHUNK)
        return carry

    many = chunks * CHUNK // LARGE
    lax.fori_loop(0, many, large, 0)
    lax.fori_loop(many * (LARGE // CHUNK), chunks, small, 0)


def close_segment(list_ref, n, null, base=0):
    for e in range(CHUNK):
        list_ref[base + n + e] = null
    return (n + CHUNK - 1) // CHUNK


def list_kernel(
    frames,
    me_ref,
    sends_ref,
    dest_ref,
    pair_tiles,
    pair_count,
    own_list,
    ghost_list,
    bounds,
    me_out,
    sends_out,
    dest_out,
):
    pairs, tiles = pair_tiles.shape
    half = own_list.shape[0] // 2
    me = me_ref[0]

    def tile_step(t, found):
        leaving, staying, m = found
        stays = dest_ref[t] == me
        n = jnp.where(stays, staying, leaving)
        count = pair_count[t]
        for b in range(0, pairs, BATCH):
            batch = range(b, min(b + BATCH, pairs))
            found = [pair_tiles[p, t] for p in batch]
            for p, f in zip(batch, found):
                code = t * TILE + f
                own_list[n] = code
                ghost_list[m] = code
                used = (p < count).astype(I32)
                near = jnp.where(f < tiles, used, 0)
                n = n + near
                m = m + used - near
        return jnp.where(stays, leaving, n), jnp.where(stays, n, staying), m

    leaving, staying, m = lax.fori_loop(0, tiles, tile_step, (0, half, 0))
    bounds[0] = close_segment(own_list, leaving, frames)
    bounds[1] = m
    for e in range(CHUNK):
        ghost_list[m + e] = 0
    bounds[2] = close_segment(own_list, staying - half, frames, half)
    me_out[0] = me_ref[0]
    for k in range(sends_ref.shape[0]):
        for g in range(sends_ref.shape[1]):
            sends_out[k, g] = sends_ref[k, g]
    for t in range(tiles):
        dest_out[t] = dest_ref[t]


def density_terms(stream, held, acc_rho, acc_pair):
    def use(t, f):
        both = lax.dot_general(stream[f], held[t], CONTRACT_FIRST, preferred_element_type=F32)
        reach = jnp.maximum(both[:, :TILE], 0.0)
        square = reach * reach
        acc_rho[t] += fold(square * reach * both[:, TILE:])
        acc_pair[t] += fold(square * square)

    return use


def hold_for_density(tiles, frame, held):
    picks = row_mask([[24, 25]], TILE)
    for t in range(tiles):
        parts = held_features(frame[t, 0:4], 1.0) + [jnp.zeros((8, TILE), F32)]
        held[t, :, 0:TILE] = jnp.concatenate(parts, axis=0).astype(BF16)
        held[t, :, TILE:] = picks


def own_density_kernel(
    own_list, bounds, base_ref, occ_ref, rho_ref, pair_ref, held, frame, stream, acc_rho, acc_pair
):
    tiles = occ_ref.shape[0]
    last = frame.shape[0] - 1
    load_own(base_ref, frame)
    hold_for_density(tiles, frame, held)
    for f in range(tiles):
        stream[f] = stream_features(frame[f, 0:4], 1.0, None)
    stream[last] = stream_features(frame[last, 0:4], 1.0, None)
    acc_rho[...] = jnp.zeros_like(acc_rho)
    acc_pair[...] = jnp.zeros_like(acc_pair)
    use = density_terms(stream, held, acc_rho, acc_pair)
    each_pair(own_list, bounds[0], use)
    each_pair(own_list, bounds[2], use, own_list.shape[0] // 2)
    for t in range(tiles):
        rho_ref[t : t + 1] = frame[t, 3:4]
    rho_ref[...] = jnp.sum(acc_rho[...], axis=1) - rho_ref[...]
    pair_ref[...] = jnp.sum(acc_pair[...], axis=1) - occ_ref[...].astype(F32)


def ghost_density_kernel(
    domains,
    me_ref,
    send_list,
    ghost_list,
    bounds,
    base_ref,
    embed_ref,
    occ_ref,
    rho_ref,
    pair_ref,
    held,
    own_ref,
    cross_ref,
    slope_ref,
    energy_ref,
    out_ref,
    frame,
    live_list,
    live_slots,
    live_bounds,
    stream,
    acc_rho,
    acc_pair,
    used_ref,
    live_ref,
):
    me = me_ref[0]
    tiles = occ_ref.shape[0]
    ghosts = send_list.shape[1]
    frames = tiles + SPAN * ghosts
    load_own(base_ref, frame)
    load_ghosts(me, domains, tiles, ghosts, own_ref, cross_ref, frame)
    live_counts(tiles, ghosts, frame, used_ref)
    stream[frames] = stream_features(frame[frames, 0:4], 1.0, None)
    acc_rho[...] = jnp.zeros_like(acc_rho)
    acc_pair[...] = jnp.zeros_like(acc_pair)
    slots = 0
    for k in range(SPAN):
        used = used_ref[k]
        for g in range(ghosts):
            live = (g < used).astype(I32)
            live_ref[tiles + k * ghosts + g] = live
            live_slots[slots] = tiles + k * ghosts + g
            slots = slots + live
    for e in range(WIDE):
        live_slots[slots + e] = frames
    live_bounds[1] = (slots + WIDE - 1) // WIDE
    unroll = CHUNK
    last = bounds[1]
    live_ref[0] = 0

    count = frames - tiles

    def filter_step(c, n):
        for b in range(0, unroll, BATCH):
            codes = [ghost_list[c * unroll + b + e] for e in range(BATCH)]
            live = [live_ref[code & (TILE - 1)] for code in codes]
            for e in range(BATCH):
                live_list[n] = codes[e]
                n = n + live[e]
        for e in range(4):
            f = tiles + jnp.minimum(4 * c + e, count - 1)
            stream[f] = stream_features(frame[f, 0:4], 1.0, None)
        return n

    steps = (last + unroll - 1) // unroll
    n = lax.fori_loop(0, steps, filter_step, 0)

    def feature_step(c, carry):
        for e in range(4):
            f = tiles + jnp.minimum(4 * c + e, count - 1)
            stream[f] = stream_features(frame[f, 0:4], 1.0, None)
        return carry

    lax.fori_loop(steps, (count + 3) // 4, feature_step, 0)
    chunks = close_segment(live_list, n, frames)
    live_bounds[0] = chunks
    each_pair(live_list, chunks, density_terms(stream, held, acc_rho, acc_pair))

    filled = occ_ref[...].astype(F32)
    embed = embed_ref[...]
    root = jnp.sqrt(1.0 + rho_ref[...] + jnp.sum(acc_rho[...], axis=1))
    slope = -0.5 * embed * filled / root
    slope_ref[...] = slope
    pair = pair_ref[...] + jnp.sum(acc_pair[...], axis=1)
    energy_ref[...] = filled * (0.5 * REPULSE * pair - embed * root)
    for k, offset in enumerate(OFFSETS):
        target = me - offset

        @pl.when((target >= 0) & (target < domains))
        def _(k=k, target=target):
            for g in range(ghosts):
                out_ref[target, g : g + 1] = slope_ref[pl.ds(send_list[k, g], 1)]


def hold_for_force(tiles, frame, slope_ref, slopes, held):
    ratio = 1.5 / (SCALE * SCALE)
    for t in range(tiles):
        slopes[t] = slope_ref[t : t + 1]
    for t in range(tiles):
        rows = frame[t, 0:4]
        distance = held_features(rows, SCALE)
        sh, sm, _ = split(slopes[t] * ratio)
        wh, wm, _ = split(rows[3:4] * ratio)
        parts = [sh, sh, sm, wh, wh, wm, jnp.zeros((2, TILE), F32)]
        held[t, :, 0:TILE] = jnp.concatenate(distance + [jnp.zeros((8, TILE), F32)], axis=0).astype(BF16)
        held[t, :, TILE:] = jnp.concatenate(distance + parts, axis=0).astype(BF16)


def stream_for_force(which, frame, slopes, stream):
    for f in which:
        rows = frame[f, 0:4]
        slope = jnp.where(rows[3:4] > 0.0, slopes[f], 0.0)
        stream[f] = stream_features(rows, SCALE, slope)


def widener(stream, wide):
    picks = row_mask([[c, 12 + c, 16 + c] for c in range(3)], 3 * TILE)

    def widen(f, at=None):
        three = lax.dot_general(stream[f], picks, CONTRACT_FIRST, preferred_element_type=F32)
        for c in range(3):
            wide[f if at is None else at, c] = three[:, c * TILE : (c + 1) * TILE]

    return widen


def widen_own(widen, tiles, last):
    step = math.gcd(tiles, 2 * WIDE)

    def some(c, carry):
        for e in range(step):
            widen(c * step + e)
        return carry

    lax.fori_loop(0, tiles // step, some, 0)
    widen(last, tiles)


def widen_ghosts(widen, slots_ref, chunks):
    def some(c, carry):
        for e in range(WIDE):
            widen(slots_ref[c * WIDE + e])
        return carry

    lax.fori_loop(0, chunks, some, 0)


def force_terms(stream, held, wide, acc):
    null = wide.shape[0] - 1

    def use(t, f):
        both = lax.dot_general(stream[f], held[t], CONTRACT_FIRST, preferred_element_type=F32)
        reach = jnp.maximum(both[:, :TILE], 0.0)
        coef = reach * reach * both[:, TILE:]
        acc[t, 3] += fold(coef)
        for q in range(3):
            acc[t, q] += fold(coef * wide[jnp.minimum(f, null), q])

    return use


def load_slopes(me, domains, tiles, ghosts, ghost_slope_ref, slopes):
    for k, offset in enumerate(OFFSETS):
        source = jnp.clip(me + offset, 0, domains - 1)
        for g in range(ghosts):
            slopes[tiles + k * ghosts + g] = ghost_slope_ref[source, g : g + 1]


def own_force_kernel(own_list, bounds, base_ref, slope_ref, sums_ref, held, stream, frame, slopes, wide, acc):
    tiles = base_ref.shape[0]
    last = frame.shape[0] - 1
    load_own(base_ref, frame)
    slopes[last] = jnp.zeros((1, TILE), F32)
    hold_for_force(tiles, frame, slope_ref, slopes, held)
    stream_for_force([*range(tiles), last], frame, slopes, stream)
    widen_own(widener(stream, wide), tiles, last)
    acc[...] = jnp.zeros_like(acc)
    each_pair(own_list, bounds[0], force_terms(stream, held, wide, acc))
    for q in range(4):
        sums_ref[q] = jnp.sum(acc[:, q], axis=1)


def staying_force_kernel(own_list, bounds, base_ref, totals_ref, held, stream, force_ref, here_ref, wide, acc, total):
    tiles = base_ref.shape[0]
    widen_own(widener(stream, wide), tiles, stream.shape[0] - 1)
    acc[...] = jnp.zeros_like(acc)
    each_pair(own_list, bounds[2], force_terms(stream, held, wide, acc), own_list.shape[0] // 2)
    for q in range(4):
        total[q] = totals_ref[q] + jnp.sum(acc[:, q], axis=1)
    for t in range(tiles):
        force = force_of(base_ref, total, t)
        force_ref[:, t * TILE : (t + 1) * TILE] = force
        here_ref[:, t * TILE : (t + 1) * TILE] = force


def ghost_force_kernel(
    domains,
    me_ref,
    dest_ref,
    place_ref,
    live_list,
    live_slots,
    live_bounds,
    frame,
    held,
    ghost_slope_ref,
    sums_ref,
    total,
    out_ref,
    slopes,
    stream,
    wide,
    acc,
):
    me = me_ref[0]
    tiles = held.shape[0]
    ghosts = ghost_slope_ref.shape[1]
    frames = tiles + SPAN * ghosts
    load_slopes(me, domains, tiles, ghosts, ghost_slope_ref, slopes)
    slopes[frames] = jnp.zeros((1, TILE), F32)
    stream_for_force(range(tiles, frames + 1), frame, slopes, stream)
    widen = widener(stream, wide)
    widen_ghosts(widen, live_slots, live_bounds[1])
    widen(frames)
    acc[...] = jnp.zeros_like(acc)
    each_pair(live_list, live_bounds[0], force_terms(stream, held, wide, acc))
    for q in range(4):
        total[q] = sums_ref[q] + jnp.sum(acc[:, q], axis=1)
    for t in range(tiles):
        force = force_of(frame, total, t)
        target = dest_ref[t]
        for q in range(3):
            out_ref[target, :, columns(3 * place_ref[t] + q)] = force[q : q + 1]


def force_of(rows_ref, total, t):
    sums = jnp.concatenate([total[q, t : t + 1] for q in range(3)], axis=0)
    return rows_ref[t, 0:3] * total[3, t : t + 1] - sums


def order_kernel(
    domains,
    ghosts,
    me_ref,
    dest_ref,
    move_row,
    own_ref,
    cross_ref,
    table_ref,
    origin_ref,
    count_ref,
    next_ref,
    atoms_ref,
):
    me = me_ref[0]
    tiles = move_row.shape[0]
    base = 4 * ghosts
    next_ref[0] = 0
    atoms_ref[...] = jnp.zeros_like(atoms_ref)

    def from_other(source):
        @pl.when((source >= 0) & (source < domains))
        def _():
            def use(ref, at):
                first = jnp.concatenate(
                    [ref[at, base + 8 * m + 3 : base + 8 * m + 4, :] for m in range(MMAX)], axis=0
                )
                lane = lax.broadcasted_iota(I32, first.shape, 1)
                flag = jnp.where((first >= 0.0) & (lane == 0), 1.0, 0.0)
                count = jnp.sum(flag).astype(I32)
                slot = next_ref[0]
                next_ref[0] = slot + count
                for m in range(MMAX):

                    @pl.when(m < count)
                    def _(m=m):
                        rows = ref[at, base + 8 * m : base + 8 * m + 8]
                        table_ref[slot + m] = rows
                        origin_ref[slot + m] = source * MMAX + m
                        atoms_ref[...] += rows[3:4]

            arrived(me, source, own_ref, cross_ref, use)

    for offset in OFFSETS[:RADIUS]:
        from_other(me + offset)

    slot = next_ref[0]
    for t in range(tiles):
        stays = dest_ref[t] == me
        rows = move_row[t]
        table_ref[slot] = rows
        origin_ref[slot] = -1 - t
        atoms_ref[...] += jnp.where(stays, rows[3:4], 0.0)
        slot = slot + stays.astype(I32)
    next_ref[0] = slot
    for offset in OFFSETS[RADIUS:]:
        from_other(me + offset)
    origin_ref[origin_ref.shape[0] - 1] = next_ref[0]
    count_ref[0] = jnp.sum(atoms_ref[...]).astype(I32)


def finish_kernel(origin_ref, table_ref, force_ref, in_ref, moved_ref):
    capacity = table_ref.shape[0] - 1
    used = origin_ref[capacity + 1]
    unroll = math.gcd(capacity, 8)

    def step(c, carry):
        for e in range(unroll):
            slot = c * unroll + e
            filled = slot < used
            origin = jnp.where(filled, origin_ref[slot], 0)
            other = jnp.maximum(origin, 0)
            stays = origin < 0
            rows = jnp.where(filled, table_ref[slot], 0.0)
            own = force_ref[:, columns(jnp.maximum(-1 - origin, 0))]
            source = lax.div(other, MMAX)
            place = lax.rem(other, MMAX)
            for q in range(3):
                sent = in_ref[source, :, columns(3 * place + q)]
                force = jnp.where(filled, jnp.where(stays, own[q : q + 1], sent), 0.0)
                new_vel = rows[4 + q : 5 + q] + TIME_STEP * force
                moved_ref[q : q + 1, columns(slot)] = rows[q : q + 1] + TIME_STEP * new_vel
                moved_ref[3 + q : 4 + q, columns(slot)] = new_vel
            moved_ref[6:7, columns(slot)] = rows[3:4]
        return carry

    lax.fori_loop(0, capacity // unroll, step, 0)


def per_device(
    positions,
    velocity,
    density_weight,
    embed_strength,
    occupied,
    send_list,
    send_count,
    pair_tiles,
    pair_count,
    migrate_dest,
):
    domains = lax.axis_size("dom")
    tiles, pairs = pair_tiles.shape
    ghosts = send_list.shape[2]
    frames = tiles + SPAN * ghosts
    me = lax.axis_index("dom").astype(I32)[None]
    chi = density_weight.reshape(tiles, TILE)
    embed = embed_strength.reshape(tiles, TILE)
    occ = occupied.reshape(tiles, TILE)
    sends = send_list[0]
    sent = send_count[0]
    pair_rows = pair_tiles.T
    inputs = (me, positions, velocity, chi, embed, occ, sends, sent, pair_rows, pair_count, migrate_dest)
    rows = 4 * ghosts + 8 * MMAX
    capacity = tiles + 2 * RADIUS * MMAX
    entries = tiles * pairs + 4 * CHUNK
    shape = jax.ShapeDtypeStruct
    scalars = shape((4,), I32)
    one_tile = shape((tiles, TILE), F32)

    def call(kernel, name, outs, in_specs, out_specs, scratch, args, final=(), keep=True, limit=8):
        single = not isinstance(outs, list)
        outs = [outs] if single else outs
        out_specs = [out_specs] if single else out_specs
        outs = [
            (pltpu.VMEM if spec is VMEM else pltpu.SMEM)(out.shape, out.dtype) if i not in final else out
            for i, (out, spec) in enumerate(zip(outs, out_specs))
        ]
        args = [
            pltpu.with_memory_space_constraint(arg, pltpu.VMEM)
            if spec is VMEM and keep
            else pltpu.with_memory_space_constraint(arg, pltpu.HBM)
            if any(arg is given for given in inputs)
            else pltpu.with_memory_space_constraint(arg, pltpu.SMEM)
            for arg, spec in zip(args, in_specs)
        ]
        results = pl.pallas_call(
            kernel,
            out_shape=outs,
            in_specs=in_specs,
            out_specs=out_specs,
            scratch_shapes=scratch,
            compiler_params=pltpu.CompilerParams(vmem_limit_bytes=limit * MIB),
            name=name,
        )(*args)
        return results[0] if single else results

    own, cross, base, move_row, places = call(
        functools.partial(pack_kernel, domains),
        "pack",
        [shape((GROUP, rows, TILE), F32)] * 2 + [shape((tiles, 8, TILE), F32)] * 2 + [shape((tiles,), I32)],
        [SMEM] * 4 + [VMEM] * 4,
        [VMEM] * 4 + [SMEM],
        [pltpu.SMEM((2 * RADIUS + 1,), I32)],
        (me, sends, sent, migrate_dest, positions, velocity, chi, occ),
        keep=False,
    )
    blocks = [[b + i for i in range(GROUP)] for b in range(0, domains, GROUP)]
    crossing = [[(b + i - RADIUS) % domains for i in range(GROUP)] for b in range(0, domains, GROUP)]
    own = lax.all_to_all(own, "dom", 0, 0, axis_index_groups=blocks)
    own_list, ghost_list, bounds, me_here, sends_here, dest_here = call(
        functools.partial(list_kernel, frames),
        "lists",
        [shape((2 * entries,), I32), shape((entries,), I32)]
        + [scalars, shape((1,), I32), shape(sends.shape, I32), shape((tiles,), I32)],
        [SMEM] * 5,
        [SMEM] * 6,
        [],
        (me, sends, migrate_dest, pair_rows, pair_count),
    )
    cross, own, bounds = lax.optimization_barrier((cross, own, bounds))
    cross = lax.all_to_all(cross, "dom", 0, 0, axis_index_groups=crossing)

    frame = pltpu.VMEM((frames + 1, 8, TILE), F32)
    stream = pltpu.VMEM((frames + 1, FEATURES, TILE), BF16)
    slopes = pltpu.VMEM((frames + 1, 1, TILE), F32)
    density_sums = [pltpu.VMEM((tiles, 8, TILE), F32)] * 2
    held_shape = shape((tiles, FEATURES, 2 * TILE), BF16)
    rho, pair_sum, held = call(
        own_density_kernel,
        "own_density",
        [one_tile] * 2 + [held_shape],
        [SMEM] * 2 + [VMEM] * 2,
        [VMEM] * 3,
        [frame, stream] + density_sums,
        (own_list, bounds, base, occ),
    )
    slope, energy, slope_out, frame_rows, live_list, live_slots, live_bounds = call(
        functools.partial(ghost_density_kernel, domains),
        "ghost_density",
        [one_tile, one_tile, shape((domains, ghosts, TILE), F32), shape((frames + 1, 8, TILE), F32)]
        + [shape((entries,), I32), shape((SPAN * ghosts + 2 * WIDE,), I32), scalars],
        [SMEM] * 4 + [VMEM] * 8,
        [VMEM] * 4 + [SMEM] * 3,
        [stream] + density_sums + [pltpu.SMEM((SPAN,), I32), pltpu.SMEM((TILE,), I32)],
        (me_here, sends_here, ghost_list, bounds, base, embed, occ, rho, pair_sum, held, own, cross),
        final=(1,),
    )
    slope_in = lax.all_to_all(slope_out, "dom", 0, 0)

    acc = pltpu.VMEM((tiles, 4, 8, TILE), F32)
    wide_own = pltpu.VMEM((tiles + 1, 3, TILE, TILE), F32)
    sums, held, stream_own = call(
        own_force_kernel,
        "own_force",
        [shape((4, tiles, TILE), F32), held_shape, shape((frames + 1, FEATURES, TILE), BF16)],
        [SMEM] * 2 + [VMEM] * 2,
        [VMEM] * 3,
        [frame, slopes, wide_own, acc],
        (own_list, bounds, base, slope),
        limit=16,
    )
    totals, force_out = call(
        functools.partial(ghost_force_kernel, domains),
        "ghost_force",
        [shape((4, tiles, TILE), F32), shape((domains, 1, 3 * MMAX * TILE), F32)],
        [SMEM] * 6 + [VMEM] * 4,
        [VMEM] * 2,
        [slopes, stream, pltpu.VMEM((frames + 1, 3, TILE, TILE), F32), acc],
        (me_here, dest_here, places, live_list, live_slots, live_bounds, frame_rows, held, slope_in, sums),
        limit=26,
    )
    force_in = lax.all_to_all(force_out, "dom", 0, 0)

    force, force_here = call(
        staying_force_kernel,
        "staying_force",
        [shape(positions.shape, F32)] * 2,
        [SMEM] * 2 + [VMEM] * 4,
        [VMEM] * 2,
        [wide_own, acc, pltpu.VMEM((4, tiles, TILE), F32)],
        (own_list, bounds, base, totals, held, stream_own),
        final=(0,),
        limit=16,
    )
    ordered, origin, count = call(
        functools.partial(order_kernel, domains, ghosts),
        "order",
        [shape((capacity + 1, 8, TILE), F32), shape((capacity + 2,), I32), shape((1,), I32)],
        [SMEM] * 2 + [VMEM] * 3,
        [VMEM, SMEM, SMEM],
        [pltpu.SMEM((1,), I32), pltpu.VMEM((1, TILE), F32)],
        (me_here, dest_here, move_row, own, cross),
        final=(2,),
    )
    moved = call(
        finish_kernel,
        "finish",
        shape((7, capacity * TILE), F32),
        [SMEM] + [VMEM] * 3,
        VMEM,
        [],
        (origin, ordered, force_here, force_in),
        final=(0,),
    )
    return (force, energy.reshape(tiles * TILE), moved, count)


def solution(mesh):
    placed = (
        P(None, "dom"),
        P(None, "dom"),
        P("dom"),
        P("dom"),
        P("dom"),
        P("dom", None, None),
        P("dom", None),
        P("dom", None),
        P("dom"),
        P("dom"),
    )
    return jax.shard_map(
        per_device,
        mesh=mesh,
        in_specs=placed,
        out_specs=(P(None, "dom"), P("dom"), P(None, "dom"), P("dom")),
        check_vma=False,
    )
```

```python
import functools
import math

import jax
import jax.numpy as jnp
from jax import lax
from jax.experimental import pallas as pl
from jax.experimental.pallas import tpu as pltpu
from jax.sharding import PartitionSpec as P

TILE = 128
RADIUS = 4
MMAX = 4
REPULSE = 0.05
TIME_STEP = 0.05
SPAN = 2 * RADIUS
GROUP = 2 * RADIUS
F32 = jnp.float32
BF16 = jnp.bfloat16
I32 = jnp.int32
LARGE = 64
GHOST_LARGE = 96
CHUNK = 16
BATCH = 4
WIDE = 16
FEATURES = 32
SCALE = 0.1 ** (1.0 / 3.0)
OFFSETS = [k - RADIUS for k in range(RADIUS)] + [k + 1 for k in range(RADIUS)]
CONTRACT_FIRST = (((0,), (0,)), ((), ()))

VMEM = pl.BlockSpec(memory_space=pltpu.VMEM)
SMEM = pl.BlockSpec(memory_space=pltpu.SMEM)
MIB = 1024 * 1024


def columns(tile):
    return pl.ds(pl.multiple_of(tile * TILE, TILE), TILE)


def split(value):
    high = value.astype(BF16).astype(F32)
    rest = value - high
    mid = rest.astype(BF16).astype(F32)
    return high, mid, rest - mid


def pack_kernel(
    domains,
    me_ref,
    send_list,
    send_count,
    dest_ref,
    pos_ref,
    vel_ref,
    chi_ref,
    occ_ref,
    own_ref,
    cross_ref,
    ghost_row,
    move_row,
    place_ref,
    rank_ref,
):
    me = me_ref[0]
    tiles = chi_ref.shape[0]
    ghosts = send_list.shape[1]
    base = 4 * ghosts
    filled = occ_ref[...].astype(F32)
    weight = chi_ref[...] * filled
    for t in range(tiles):
        span = slice(t * TILE, (t + 1) * TILE)
        ghost_row[t, 0:3] = pos_ref[:, span]
        ghost_row[t, 3:4] = weight[t : t + 1]
        move_row[t, 0:3] = pos_ref[:, span]
        move_row[t, 3:4] = filled[t : t + 1]
        move_row[t, 4:7] = vel_ref[:, span]
    nothing = jnp.full((1, TILE), -1.0, F32)

    def place(target, rows):
        inside = (target // GROUP) == (me // GROUP)

        @pl.when(inside)
        def _():
            rows(own_ref, target % GROUP)

        @pl.when(jnp.logical_not(inside))
        def _():
            rows(cross_ref, (target + RADIUS) % GROUP)

    for k, offset in enumerate(OFFSETS):
        target = me - offset

        @pl.when((target >= 0) & (target < domains))
        def _(k=k, target=target):
            used = send_count[k]

            def rows(out_ref, at):
                for g in range(ghosts):
                    block = ghost_row[send_list[k, g]]
                    live = g < used
                    out_ref[at, 4 * g : 4 * g + 3] = block[0:3]
                    out_ref[at, 4 * g + 3 : 4 * g + 4] = jnp.where(live, block[3:4], nothing)
                for m in range(MMAX):
                    out_ref[at, base + 8 * m + 3 : base + 8 * m + 4] = nothing

            place(target, rows)

    for r in range(2 * RADIUS + 1):
        rank_ref[r] = 0

    for t in range(tiles):
        target = dest_ref[t]
        relative = target - me + RADIUS
        rank = rank_ref[relative]
        rank_ref[relative] = rank + 1
        rank = jnp.minimum(rank, MMAX - 1)
        place_ref[t] = rank
        inside = lax.div(target, GROUP) == lax.div(me, GROUP)
        row = pl.ds(pl.multiple_of(base + 8 * rank, 8), 8)
        own_ref[lax.rem(jnp.where(inside, target, me), GROUP), row] = move_row[t]
        cross_ref[lax.rem(jnp.where(inside, me, target) + RADIUS, GROUP), row] = move_row[t]


def arrived(me, source, own_ref, cross_ref, use):
    inside = (source // GROUP) == (me // GROUP)

    @pl.when(inside)
    def _():
        use(own_ref, source % GROUP)

    @pl.when(jnp.logical_not(inside))
    def _():
        use(cross_ref, (source + RADIUS) % GROUP)


def load_own(base_ref, frame):
    tiles = base_ref.shape[0]
    last = frame.shape[0] - 1
    frame[0:tiles] = base_ref[...]
    frame[last, 0:4] = jnp.full((4, TILE), -1.0, F32)


def load_ghosts(me, domains, tiles, ghosts, own_ref, cross_ref, frame):
    for k, offset in enumerate(OFFSETS):
        source = me + offset
        start = tiles + k * ghosts
        valid = (source >= 0) & (source < domains)

        @pl.when(valid)
        def _(start=start, source=source):
            def use(ref, at):
                for g in range(ghosts):
                    frame[start + g, 0:4] = ref[at, 4 * g : 4 * g + 4]

            arrived(me, source, own_ref, cross_ref, use)

        @pl.when(jnp.logical_not(valid))
        def _(start=start):
            for g in range(ghosts):
                frame[start + g, 0:4] = jnp.full((4, TILE), -1.0, F32)


def live_counts(tiles, ghosts, frame, used_ref):
    for k in range(SPAN):
        start = tiles + k * ghosts
        first = frame[start : start + ghosts, 3, :]
        lane = lax.broadcasted_iota(I32, first.shape, 1)
        flag = jnp.where((first >= 0.0) & (lane == 0), 1.0, 0.0)
        used_ref[k] = jnp.sum(flag).astype(I32)


def scaled(rows, scale):
    half = rows[0:3] * 0.5
    norm = 0.5 - (half[0:1] * half[0:1] + half[1:2] * half[1:2] + half[2:3] * half[2:3])
    norm = jnp.where(rows[3:4] > 0.0, norm, -64.0) * scale
    return half, norm


def stream_features(rows, scale, slope):
    half, norm = scaled(rows, scale)
    high, mid, low = split(half + half)
    one = jnp.ones((1, TILE), F32)
    nh, nm, nl = split(norm)
    weight = jnp.maximum(rows[3:4], 0.0)
    wh, wm, _ = split(weight)
    if slope is None:
        tail = [wh, wm, jnp.zeros((6, TILE), F32)]
    else:
        sh, sm, _ = split(slope)
        tail = [wh, wm, wh, sh, sm, sh, jnp.zeros((2, TILE), F32)]
    parts = [high, one, high, one, high, one, mid, nm, low, nl, mid, nh] + tail
    return jnp.concatenate(parts, axis=0).astype(BF16)


def held_features(rows, scale):
    half, norm = scaled(rows, scale)
    high, mid, low = split(half * scale)
    nh, nm, nl = split(norm)
    one = jnp.ones((1, TILE), F32)
    return [high, nh, mid, nm, low, nl, high, one, high, one, mid, one]


def row_mask(columns_of, width):
    row = lax.broadcasted_iota(I32, (FEATURES, width), 0)
    lane = lax.broadcasted_iota(I32, (FEATURES, width), 1) // TILE
    mask = jnp.zeros((FEATURES, width), jnp.bool_)
    for block, rows in enumerate(columns_of):
        for r in rows:
            mask = mask | ((row == r) & (lane == block))
    return jnp.where(mask, 1.0, 0.0).astype(BF16)


def fold(value):
    return value.reshape(TILE // 8, 8, TILE).sum(axis=0)


def each_pair(list_ref, chunks, use, base=0, size=LARGE):
    def group(start, count):
        for e in range(count):
            code = list_ref[start + e]
            use(lax.shift_right_logical(code, 7), code & (TILE - 1))

    def large(c, carry):
        group(base + c * size, size)
        return carry

    def small(c, carry):
        group(base + c * CHUNK, CHUNK)
        return carry

    many = chunks * CHUNK // size
    lax.fori_loop(0, many, large, 0)
    lax.fori_loop(many * (size // CHUNK), chunks, small, 0)


def close_segment(list_ref, n, null, base=0):
    for e in range(CHUNK):
        list_ref[base + n + e] = null
    return (n + CHUNK - 1) // CHUNK


def list_kernel(
    frames,
    me_ref,
    sends_ref,
    dest_ref,
    pair_tiles,
    pair_count,
    own_list,
    ghost_list,
    bounds,
    me_out,
    sends_out,
    dest_out,
):
    pairs, tiles = pair_tiles.shape
    half = own_list.shape[0] // 2
    me = me_ref[0]

    def tile_step(t, found):
        leaving, staying, m = found
        stays = dest_ref[t] == me
        n = jnp.where(stays, staying, leaving)
        count = pair_count[t]
        for b in range(0, pairs, BATCH):
            batch = range(b, min(b + BATCH, pairs))
            found = [pair_tiles[p, t] for p in batch]
            for p, f in zip(batch, found):
                code = t * TILE + f
                own_list[n] = code
                ghost_list[m] = code
                used = (p < count).astype(I32)
                near = jnp.where(f < tiles, used, 0)
                n = n + near
                m = m + used - near
        return jnp.where(stays, leaving, n), jnp.where(stays, n, staying), m

    leaving, staying, m = lax.fori_loop(0, tiles, tile_step, (0, half, 0))
    bounds[0] = close_segment(own_list, leaving, frames)
    bounds[1] = m
    for e in range(CHUNK):
        ghost_list[m + e] = 0
    bounds[2] = close_segment(own_list, staying - half, frames, half)
    me_out[0] = me_ref[0]
    for k in range(sends_ref.shape[0]):
        for g in range(sends_ref.shape[1]):
            sends_out[k, g] = sends_ref[k, g]
    for t in range(tiles):
        dest_out[t] = dest_ref[t]


def density_terms(stream, held, acc_rho, acc_pair):
    def use(t, f):
        both = lax.dot_general(stream[f], held[t], CONTRACT_FIRST, preferred_element_type=F32)
        reach = jnp.maximum(both[:, :TILE], 0.0)
        square = reach * reach
        acc_rho[t] += fold(square * reach * both[:, TILE:])
        acc_pair[t] += fold(square * square)

    return use


def hold_for_density(tiles, frame, held):
    picks = row_mask([[24, 25]], TILE)
    for t in range(tiles):
        parts = held_features(frame[t, 0:4], 1.0) + [jnp.zeros((8, TILE), F32)]
        held[t, :, 0:TILE] = jnp.concatenate(parts, axis=0).astype(BF16)
        held[t, :, TILE:] = picks


def own_density_kernel(
    own_list, bounds, base_ref, occ_ref, rho_ref, pair_ref, held, frame, stream, acc_rho, acc_pair
):
    tiles = occ_ref.shape[0]
    last = frame.shape[0] - 1
    load_own(base_ref, frame)
    hold_for_density(tiles, frame, held)
    for f in range(tiles):
        stream[f] = stream_features(frame[f, 0:4], 1.0, None)
    stream[last] = stream_features(frame[last, 0:4], 1.0, None)
    acc_rho[...] = jnp.zeros_like(acc_rho)
    acc_pair[...] = jnp.zeros_like(acc_pair)
    use = density_terms(stream, held, acc_rho, acc_pair)
    each_pair(own_list, bounds[0], use)
    each_pair(own_list, bounds[2], use, own_list.shape[0] // 2)
    for t in range(tiles):
        rho_ref[t : t + 1] = frame[t, 3:4]
    rho_ref[...] = jnp.sum(acc_rho[...], axis=1) - rho_ref[...]
    pair_ref[...] = jnp.sum(acc_pair[...], axis=1) - occ_ref[...].astype(F32)


def ghost_density_kernel(
    domains,
    me_ref,
    send_list,
    ghost_list,
    bounds,
    base_ref,
    embed_ref,
    occ_ref,
    rho_ref,
    pair_ref,
    held,
    own_ref,
    cross_ref,
    slope_ref,
    energy_ref,
    out_ref,
    frame,
    live_list,
    live_slots,
    live_bounds,
    stream,
    acc_rho,
    acc_pair,
    used_ref,
    live_ref,
):
    me = me_ref[0]
    tiles = occ_ref.shape[0]
    ghosts = send_list.shape[1]
    frames = tiles + SPAN * ghosts
    load_own(base_ref, frame)
    load_ghosts(me, domains, tiles, ghosts, own_ref, cross_ref, frame)
    live_counts(tiles, ghosts, frame, used_ref)
    stream[frames] = stream_features(frame[frames, 0:4], 1.0, None)
    acc_rho[...] = jnp.zeros_like(acc_rho)
    acc_pair[...] = jnp.zeros_like(acc_pair)
    slots = 0
    for k in range(SPAN):
        used = used_ref[k]
        for g in range(ghosts):
            live = (g < used).astype(I32)
            live_ref[tiles + k * ghosts + g] = live
            live_slots[slots] = tiles + k * ghosts + g
            slots = slots + live
    for e in range(WIDE):
        live_slots[slots + e] = frames
    live_bounds[1] = (slots + WIDE - 1) // WIDE
    unroll = CHUNK
    last = bounds[1]
    live_ref[0] = 0

    count = frames - tiles

    def filter_step(c, n):
        for b in range(0, unroll, BATCH):
            codes = [ghost_list[c * unroll + b + e] for e in range(BATCH)]
            live = [live_ref[code & (TILE - 1)] for code in codes]
            for e in range(BATCH):
                live_list[n] = codes[e]
                n = n + live[e]
        for e in range(4):
            f = tiles + jnp.minimum(4 * c + e, count - 1)
            stream[f] = stream_features(frame[f, 0:4], 1.0, None)
        return n

    steps = (last + unroll - 1) // unroll
    n = lax.fori_loop(0, steps, filter_step, 0)

    def feature_step(c, carry):
        for e in range(4):
            f = tiles + jnp.minimum(4 * c + e, count - 1)
            stream[f] = stream_features(frame[f, 0:4], 1.0, None)
        return carry

    lax.fori_loop(steps, (count + 3) // 4, feature_step, 0)
    chunks = close_segment(live_list, n, frames)
    live_bounds[0] = chunks
    use = density_terms(stream, held, acc_rho, acc_pair)
    each_pair(live_list, chunks, use, size=GHOST_LARGE)

    filled = occ_ref[...].astype(F32)
    embed = embed_ref[...]
    root = jnp.sqrt(1.0 + rho_ref[...] + jnp.sum(acc_rho[...], axis=1))
    slope = -0.5 * embed * filled / root
    slope_ref[...] = slope
    pair = pair_ref[...] + jnp.sum(acc_pair[...], axis=1)
    energy_ref[...] = filled * (0.5 * REPULSE * pair - embed * root)
    for k, offset in enumerate(OFFSETS):
        target = me - offset

        @pl.when((target >= 0) & (target < domains))
        def _(k=k, target=target):
            for g in range(ghosts):
                out_ref[target, g : g + 1] = slope_ref[pl.ds(send_list[k, g], 1)]


def hold_for_force(tiles, frame, slope_ref, slopes, held):
    ratio = 1.5 / (SCALE * SCALE)
    for t in range(tiles):
        slopes[t] = slope_ref[t : t + 1]
    for t in range(tiles):
        rows = frame[t, 0:4]
        distance = held_features(rows, SCALE)
        sh, sm, _ = split(slopes[t] * ratio)
        wh, wm, _ = split(rows[3:4] * ratio)
        parts = [sh, sh, sm, wh, wh, wm, jnp.zeros((2, TILE), F32)]
        held[t, :, 0:TILE] = jnp.concatenate(distance + [jnp.zeros((8, TILE), F32)], axis=0).astype(BF16)
        held[t, :, TILE:] = jnp.concatenate(distance + parts, axis=0).astype(BF16)


def stream_for_force(which, frame, slopes, stream):
    for f in which:
        rows = frame[f, 0:4]
        slope = jnp.where(rows[3:4] > 0.0, slopes[f], 0.0)
        stream[f] = stream_features(rows, SCALE, slope)


def widener(stream, wide):
    picks = row_mask([[c, 12 + c, 16 + c] for c in range(3)], 3 * TILE)

    def widen(f, at=None):
        three = lax.dot_general(stream[f], picks, CONTRACT_FIRST, preferred_element_type=F32)
        for c in range(3):
            wide[f if at is None else at, c] = three[:, c * TILE : (c + 1) * TILE]

    return widen


def widen_own(widen, tiles, last):
    step = math.gcd(tiles, WIDE)

    def some(c, carry):
        for e in range(step):
            widen(c * step + e)
        return carry

    lax.fori_loop(0, tiles // step, some, 0)
    widen(last, tiles)


def widen_ghosts(widen, slots_ref, chunks):
    def some(c, carry):
        for e in range(WIDE):
            widen(slots_ref[c * WIDE + e])
        return carry

    lax.fori_loop(0, chunks, some, 0)


def force_terms(stream, held, wide, acc):
    null = wide.shape[0] - 1

    def use(t, f):
        both = lax.dot_general(stream[f], held[t], CONTRACT_FIRST, preferred_element_type=F32)
        reach = jnp.maximum(both[:, :TILE], 0.0)
        coef = reach * reach * both[:, TILE:]
        acc[t, 3] += fold(coef)
        for q in range(3):
            acc[t, q] += fold(coef * wide[jnp.minimum(f, null), q])

    return use


def load_slopes(me, domains, tiles, ghosts, ghost_slope_ref, slopes):
    for k, offset in enumerate(OFFSETS):
        source = jnp.clip(me + offset, 0, domains - 1)
        for g in range(ghosts):
            slopes[tiles + k * ghosts + g] = ghost_slope_ref[source, g : g + 1]


def own_force_kernel(own_list, bounds, base_ref, slope_ref, sums_ref, held, stream, frame, slopes, wide, acc):
    tiles = base_ref.shape[0]
    last = frame.shape[0] - 1
    load_own(base_ref, frame)
    slopes[last] = jnp.zeros((1, TILE), F32)
    hold_for_force(tiles, frame, slope_ref, slopes, held)
    stream_for_force([*range(tiles), last], frame, slopes, stream)
    widen_own(widener(stream, wide), tiles, last)
    acc[...] = jnp.zeros_like(acc)
    each_pair(own_list, bounds[0], force_terms(stream, held, wide, acc))
    for q in range(4):
        sums_ref[q] = jnp.sum(acc[:, q], axis=1)


def staying_force_kernel(own_list, bounds, base_ref, totals_ref, held, stream, force_ref, here_ref, wide, acc, total):
    tiles = base_ref.shape[0]
    widen_own(widener(stream, wide), tiles, stream.shape[0] - 1)
    acc[...] = jnp.zeros_like(acc)
    each_pair(own_list, bounds[2], force_terms(stream, held, wide, acc), own_list.shape[0] // 2)
    for q in range(4):
        total[q] = totals_ref[q] + jnp.sum(acc[:, q], axis=1)
    for t in range(tiles):
        force = force_of(base_ref, total, t)
        force_ref[:, t * TILE : (t + 1) * TILE] = force
        here_ref[:, t * TILE : (t + 1) * TILE] = force


def ghost_force_kernel(
    domains,
    me_ref,
    dest_ref,
    place_ref,
    live_list,
    live_slots,
    live_bounds,
    frame,
    held,
    ghost_slope_ref,
    sums_ref,
    total,
    out_ref,
    slopes,
    stream,
    wide,
    acc,
):
    me = me_ref[0]
    tiles = held.shape[0]
    ghosts = ghost_slope_ref.shape[1]
    frames = tiles + SPAN * ghosts
    load_slopes(me, domains, tiles, ghosts, ghost_slope_ref, slopes)
    slopes[frames] = jnp.zeros((1, TILE), F32)
    stream_for_force(range(tiles, frames + 1), frame, slopes, stream)
    widen = widener(stream, wide)
    widen_ghosts(widen, live_slots, live_bounds[1])
    widen(frames)
    acc[...] = jnp.zeros_like(acc)
    use = force_terms(stream, held, wide, acc)
    each_pair(live_list, live_bounds[0], use, size=GHOST_LARGE)
    for q in range(4):
        total[q] = sums_ref[q] + jnp.sum(acc[:, q], axis=1)
    for t in range(tiles):
        force = force_of(frame, total, t)
        target = dest_ref[t]
        for q in range(3):
            out_ref[target, :, columns(3 * place_ref[t] + q)] = force[q : q + 1]


def force_of(rows_ref, total, t):
    sums = jnp.concatenate([total[q, t : t + 1] for q in range(3)], axis=0)
    return rows_ref[t, 0:3] * total[3, t : t + 1] - sums


def order_kernel(
    domains,
    ghosts,
    me_ref,
    dest_ref,
    move_row,
    own_ref,
    cross_ref,
    table_ref,
    origin_ref,
    count_ref,
    next_ref,
    atoms_ref,
):
    me = me_ref[0]
    tiles = move_row.shape[0]
    base = 4 * ghosts
    next_ref[0] = 0
    atoms_ref[...] = jnp.zeros_like(atoms_ref)

    def from_other(source):
        @pl.when((source >= 0) & (source < domains))
        def _():
            def use(ref, at):
                first = jnp.concatenate(
                    [ref[at, base + 8 * m + 3 : base + 8 * m + 4, :] for m in range(MMAX)], axis=0
                )
                lane = lax.broadcasted_iota(I32, first.shape, 1)
                flag = jnp.where((first >= 0.0) & (lane == 0), 1.0, 0.0)
                count = jnp.sum(flag).astype(I32)
                slot = next_ref[0]
                next_ref[0] = slot + count
                for m in range(MMAX):

                    @pl.when(m < count)
                    def _(m=m):
                        rows = ref[at, base + 8 * m : base + 8 * m + 8]
                        table_ref[slot + m] = rows
                        origin_ref[slot + m] = source * MMAX + m
                        atoms_ref[...] += rows[3:4]

            arrived(me, source, own_ref, cross_ref, use)

    for offset in OFFSETS[:RADIUS]:
        from_other(me + offset)

    slot = next_ref[0]
    for t in range(tiles):
        stays = dest_ref[t] == me
        rows = move_row[t]
        table_ref[slot] = rows
        origin_ref[slot] = -1 - t
        atoms_ref[...] += jnp.where(stays, rows[3:4], 0.0)
        slot = slot + stays.astype(I32)
    next_ref[0] = slot
    for offset in OFFSETS[RADIUS:]:
        from_other(me + offset)
    origin_ref[origin_ref.shape[0] - 1] = next_ref[0]
    count_ref[0] = jnp.sum(atoms_ref[...]).astype(I32)


def finish_kernel(origin_ref, table_ref, force_ref, in_ref, moved_ref):
    capacity = table_ref.shape[0] - 1
    used = origin_ref[capacity + 1]
    unroll = math.gcd(capacity, 8)

    def step(c, carry):
        for e in range(unroll):
            slot = c * unroll + e
            filled = slot < used
            origin = jnp.where(filled, origin_ref[slot], 0)
            other = jnp.maximum(origin, 0)
            stays = origin < 0
            rows = jnp.where(filled, table_ref[slot], 0.0)
            own = force_ref[:, columns(jnp.maximum(-1 - origin, 0))]
            source = lax.div(other, MMAX)
            place = lax.rem(other, MMAX)
            for q in range(3):
                sent = in_ref[source, :, columns(3 * place + q)]
                force = jnp.where(filled, jnp.where(stays, own[q : q + 1], sent), 0.0)
                new_vel = rows[4 + q : 5 + q] + TIME_STEP * force
                moved_ref[q : q + 1, columns(slot)] = rows[q : q + 1] + TIME_STEP * new_vel
                moved_ref[3 + q : 4 + q, columns(slot)] = new_vel
            moved_ref[6:7, columns(slot)] = rows[3:4]
        return carry

    lax.fori_loop(0, capacity // unroll, step, 0)


def per_device(
    positions,
    velocity,
    density_weight,
    embed_strength,
    occupied,
    send_list,
    send_count,
    pair_tiles,
    pair_count,
    migrate_dest,
):
    domains = lax.axis_size("dom")
    tiles, pairs = pair_tiles.shape
    ghosts = send_list.shape[2]
    frames = tiles + SPAN * ghosts
    me = lax.axis_index("dom").astype(I32)[None]
    chi = density_weight.reshape(tiles, TILE)
    embed = embed_strength.reshape(tiles, TILE)
    occ = occupied.reshape(tiles, TILE)
    sends = send_list[0]
    sent = send_count[0]
    pair_rows = pair_tiles.T
    inputs = (me, positions, velocity, chi, embed, occ, sends, sent, pair_rows, pair_count, migrate_dest)
    rows = 4 * ghosts + 8 * MMAX
    capacity = tiles + 2 * RADIUS * MMAX
    entries = tiles * pairs + 4 * CHUNK
    shape = jax.ShapeDtypeStruct
    scalars = shape((4,), I32)
    one_tile = shape((tiles, TILE), F32)

    def call(kernel, name, outs, in_specs, out_specs, scratch, args, final=(), keep=True, limit=8):
        single = not isinstance(outs, list)
        outs = [outs] if single else outs
        out_specs = [out_specs] if single else out_specs
        outs = [
            (pltpu.VMEM if spec is VMEM else pltpu.SMEM)(out.shape, out.dtype) if i not in final else out
            for i, (out, spec) in enumerate(zip(outs, out_specs))
        ]
        args = [
            pltpu.with_memory_space_constraint(arg, pltpu.VMEM)
            if spec is VMEM and keep
            else pltpu.with_memory_space_constraint(arg, pltpu.HBM)
            if any(arg is given for given in inputs)
            else pltpu.with_memory_space_constraint(arg, pltpu.SMEM)
            for arg, spec in zip(args, in_specs)
        ]
        results = pl.pallas_call(
            kernel,
            out_shape=outs,
            in_specs=in_specs,
            out_specs=out_specs,
            scratch_shapes=scratch,
            compiler_params=pltpu.CompilerParams(vmem_limit_bytes=limit * MIB),
            name=name,
        )(*args)
        return results[0] if single else results

    own, cross, base, move_row, places = call(
        functools.partial(pack_kernel, domains),
        "pack",
        [shape((GROUP, rows, TILE), F32)] * 2 + [shape((tiles, 8, TILE), F32)] * 2 + [shape((tiles,), I32)],
        [SMEM] * 4 + [VMEM] * 4,
        [VMEM] * 4 + [SMEM],
        [pltpu.SMEM((2 * RADIUS + 1,), I32)],
        (me, sends, sent, migrate_dest, positions, velocity, chi, occ),
        keep=False,
    )
    blocks = [[b + i for i in range(GROUP)] for b in range(0, domains, GROUP)]
    crossing = [[(b + i - RADIUS) % domains for i in range(GROUP)] for b in range(0, domains, GROUP)]
    own = lax.all_to_all(own, "dom", 0, 0, axis_index_groups=blocks)
    own_list, ghost_list, bounds, me_here, sends_here, dest_here = call(
        functools.partial(list_kernel, frames),
        "lists",
        [shape((2 * entries,), I32), shape((entries,), I32)]
        + [scalars, shape((1,), I32), shape(sends.shape, I32), shape((tiles,), I32)],
        [SMEM] * 5,
        [SMEM] * 6,
        [],
        (me, sends, migrate_dest, pair_rows, pair_count),
    )
    cross, own, bounds = lax.optimization_barrier((cross, own, bounds))
    cross = lax.all_to_all(cross, "dom", 0, 0, axis_index_groups=crossing)

    frame = pltpu.VMEM((frames + 1, 8, TILE), F32)
    stream = pltpu.VMEM((frames + 1, FEATURES, TILE), BF16)
    slopes = pltpu.VMEM((frames + 1, 1, TILE), F32)
    density_sums = [pltpu.VMEM((tiles, 8, TILE), F32)] * 2
    held_shape = shape((tiles, FEATURES, 2 * TILE), BF16)
    rho, pair_sum, held = call(
        own_density_kernel,
        "own_density",
        [one_tile] * 2 + [held_shape],
        [SMEM] * 2 + [VMEM] * 2,
        [VMEM] * 3,
        [frame, stream] + density_sums,
        (own_list, bounds, base, occ),
    )
    slope, energy, slope_out, frame_rows, live_list, live_slots, live_bounds = call(
        functools.partial(ghost_density_kernel, domains),
        "ghost_density",
        [one_tile, one_tile, shape((domains, ghosts, TILE), F32), shape((frames + 1, 8, TILE), F32)]
        + [shape((entries,), I32), shape((SPAN * ghosts + 2 * WIDE,), I32), scalars],
        [SMEM] * 4 + [VMEM] * 8,
        [VMEM] * 4 + [SMEM] * 3,
        [stream] + density_sums + [pltpu.SMEM((SPAN,), I32), pltpu.SMEM((TILE,), I32)],
        (me_here, sends_here, ghost_list, bounds, base, embed, occ, rho, pair_sum, held, own, cross),
        final=(1,),
    )
    slope_in = lax.all_to_all(slope_out, "dom", 0, 0)

    acc = pltpu.VMEM((tiles, 4, 8, TILE), F32)
    wide_own = pltpu.VMEM((tiles + 1, 3, TILE, TILE), F32)
    sums, held, stream_own = call(
        own_force_kernel,
        "own_force",
        [shape((4, tiles, TILE), F32), held_shape, shape((frames + 1, FEATURES, TILE), BF16)],
        [SMEM] * 2 + [VMEM] * 2,
        [VMEM] * 3,
        [frame, slopes, wide_own, acc],
        (own_list, bounds, base, slope),
        limit=16,
    )
    totals, force_out = call(
        functools.partial(ghost_force_kernel, domains),
        "ghost_force",
        [shape((4, tiles, TILE), F32), shape((domains, 1, 3 * MMAX * TILE), F32)],
        [SMEM] * 6 + [VMEM] * 4,
        [VMEM] * 2,
        [slopes, stream, pltpu.VMEM((frames + 1, 3, TILE, TILE), F32), acc],
        (me_here, dest_here, places, live_list, live_slots, live_bounds, frame_rows, held, slope_in, sums),
        limit=26,
    )
    force_in = lax.all_to_all(force_out, "dom", 0, 0)

    force, force_here = call(
        staying_force_kernel,
        "staying_force",
        [shape(positions.shape, F32)] * 2,
        [SMEM] * 2 + [VMEM] * 4,
        [VMEM] * 2,
        [wide_own, acc, pltpu.VMEM((4, tiles, TILE), F32)],
        (own_list, bounds, base, totals, held, stream_own),
        final=(0,),
        limit=16,
    )
    ordered, origin, count = call(
        functools.partial(order_kernel, domains, ghosts),
        "order",
        [shape((capacity + 1, 8, TILE), F32), shape((capacity + 2,), I32), shape((1,), I32)],
        [SMEM] * 2 + [VMEM] * 3,
        [VMEM, SMEM, SMEM],
        [pltpu.SMEM((1,), I32), pltpu.VMEM((1, TILE), F32)],
        (me_here, dest_here, move_row, own, cross),
        final=(2,),
    )
    moved = call(
        finish_kernel,
        "finish",
        shape((7, capacity * TILE), F32),
        [SMEM] + [VMEM] * 3,
        VMEM,
        [],
        (origin, ordered, force_here, force_in),
        final=(0,),
    )
    return (force, energy.reshape(tiles * TILE), moved, count)


def solution(mesh):
    placed = (
        P(None, "dom"),
        P(None, "dom"),
        P("dom"),
        P("dom"),
        P("dom"),
        P("dom", None, None),
        P("dom", None),
        P("dom", None),
        P("dom"),
        P("dom"),
    )
    return jax.shard_map(
        per_device,
        mesh=mesh,
        in_specs=placed,
        out_specs=(P(None, "dom"), P("dom"), P(None, "dom"), P("dom")),
        check_vma=False,
    )
```

```python
import functools
import math

import jax
import jax.numpy as jnp
from jax import lax
from jax.experimental import pallas as pl
from jax.experimental.pallas import tpu as pltpu
from jax.sharding import PartitionSpec as P

TILE = 128
RADIUS = 4
MMAX = 4
REPULSE = 0.05
TIME_STEP = 0.05
SPAN = 2 * RADIUS
GROUP = 2 * RADIUS
F32 = jnp.float32
BF16 = jnp.bfloat16
I32 = jnp.int32
LARGE = 64
GHOST_LARGE = 96
CHUNK = 16
BATCH = 4
WIDE = 16
FEATURES = 32
SCALE = 0.1 ** (1.0 / 3.0)
OFFSETS = [k - RADIUS for k in range(RADIUS)] + [k + 1 for k in range(RADIUS)]
CONTRACT_FIRST = (((0,), (0,)), ((), ()))

VMEM = pl.BlockSpec(memory_space=pltpu.VMEM)
SMEM = pl.BlockSpec(memory_space=pltpu.SMEM)
MIB = 1024 * 1024


def columns(tile):
    return pl.ds(pl.multiple_of(tile * TILE, TILE), TILE)


def split(value):
    high = value.astype(BF16).astype(F32)
    rest = value - high
    mid = rest.astype(BF16).astype(F32)
    return high, mid, rest - mid


def pack_kernel(
    domains,
    me_ref,
    send_list,
    send_count,
    dest_ref,
    pos_ref,
    vel_ref,
    chi_ref,
    occ_ref,
    own_ref,
    cross_ref,
    ghost_row,
    move_row,
    place_ref,
    rank_ref,
):
    me = me_ref[0]
    tiles = chi_ref.shape[0]
    ghosts = send_list.shape[1]
    base = 4 * ghosts
    filled = occ_ref[...].astype(F32)
    weight = chi_ref[...] * filled
    for t in range(tiles):
        span = slice(t * TILE, (t + 1) * TILE)
        ghost_row[t, 0:3] = pos_ref[:, span]
        ghost_row[t, 3:4] = weight[t : t + 1]
        move_row[t, 0:3] = pos_ref[:, span]
        move_row[t, 3:4] = filled[t : t + 1]
        move_row[t, 4:7] = vel_ref[:, span]
    nothing = jnp.full((1, TILE), -1.0, F32)

    def place(target, rows):
        inside = (target // GROUP) == (me // GROUP)

        @pl.when(inside)
        def _():
            rows(own_ref, target % GROUP)

        @pl.when(jnp.logical_not(inside))
        def _():
            rows(cross_ref, (target + RADIUS) % GROUP)

    for k, offset in enumerate(OFFSETS):
        target = me - offset

        @pl.when((target >= 0) & (target < domains))
        def _(k=k, target=target):
            used = send_count[k]

            def rows(out_ref, at):
                for g in range(ghosts):
                    block = ghost_row[send_list[k, g]]
                    live = g < used
                    out_ref[at, 4 * g : 4 * g + 3] = block[0:3]
                    out_ref[at, 4 * g + 3 : 4 * g + 4] = jnp.where(live, block[3:4], nothing)
                for m in range(MMAX):
                    out_ref[at, base + 8 * m + 3 : base + 8 * m + 4] = nothing

            place(target, rows)

    for r in range(2 * RADIUS + 1):
        rank_ref[r] = 0

    for t in range(tiles):
        target = dest_ref[t]
        relative = target - me + RADIUS
        rank = rank_ref[relative]
        rank_ref[relative] = rank + 1
        rank = jnp.minimum(rank, MMAX - 1)
        place_ref[t] = rank
        inside = lax.div(target, GROUP) == lax.div(me, GROUP)
        row = pl.ds(pl.multiple_of(base + 8 * rank, 8), 8)
        own_ref[lax.rem(jnp.where(inside, target, me), GROUP), row] = move_row[t]
        cross_ref[lax.rem(jnp.where(inside, me, target) + RADIUS, GROUP), row] = move_row[t]


def arrived(me, source, own_ref, cross_ref, use):
    inside = (source // GROUP) == (me // GROUP)

    @pl.when(inside)
    def _():
        use(own_ref, source % GROUP)

    @pl.when(jnp.logical_not(inside))
    def _():
        use(cross_ref, (source + RADIUS) % GROUP)


def load_own(base_ref, frame):
    tiles = base_ref.shape[0]
    last = frame.shape[0] - 1
    frame[0:tiles] = base_ref[...]
    frame[last, 0:4] = jnp.full((4, TILE), -1.0, F32)


def load_ghosts(me, domains, tiles, ghosts, own_ref, cross_ref, frame):
    for k, offset in enumerate(OFFSETS):
        source = me + offset
        start = tiles + k * ghosts
        valid = (source >= 0) & (source < domains)

        @pl.when(valid)
        def _(start=start, source=source):
            def use(ref, at):
                for g in range(ghosts):
                    frame[start + g, 0:4] = ref[at, 4 * g : 4 * g + 4]

            arrived(me, source, own_ref, cross_ref, use)

        @pl.when(jnp.logical_not(valid))
        def _(start=start):
            for g in range(ghosts):
                frame[start + g, 0:4] = jnp.full((4, TILE), -1.0, F32)


def live_counts(tiles, ghosts, frame, used_ref):
    for k in range(SPAN):
        start = tiles + k * ghosts
        first = frame[start : start + ghosts, 3, :]
        lane = lax.broadcasted_iota(I32, first.shape, 1)
        flag = jnp.where((first >= 0.0) & (lane == 0), 1.0, 0.0)
        used_ref[k] = jnp.sum(flag).astype(I32)


def scaled(rows, scale):
    half = rows[0:3] * 0.5
    norm = 0.5 - (half[0:1] * half[0:1] + half[1:2] * half[1:2] + half[2:3] * half[2:3])
    norm = jnp.where(rows[3:4] > 0.0, norm, -64.0) * scale
    return half, norm


def stream_features(rows, scale, slope):
    half, norm = scaled(rows, scale)
    high, mid, low = split(half + half)
    one = jnp.ones((1, TILE), F32)
    nh, nm, nl = split(norm)
    weight = jnp.maximum(rows[3:4], 0.0)
    wh, wm, _ = split(weight)
    if slope is None:
        tail = [wh, wm, jnp.zeros((6, TILE), F32)]
    else:
        sh, sm, _ = split(slope)
        tail = [wh, wm, wh, sh, sm, sh, jnp.zeros((2, TILE), F32)]
    parts = [high, one, high, one, high, one, mid, nm, low, nl, mid, nh] + tail
    return jnp.concatenate(parts, axis=0).astype(BF16)


def held_features(rows, scale):
    half, norm = scaled(rows, scale)
    high, mid, low = split(half * scale)
    nh, nm, nl = split(norm)
    one = jnp.ones((1, TILE), F32)
    return [high, nh, mid, nm, low, nl, high, one, high, one, mid, one]


def row_mask(columns_of, width):
    row = lax.broadcasted_iota(I32, (FEATURES, width), 0)
    lane = lax.broadcasted_iota(I32, (FEATURES, width), 1) // TILE
    mask = jnp.zeros((FEATURES, width), jnp.bool_)
    for block, rows in enumerate(columns_of):
        for r in rows:
            mask = mask | ((row == r) & (lane == block))
    return jnp.where(mask, 1.0, 0.0).astype(BF16)


def fold(value):
    return value.reshape(TILE // 8, 8, TILE).sum(axis=0)


def each_pair(list_ref, chunks, use, base=0, size=LARGE):
    def group(start, count):
        for e in range(count):
            code = list_ref[start + e]
            use(lax.shift_right_logical(code, 7), code & (TILE - 1))

    def large(c, carry):
        group(base + c * size, size)
        return carry

    def small(c, carry):
        group(base + c * CHUNK, CHUNK)
        return carry

    many = chunks * CHUNK // size
    lax.fori_loop(0, many, large, 0)
    lax.fori_loop(many * (size // CHUNK), chunks, small, 0)


def close_segment(list_ref, n, null, base=0):
    for e in range(CHUNK):
        list_ref[base + n + e] = null
    return (n + CHUNK - 1) // CHUNK


def list_kernel(
    frames,
    me_ref,
    sends_ref,
    dest_ref,
    pair_tiles,
    pair_count,
    own_list,
    ghost_list,
    bounds,
    me_out,
    sends_out,
    dest_out,
):
    pairs, tiles = pair_tiles.shape
    half = own_list.shape[0] // 2
    me = me_ref[0]

    def tile_step(t, found):
        leaving, staying, m = found
        stays = dest_ref[t] == me
        n = jnp.where(stays, staying, leaving)
        count = pair_count[t]
        for b in range(0, pairs, BATCH):
            batch = range(b, min(b + BATCH, pairs))
            found = [pair_tiles[p, t] for p in batch]
            for p, f in zip(batch, found):
                code = t * TILE + f
                own_list[n] = code
                ghost_list[m] = code
                used = (p < count).astype(I32)
                near = jnp.where(f < tiles, used, 0)
                n = n + near
                m = m + used - near
        return jnp.where(stays, leaving, n), jnp.where(stays, n, staying), m

    leaving, staying, m = lax.fori_loop(0, tiles, tile_step, (0, half, 0))
    bounds[0] = close_segment(own_list, leaving, frames)
    bounds[1] = m
    for e in range(CHUNK):
        ghost_list[m + e] = 0
    bounds[2] = close_segment(own_list, staying - half, frames, half)
    me_out[0] = me_ref[0]
    for k in range(sends_ref.shape[0]):
        for g in range(sends_ref.shape[1]):
            sends_out[k, g] = sends_ref[k, g]
    for t in range(tiles):
        dest_out[t] = dest_ref[t]


def density_terms(stream, held, acc_rho, acc_pair):
    def use(t, f):
        both = lax.dot_general(stream[f], held[t], CONTRACT_FIRST, preferred_element_type=F32)
        reach = jnp.maximum(both[:, :TILE], 0.0)
        square = reach * reach
        acc_rho[t] += fold(square * reach * both[:, TILE:])
        acc_pair[t] += fold(square * square)

    return use


def hold_for_density(tiles, frame, held):
    picks = row_mask([[24, 25]], TILE)
    for t in range(tiles):
        parts = held_features(frame[t, 0:4], 1.0) + [jnp.zeros((8, TILE), F32)]
        held[t, :, 0:TILE] = jnp.concatenate(parts, axis=0).astype(BF16)
        held[t, :, TILE:] = picks


def own_density_kernel(
    own_list, bounds, base_ref, occ_ref, rho_ref, pair_ref, held, frame, stream, acc_rho, acc_pair
):
    tiles = occ_ref.shape[0]
    last = frame.shape[0] - 1
    load_own(base_ref, frame)
    hold_for_density(tiles, frame, held)
    for f in range(tiles):
        stream[f] = stream_features(frame[f, 0:4], 1.0, None)
    stream[last] = stream_features(frame[last, 0:4], 1.0, None)
    acc_rho[...] = jnp.zeros_like(acc_rho)
    acc_pair[...] = jnp.zeros_like(acc_pair)
    use = density_terms(stream, held, acc_rho, acc_pair)
    each_pair(own_list, bounds[0], use)
    each_pair(own_list, bounds[2], use, own_list.shape[0] // 2)
    for t in range(tiles):
        rho_ref[t : t + 1] = frame[t, 3:4]
    rho_ref[...] = jnp.sum(acc_rho[...], axis=1) - rho_ref[...]
    pair_ref[...] = jnp.sum(acc_pair[...], axis=1) - occ_ref[...].astype(F32)


def ghost_density_kernel(
    domains,
    me_ref,
    send_list,
    ghost_list,
    bounds,
    base_ref,
    embed_ref,
    occ_ref,
    rho_ref,
    pair_ref,
    held,
    own_ref,
    cross_ref,
    slope_ref,
    energy_ref,
    out_ref,
    frame,
    live_list,
    live_slots,
    live_bounds,
    stream,
    acc_rho,
    acc_pair,
    used_ref,
    live_ref,
):
    me = me_ref[0]
    tiles = occ_ref.shape[0]
    ghosts = send_list.shape[1]
    frames = tiles + SPAN * ghosts
    load_own(base_ref, frame)
    load_ghosts(me, domains, tiles, ghosts, own_ref, cross_ref, frame)
    live_counts(tiles, ghosts, frame, used_ref)
    stream[frames] = stream_features(frame[frames, 0:4], 1.0, None)
    acc_rho[...] = jnp.zeros_like(acc_rho)
    acc_pair[...] = jnp.zeros_like(acc_pair)
    slots = 0
    for k in range(SPAN):
        used = used_ref[k]
        for g in range(ghosts):
            live = (g < used).astype(I32)
            live_ref[tiles + k * ghosts + g] = live
            live_slots[slots] = tiles + k * ghosts + g
            slots = slots + live
    for e in range(WIDE):
        live_slots[slots + e] = frames
    live_bounds[1] = (slots + WIDE - 1) // WIDE
    unroll = CHUNK
    last = bounds[1]
    live_ref[0] = 0

    count = frames - tiles

    def filter_step(c, n):
        for b in range(0, unroll, BATCH):
            codes = [ghost_list[c * unroll + b + e] for e in range(BATCH)]
            live = [live_ref[code & (TILE - 1)] for code in codes]
            for e in range(BATCH):
                live_list[n] = codes[e]
                n = n + live[e]
        for e in range(4):
            f = tiles + jnp.minimum(4 * c + e, count - 1)
            stream[f] = stream_features(frame[f, 0:4], 1.0, None)
        return n

    steps = (last + unroll - 1) // unroll
    n = lax.fori_loop(0, steps, filter_step, 0)

    def feature_step(c, carry):
        for e in range(4):
            f = tiles + jnp.minimum(4 * c + e, count - 1)
            stream[f] = stream_features(frame[f, 0:4], 1.0, None)
        return carry

    lax.fori_loop(steps, (count + 3) // 4, feature_step, 0)
    chunks = close_segment(live_list, n, frames)
    live_bounds[0] = chunks
    use = density_terms(stream, held, acc_rho, acc_pair)
    each_pair(live_list, chunks, use, size=GHOST_LARGE)

    filled = occ_ref[...].astype(F32)
    embed = embed_ref[...]
    root = jnp.sqrt(1.0 + rho_ref[...] + jnp.sum(acc_rho[...], axis=1))
    slope = -0.5 * embed * filled / root
    slope_ref[...] = slope
    pair = pair_ref[...] + jnp.sum(acc_pair[...], axis=1)
    energy_ref[...] = filled * (0.5 * REPULSE * pair - embed * root)
    for k, offset in enumerate(OFFSETS):
        target = me - offset

        @pl.when((target >= 0) & (target < domains))
        def _(k=k, target=target):
            for g in range(ghosts):
                out_ref[target, g : g + 1] = slope_ref[pl.ds(send_list[k, g], 1)]


def hold_for_force(tiles, frame, slope_ref, slopes, held):
    ratio = 1.5 / (SCALE * SCALE)
    for t in range(tiles):
        slopes[t] = slope_ref[t : t + 1]
    for t in range(tiles):
        rows = frame[t, 0:4]
        distance = held_features(rows, SCALE)
        sh, sm, _ = split(slopes[t] * ratio)
        wh, wm, _ = split(rows[3:4] * ratio)
        parts = [sh, sh, sm, wh, wh, wm, jnp.zeros((2, TILE), F32)]
        held[t, :, 0:TILE] = jnp.concatenate(distance + [jnp.zeros((8, TILE), F32)], axis=0).astype(BF16)
        held[t, :, TILE:] = jnp.concatenate(distance + parts, axis=0).astype(BF16)


def stream_for_force(which, frame, slopes, stream):
    for f in which:
        rows = frame[f, 0:4]
        slope = jnp.where(rows[3:4] > 0.0, slopes[f], 0.0)
        stream[f] = stream_features(rows, SCALE, slope)


def widener(stream, wide):
    picks = row_mask([[c, 12 + c, 16 + c] for c in range(3)], 3 * TILE)

    def widen(f, at=None):
        three = lax.dot_general(stream[f], picks, CONTRACT_FIRST, preferred_element_type=F32)
        for c in range(3):
            wide[f if at is None else at, c] = three[:, c * TILE : (c + 1) * TILE]

    return widen


def widen_own(widen, tiles, last):
    step = math.gcd(tiles, WIDE)

    def some(c, carry):
        for e in range(step):
            widen(c * step + e)
        return carry

    lax.fori_loop(0, tiles // step, some, 0)
    widen(last, tiles)


def widen_ghosts(widen, slots_ref, chunks):
    def some(c, carry):
        for e in range(WIDE):
            widen(slots_ref[c * WIDE + e])
        return carry

    lax.fori_loop(0, chunks, some, 0)


def force_terms(stream, held, wide, acc):
    null = wide.shape[0] - 1

    def use(t, f):
        both = lax.dot_general(stream[f], held[t], CONTRACT_FIRST, preferred_element_type=F32)
        reach = jnp.maximum(both[:, :TILE], 0.0)
        coef = reach * reach * both[:, TILE:]
        acc[t, 3] += fold(coef)
        for q in range(3):
            acc[t, q] += fold(coef * wide[jnp.minimum(f, null), q])

    return use


def load_slopes(me, domains, tiles, ghosts, ghost_slope_ref, slopes):
    for k, offset in enumerate(OFFSETS):
        source = jnp.clip(me + offset, 0, domains - 1)
        for g in range(ghosts):
            slopes[tiles + k * ghosts + g] = ghost_slope_ref[source, g : g + 1]


def own_force_kernel(own_list, bounds, base_ref, slope_ref, sums_ref, held, stream, frame, slopes, wide, acc):
    tiles = base_ref.shape[0]
    last = frame.shape[0] - 1
    load_own(base_ref, frame)
    slopes[last] = jnp.zeros((1, TILE), F32)
    hold_for_force(tiles, frame, slope_ref, slopes, held)
    stream_for_force([*range(tiles), last], frame, slopes, stream)
    widen_own(widener(stream, wide), tiles, last)
    acc[...] = jnp.zeros_like(acc)
    each_pair(own_list, bounds[0], force_terms(stream, held, wide, acc))
    for q in range(4):
        sums_ref[q] = jnp.sum(acc[:, q], axis=1)


def staying_force_kernel(own_list, bounds, base_ref, totals_ref, held, stream, force_ref, here_ref, wide, acc, total):
    tiles = base_ref.shape[0]
    widen_own(widener(stream, wide), tiles, stream.shape[0] - 1)
    acc[...] = jnp.zeros_like(acc)
    each_pair(own_list, bounds[2], force_terms(stream, held, wide, acc), own_list.shape[0] // 2)
    for q in range(4):
        total[q] = totals_ref[q] + jnp.sum(acc[:, q], axis=1)
    for t in range(tiles):
        force = force_of(base_ref, total, t)
        force_ref[:, t * TILE : (t + 1) * TILE] = force
        here_ref[:, t * TILE : (t + 1) * TILE] = force


def ghost_force_kernel(
    domains,
    me_ref,
    dest_ref,
    place_ref,
    live_list,
    live_slots,
    live_bounds,
    frame,
    held,
    ghost_slope_ref,
    sums_ref,
    total,
    out_ref,
    slopes,
    stream,
    wide,
    acc,
):
    me = me_ref[0]
    tiles = held.shape[0]
    ghosts = ghost_slope_ref.shape[1]
    frames = tiles + SPAN * ghosts
    load_slopes(me, domains, tiles, ghosts, ghost_slope_ref, slopes)
    slopes[frames] = jnp.zeros((1, TILE), F32)
    stream_for_force(range(tiles, frames + 1), frame, slopes, stream)
    widen = widener(stream, wide)
    widen_ghosts(widen, live_slots, live_bounds[1])
    widen(frames)
    acc[...] = jnp.zeros_like(acc)
    use = force_terms(stream, held, wide, acc)
    each_pair(live_list, live_bounds[0], use, size=GHOST_LARGE)
    for q in range(4):
        total[q] = sums_ref[q] + jnp.sum(acc[:, q], axis=1)
    for t in range(tiles):
        force = force_of(frame, total, t)
        target = dest_ref[t]
        for q in range(3):
            out_ref[target, :, columns(3 * place_ref[t] + q)] = force[q : q + 1]


def force_of(rows_ref, total, t):
    sums = jnp.concatenate([total[q, t : t + 1] for q in range(3)], axis=0)
    return rows_ref[t, 0:3] * total[3, t : t + 1] - sums


def order_kernel(
    domains,
    ghosts,
    me_ref,
    dest_ref,
    move_row,
    own_ref,
    cross_ref,
    table_ref,
    origin_ref,
    count_ref,
    next_ref,
    atoms_ref,
):
    me = me_ref[0]
    tiles = move_row.shape[0]
    base = 4 * ghosts
    next_ref[0] = 0
    atoms_ref[...] = jnp.zeros_like(atoms_ref)

    def from_other(source):
        @pl.when((source >= 0) & (source < domains))
        def _():
            def use(ref, at):
                first = jnp.concatenate(
                    [ref[at, base + 8 * m + 3 : base + 8 * m + 4, :] for m in range(MMAX)], axis=0
                )
                lane = lax.broadcasted_iota(I32, first.shape, 1)
                flag = jnp.where((first >= 0.0) & (lane == 0), 1.0, 0.0)
                count = jnp.sum(flag).astype(I32)
                slot = next_ref[0]
                next_ref[0] = slot + count
                for m in range(MMAX):

                    @pl.when(m < count)
                    def _(m=m):
                        rows = ref[at, base + 8 * m : base + 8 * m + 8]
                        table_ref[slot + m] = rows
                        origin_ref[slot + m] = source * MMAX + m
                        atoms_ref[...] += rows[3:4]

            arrived(me, source, own_ref, cross_ref, use)

    for offset in OFFSETS[:RADIUS]:
        from_other(me + offset)

    slot = next_ref[0]
    for t in range(tiles):
        stays = dest_ref[t] == me
        rows = move_row[t]
        table_ref[slot] = rows
        origin_ref[slot] = -1 - t
        atoms_ref[...] += jnp.where(stays, rows[3:4], 0.0)
        slot = slot + stays.astype(I32)
    next_ref[0] = slot
    for offset in OFFSETS[RADIUS:]:
        from_other(me + offset)
    origin_ref[origin_ref.shape[0] - 1] = next_ref[0]
    count_ref[0] = jnp.sum(atoms_ref[...]).astype(I32)


def finish_kernel(origin_ref, table_ref, force_ref, in_ref, moved_ref):
    capacity = table_ref.shape[0] - 1
    used = origin_ref[capacity + 1]
    unroll = math.gcd(capacity, 16)

    def step(c, carry):
        for e in range(unroll):
            slot = c * unroll + e
            filled = slot < used
            origin = jnp.where(filled, origin_ref[slot], 0)
            other = jnp.maximum(origin, 0)
            stays = origin < 0
            rows = jnp.where(filled, table_ref[slot], 0.0)
            own = force_ref[:, columns(jnp.maximum(-1 - origin, 0))]
            source = lax.div(other, MMAX)
            place = lax.rem(other, MMAX)
            for q in range(3):
                sent = in_ref[source, :, columns(3 * place + q)]
                force = jnp.where(filled, jnp.where(stays, own[q : q + 1], sent), 0.0)
                new_vel = rows[4 + q : 5 + q] + TIME_STEP * force
                moved_ref[q : q + 1, columns(slot)] = rows[q : q + 1] + TIME_STEP * new_vel
                moved_ref[3 + q : 4 + q, columns(slot)] = new_vel
            moved_ref[6:7, columns(slot)] = rows[3:4]
        return carry

    lax.fori_loop(0, capacity // unroll, step, 0)


def per_device(
    positions,
    velocity,
    density_weight,
    embed_strength,
    occupied,
    send_list,
    send_count,
    pair_tiles,
    pair_count,
    migrate_dest,
):
    domains = lax.axis_size("dom")
    tiles, pairs = pair_tiles.shape
    ghosts = send_list.shape[2]
    frames = tiles + SPAN * ghosts
    me = lax.axis_index("dom").astype(I32)[None]
    chi = density_weight.reshape(tiles, TILE)
    embed = embed_strength.reshape(tiles, TILE)
    occ = occupied.reshape(tiles, TILE)
    sends = send_list[0]
    sent = send_count[0]
    pair_rows = pair_tiles.T
    inputs = (me, positions, velocity, chi, embed, occ, sends, sent, pair_rows, pair_count, migrate_dest)
    rows = 4 * ghosts + 8 * MMAX
    capacity = tiles + 2 * RADIUS * MMAX
    entries = tiles * pairs + 4 * CHUNK
    shape = jax.ShapeDtypeStruct
    scalars = shape((4,), I32)
    one_tile = shape((tiles, TILE), F32)

    def call(kernel, name, outs, in_specs, out_specs, scratch, args, final=(), keep=True, limit=8):
        single = not isinstance(outs, list)
        outs = [outs] if single else outs
        out_specs = [out_specs] if single else out_specs
        outs = [
            (pltpu.VMEM if spec is VMEM else pltpu.SMEM)(out.shape, out.dtype) if i not in final else out
            for i, (out, spec) in enumerate(zip(outs, out_specs))
        ]
        args = [
            pltpu.with_memory_space_constraint(arg, pltpu.VMEM)
            if spec is VMEM and keep
            else pltpu.with_memory_space_constraint(arg, pltpu.HBM)
            if any(arg is given for given in inputs)
            else pltpu.with_memory_space_constraint(arg, pltpu.SMEM)
            for arg, spec in zip(args, in_specs)
        ]
        results = pl.pallas_call(
            kernel,
            out_shape=outs,
            in_specs=in_specs,
            out_specs=out_specs,
            scratch_shapes=scratch,
            compiler_params=pltpu.CompilerParams(vmem_limit_bytes=limit * MIB),
            name=name,
        )(*args)
        return results[0] if single else results

    own, cross, base, move_row, places = call(
        functools.partial(pack_kernel, domains),
        "pack",
        [shape((GROUP, rows, TILE), F32)] * 2 + [shape((tiles, 8, TILE), F32)] * 2 + [shape((tiles,), I32)],
        [SMEM] * 4 + [VMEM] * 4,
        [VMEM] * 4 + [SMEM],
        [pltpu.SMEM((2 * RADIUS + 1,), I32)],
        (me, sends, sent, migrate_dest, positions, velocity, chi, occ),
        keep=False,
    )
    blocks = [[b + i for i in range(GROUP)] for b in range(0, domains, GROUP)]
    crossing = [[(b + i - RADIUS) % domains for i in range(GROUP)] for b in range(0, domains, GROUP)]
    own = lax.all_to_all(own, "dom", 0, 0, axis_index_groups=blocks)
    own_list, ghost_list, bounds, me_here, sends_here, dest_here = call(
        functools.partial(list_kernel, frames),
        "lists",
        [shape((2 * entries,), I32), shape((entries,), I32)]
        + [scalars, shape((1,), I32), shape(sends.shape, I32), shape((tiles,), I32)],
        [SMEM] * 5,
        [SMEM] * 6,
        [],
        (me, sends, migrate_dest, pair_rows, pair_count),
    )
    cross, own, bounds = lax.optimization_barrier((cross, own, bounds))
    cross = lax.all_to_all(cross, "dom", 0, 0, axis_index_groups=crossing)

    frame = pltpu.VMEM((frames + 1, 8, TILE), F32)
    stream = pltpu.VMEM((frames + 1, FEATURES, TILE), BF16)
    slopes = pltpu.VMEM((frames + 1, 1, TILE), F32)
    density_sums = [pltpu.VMEM((tiles, 8, TILE), F32)] * 2
    held_shape = shape((tiles, FEATURES, 2 * TILE), BF16)
    rho, pair_sum, held = call(
        own_density_kernel,
        "own_density",
        [one_tile] * 2 + [held_shape],
        [SMEM] * 2 + [VMEM] * 2,
        [VMEM] * 3,
        [frame, stream] + density_sums,
        (own_list, bounds, base, occ),
    )
    slope, energy, slope_out, frame_rows, live_list, live_slots, live_bounds = call(
        functools.partial(ghost_density_kernel, domains),
        "ghost_density",
        [one_tile, one_tile, shape((domains, ghosts, TILE), F32), shape((frames + 1, 8, TILE), F32)]
        + [shape((entries,), I32), shape((SPAN * ghosts + 2 * WIDE,), I32), scalars],
        [SMEM] * 4 + [VMEM] * 8,
        [VMEM] * 4 + [SMEM] * 3,
        [stream] + density_sums + [pltpu.SMEM((SPAN,), I32), pltpu.SMEM((TILE,), I32)],
        (me_here, sends_here, ghost_list, bounds, base, embed, occ, rho, pair_sum, held, own, cross),
        final=(1,),
    )
    slope_in = lax.all_to_all(slope_out, "dom", 0, 0)

    acc = pltpu.VMEM((tiles, 4, 8, TILE), F32)
    wide_own = pltpu.VMEM((tiles + 1, 3, TILE, TILE), F32)
    sums, held, stream_own = call(
        own_force_kernel,
        "own_force",
        [shape((4, tiles, TILE), F32), held_shape, shape((frames + 1, FEATURES, TILE), BF16)],
        [SMEM] * 2 + [VMEM] * 2,
        [VMEM] * 3,
        [frame, slopes, wide_own, acc],
        (own_list, bounds, base, slope),
        limit=16,
    )
    totals, force_out = call(
        functools.partial(ghost_force_kernel, domains),
        "ghost_force",
        [shape((4, tiles, TILE), F32), shape((domains, 1, 3 * MMAX * TILE), F32)],
        [SMEM] * 6 + [VMEM] * 4,
        [VMEM] * 2,
        [slopes, stream, pltpu.VMEM((frames + 1, 3, TILE, TILE), F32), acc],
        (me_here, dest_here, places, live_list, live_slots, live_bounds, frame_rows, held, slope_in, sums),
        limit=26,
    )
    force_in = lax.all_to_all(force_out, "dom", 0, 0)

    force, force_here = call(
        staying_force_kernel,
        "staying_force",
        [shape(positions.shape, F32)] * 2,
        [SMEM] * 2 + [VMEM] * 4,
        [VMEM] * 2,
        [wide_own, acc, pltpu.VMEM((4, tiles, TILE), F32)],
        (own_list, bounds, base, totals, held, stream_own),
        final=(0,),
        limit=16,
    )
    ordered, origin, count = call(
        functools.partial(order_kernel, domains, ghosts),
        "order",
        [shape((capacity + 1, 8, TILE), F32), shape((capacity + 2,), I32), shape((1,), I32)],
        [SMEM] * 2 + [VMEM] * 3,
        [VMEM, SMEM, SMEM],
        [pltpu.SMEM((1,), I32), pltpu.VMEM((1, TILE), F32)],
        (me_here, dest_here, move_row, own, cross),
        final=(2,),
    )
    moved = call(
        finish_kernel,
        "finish",
        shape((7, capacity * TILE), F32),
        [SMEM] + [VMEM] * 3,
        VMEM,
        [],
        (origin, ordered, force_here, force_in),
        final=(0,),
    )
    return (force, energy.reshape(tiles * TILE), moved, count)


def solution(mesh):
    placed = (
        P(None, "dom"),
        P(None, "dom"),
        P("dom"),
        P("dom"),
        P("dom"),
        P("dom", None, None),
        P("dom", None),
        P("dom", None),
        P("dom"),
        P("dom"),
    )
    return jax.shard_map(
        per_device,
        mesh=mesh,
        in_specs=placed,
        out_specs=(P(None, "dom"), P("dom"), P(None, "dom"), P("dom")),
        check_vma=False,
    )
```
